512 devices in a mesh: lat: 16 (over y, core), lon: 32 (over z, x).
Axes of the slice: x: 4, y: 8, z: 8, core: 2. Of those that a mesh axis runs over, the one named last changes fastest.
Arguments:
- forcing: float32 [2560, 4096], P('lat', 'lon'), may hold values from -28 to 28
- search_direction: float32 [2560, 4096], P('lat', 'lon'), may hold values from -28 to 28
- ocean_depth: float32 [2560, 4096], P('lat', 'lon'), may hold values from 0.5 to 8
- land_mask: int32 [2560, 4096], P('lat', 'lon'), may hold values 0 or 1
- fold_map: int32 [4096], replicated, may hold values from 0 to 4095, as said below
Outputs:
- scaled_height: float32 [2560, 4096], P('lat', 'lon')
- residual: float32 [2560, 4096], P('lat', 'lon')
The draws below stay inside these ranges and needn't reach their ends.
Inputs may be any that keep to these rules, and one draw needn't show every extreme that they name: `fold_map`: column j's partner across the fold is (c - j) mod 4096 for one c of 0 to 4095, so the map is its own inverse.
All inputs are finite; a program needn't handle non-finite values. No bound on the sum of `land_mask` on one device may be relied on, other than what follows from the above.
Results may differ from the reference program's by a relative error of at most 0.0003.
Values sent between devices are 32-bit elements; how exact they have to be, the bound alone decides.
No kernel may reach another device: no remote copies, remote signals or barrier semaphores. Data moves between devices by JAX's collectives and lax.ppermute only.
A program may use at most 64 MiB of HBM per device.

```python
import math
import jax
import jax.numpy as jnp
import numpy as np
from jax import lax

STEPS = 8
OUTER = 1
REACH = 256
NX = 2560
NY = 4096


def field_profile():
    lat_ramp = jnp.arange(NX, dtype=jnp.float32) / NX
    lon_ramp = jnp.arange(NY, dtype=jnp.float32) / NY
    north_gap = (NX - 1 - jnp.arange(NX, dtype=jnp.float32)) / 8.0
    north_boost = 1.0 + 1.5 * jnp.exp(-north_gap)
    return jnp.exp(jnp.log(3.0) * (lat_ramp[:, None] + lon_ramp[None, :])) * north_boost[:, None]


def rough_field(key):
    first_key = jax.random.fold_in(key, 0)
    values = jax.random.truncated_normal(first_key, -4.0, 4.0, (NX, NY), jnp.float32)
    return (0.3 * values * field_profile()).astype(jnp.float32)


def draw_forcing(key, part):
    return rough_field(jax.random.fold_in(key, 11))


def draw_search_direction(key, part):
    return rough_field(jax.random.fold_in(key, 23))


def draw_fold_map(key, part):
    pivot_column = jax.random.randint(jax.random.fold_in(key, 7), (), 0, NY, dtype=jnp.int32)
    return ((pivot_column - jnp.arange(NY, dtype=jnp.int32)) % NY).astype(jnp.int32)


def set_ends(drawn, stream_key, smallest, top_value):
    longest = drawn.shape.index(max(drawn.shape))
    spots = []
    for shift in (0, 1):
        where = [jax.random.randint(jax.random.fold_in(stream_key, axis), (), 0, length) for axis, length in enumerate(drawn.shape)]
        where[longest] = (where[longest] + shift) % drawn.shape[longest]
        spots.append(tuple(where))
    return drawn.at[spots[0]].set(smallest).at[spots[1]].set(top_value)


def level_of(key, extent, pieces, low, largest):
    level = 1.0
    for dim, shards_of in pieces:
        draws = jax.random.uniform(jax.random.fold_in(jax.random.fold_in(key, 6), dim), (shards_of,), jnp.float32, low / len(pieces), largest / len(pieces))
        level = level * jnp.repeat(jnp.exp(draws), extent[dim] // shards_of).reshape((-1,) + (1,) * (len(extent) - 1 - dim))
    return level


def setup_inputs(seed: int = 0) -> dict:
    key_of = jax.random.split(jax.random.key(seed), 6)
    forcing = draw_forcing(jax.random.fold_in(key_of[5], 71), 0)
    search_direction = draw_search_direction(jax.random.fold_in(key_of[5], 71), 0)
    ocean_depth = jnp.clip(jnp.exp(math.log(8.0) - 2.7725887 * jax.random.uniform(key_of[2], (NX, NY), jnp.float32) ** level_of(key_of[2], (NX, NY), ((0, 16), (1, 32)), -0.2, 0.2)), 0.5, 8.0)
    land_mask = set_ends((jax.random.randint(key_of[3], (NX, NY), 0, 8) < 7).astype(jnp.int32), jax.random.fold_in(key_of[3], 1), 0, 1)
    fold_map = draw_fold_map(jax.random.fold_in(key_of[5], 71), 0)
    return dict(forcing=forcing, search_direction=search_direction, ocean_depth=ocean_depth, land_mask=land_mask, fold_map=fold_map)


PRECISE = lax.Precision.HIGHEST
DIRECTIONS = ((1, 0), (-1, 0), (0, 1), (0, -1), (1, 1), (-1, -1), (1, -1), (-1, 1))
LINK_FACTORS = (1.0, 1.0, 1.0, 1.0, 0.5, 0.5, 0.5, 0.5)

def chebyshev_table(basis_steps):
    number = 2 * basis_steps + 1
    matrix = np.zeros((number, number), np.float32)
    for offset, length in ((0, basis_steps + 1), (basis_steps + 1, basis_steps)):
        for column in range(length - 1):
            matrix[offset + column, offset + column] = 1.0
            if column == 0:
                matrix[offset + 1, offset] = 1.0
            else:
                matrix[offset + column + 1, offset + column] = 0.5
                matrix[offset + column - 1, offset + column] = 0.5
    return matrix

def coordinates(gram_matrix, basis_steps):
    number = 2 * basis_steps + 1
    shift_matrix = jnp.asarray(chebyshev_table(basis_steps))
    unit_rows = jnp.eye(number, dtype=jnp.float32)
    solution_coords = jnp.zeros((number,), jnp.float32)
    direction_coords = unit_rows[0]
    residual_coords = unit_rows[basis_steps + 1]
    norm_now = jnp.dot(residual_coords, jnp.dot(gram_matrix, residual_coords, precision=PRECISE), precision=PRECISE)
    for inner_step in range(basis_steps):
        mapped = jnp.dot(shift_matrix, direction_coords, precision=PRECISE)
        curvature = jnp.dot(direction_coords, jnp.dot(gram_matrix, mapped, precision=PRECISE), precision=PRECISE)
        step_length = norm_now / curvature
        solution_coords = solution_coords + step_length * direction_coords
        residual_coords = residual_coords - step_length * mapped
        norm_next = jnp.dot(residual_coords, jnp.dot(gram_matrix, residual_coords, precision=PRECISE), precision=PRECISE)
        direction_coords = residual_coords + norm_next / norm_now * direction_coords
        norm_now = norm_next
    return (solution_coords, residual_coords, direction_coords)

def pad_ghosts(source, fold_map):
    fold_row = jnp.take(source[-1], fold_map)
    zeros_row = jnp.zeros((1, source.shape[1]), source.dtype)
    stacked = jnp.concatenate([zeros_row, source, fold_row[None, :]], axis=0)
    return jnp.concatenate([stacked[:, -1:], stacked, stacked[:, :1]], axis=1)

def neighbour(padded, north_step, east_step):
    row_total = padded.shape[0] - 2
    column_total = padded.shape[1] - 2
    return padded[1 + north_step:1 + north_step + row_total, 1 + east_step:1 + east_step + column_total]

def reference(forcing, search_direction, ocean_depth, land_mask, fold_map):
    ocean_flag = land_mask.astype(jnp.float32)
    column_depth = ocean_depth * ocean_flag
    padded_depth = pad_ghosts(column_depth, fold_map)
    padded_wet = (padded_depth > 0.0).astype(jnp.float32)
    centre_wet = padded_wet[1:-1, 1:-1]
    weight_list = []
    link_sum = jnp.zeros_like(column_depth)
    for direction_index in range(8):
        north_step, east_step = DIRECTIONS[direction_index]
        weight = LINK_FACTORS[direction_index] * 0.5 * (column_depth + neighbour(padded_depth, north_step, east_step)) * centre_wet * neighbour(padded_wet, north_step, east_step)
        weight_list.append(weight)
        link_sum = link_sum + weight
    diagonal = centre_wet * (column_depth / (REACH * REACH) + link_sum) + (1.0 - centre_wet)
    inverse_root = lax.rsqrt(diagonal)

    def operate(source):
        padded = pad_ghosts(inverse_root * source, fold_map)
        running = jnp.zeros_like(source)
        for direction_index in range(8):
            north_step, east_step = DIRECTIONS[direction_index]
            running = running + weight_list[direction_index] * neighbour(padded, north_step, east_step)
        return -inverse_root * running
    operate_many = jax.vmap(operate)
    scaled_height = jnp.zeros_like(forcing)
    residual = ocean_flag * forcing
    direction = ocean_flag * search_direction
    for outer_step in range(OUTER):
        earlier = jnp.stack([direction, residual])
        current = operate_many(earlier)
        stored = [earlier, current]
        for power in range(1, STEPS):
            if power == STEPS - 1:
                earlier = earlier[:1]
                current = current[:1]
            upcoming = 2.0 * operate_many(current) - earlier
            earlier = current
            current = upcoming
            stored.append(current)
        krylov_basis = jnp.stack([member[0] for member in stored] + [member[1] for member in stored[:STEPS]])
        flattened = krylov_basis.reshape(krylov_basis.shape[0], -1)
        gram_matrix = jnp.dot(flattened, flattened.T, precision=PRECISE)
        solution_coords, residual_coords, direction_coords = coordinates(gram_matrix, STEPS)
        scaled_height = scaled_height + jnp.einsum('k,kij->ij', solution_coords, krylov_basis, precision=PRECISE)
        residual = jnp.einsum('k,kij->ij', residual_coords, krylov_basis, precision=PRECISE)
        direction = jnp.einsum('k,kij->ij', direction_coords, krylov_basis, precision=PRECISE)
    return (scaled_height, residual)
```

```python
import functools

import jax
import jax.numpy as jnp
from jax import lax
from jax.experimental import pallas as pl
from jax.experimental.pallas import tpu as pltpu
from jax.sharding import Mesh
from jax.sharding import PartitionSpec as P

STEPS = 8
REACH = 256
ROWS = 160
LANES = 128
EXT = ROWS + 32
EDGE = 9
BLK = 40
LON = ("lon_0", "lon_1")
VECTORS = 2 * STEPS + 1
F32 = jnp.float32


def lanes_of(rows):
    return lax.broadcasted_iota(jnp.int32, (rows, LANES), 1)


def shift_east(a, b, lane):
    ra, rb = pltpu.roll(a, 1, 1), pltpu.roll(b, 1, 1)
    first = lane == 0
    return jnp.where(first, rb, ra), jnp.where(first, ra, rb)


def shift_west(a, b, lane):
    ra, rb = pltpu.roll(a, LANES - 1, 1), pltpu.roll(b, LANES - 1, 1)
    last = lane == LANES - 1
    return jnp.where(last, rb, ra), jnp.where(last, ra, rb)


def pack_kernel(f_ref, p_ref, d_ref, m_ref, x_ref, east_ref, west_ref):
    for g in range(ROWS // 8):
        rows = pl.ds(8 * g, 8)
        flag = m_ref[rows, :].astype(F32)
        x_ref[0, rows, :] = d_ref[rows, :] * flag
        x_ref[1, rows, :] = f_ref[rows, :] * flag
        x_ref[2, rows, :] = p_ref[rows, :] * flag
    lane = lanes_of(8)
    for v in range(BLK // 8):
        east = jnp.zeros((8, LANES), F32)
        west = jnp.zeros((8, LANES), F32)
        for q in range(3):
            for blk in range(4):
                at = EDGE * (4 * q + blk)
                tile = x_ref[q, pl.ds(BLK * blk + 8 * v, 8), :]
                inside = (lane >= at) & (lane < at + EDGE)
                west = jnp.where(inside, pltpu.roll(tile, at, 1) if at else tile, west)
                east = jnp.where(inside, pltpu.roll(tile, (at + EDGE) % LANES, 1), east)
        east_ref[pl.ds(8 * v, 8), :] = east
        west_ref[pl.ds(8 * v, 8), :] = west
    for slot, (q, row) in enumerate(((0, ROWS - 8), (1, ROWS - 8), (2, ROWS - 8), (0, ROWS - 16))):
        tile = x_ref[q, pl.ds(row, 8), :]
        east_ref[pl.ds(BLK + 8 * slot, 8), :] = tile
        west_ref[pl.ds(BLK + 8 * slot, 8), :] = tile


def unpack_halo(from_west, from_east, q, blk, v, lane):
    at = EDGE * (4 * q + blk)
    right = from_east[pl.ds(8 * v, 8), :]
    left = from_west[pl.ds(8 * v, 8), :]
    right = pltpu.roll(right, LANES - at, 1) if at else right
    left = pltpu.roll(left, (2 * LANES - EDGE - at) % LANES, 1)
    return jnp.where(lane < EDGE, right, jnp.where(lane >= LANES - EDGE, left, 0.0))


def turn_kernel(r_ref, x_ref, fw_ref, fe_ref, north_ref, south_ref, fold_ref, next_ref, t1_ref, t2_ref):
    lane = lanes_of(8)
    top, low = ROWS // 8 - 1, 0
    for slot, (q, g) in enumerate(((0, top), (1, top), (2, top), (0, top - 1))):
        north_ref[pl.ds(8 * slot, 8), :] = x_ref[q, pl.ds(8 * g, 8), :]
        blk, v = 8 * g // BLK, (8 * g % BLK) // 8
        north_ref[pl.ds(32 + 8 * slot, 8), :] = unpack_halo(fw_ref, fe_ref, q, blk, v, lane)
    for slot, (q, g) in enumerate(((0, low), (1, low), (2, low), (0, low + 1))):
        south_ref[pl.ds(8 * slot, 8), :] = x_ref[q, pl.ds(8 * g, 8), :]
        blk, v = 8 * g // BLK, (8 * g % BLK) // 8
        south_ref[pl.ds(32 + 8 * slot, 8), :] = unpack_halo(fw_ref, fe_ref, q, blk, v, lane)
    reach = r_ref[0]
    along = reach - lane
    pick = along & (LANES - 1)
    place_a = along
    place_b = jnp.where(lane < EDGE, along - LANES, along + LANES)
    halo = (lane < EDGE) | (lane >= LANES - EDGE)
    for slot in range(4):
        rows = pl.ds(8 * slot, 8)
        own = jnp.take_along_axis(north_ref[rows, :], pick, axis=1, mode="promise_in_bounds")
        west = jnp.take_along_axis(fw_ref[pl.ds(BLK + 8 * slot, 8), :], pick, axis=1, mode="promise_in_bounds")
        east = jnp.take_along_axis(fe_ref[pl.ds(BLK + 8 * slot, 8), :], pick, axis=1, mode="promise_in_bounds")
        for part, place in ((0, place_a), (32, place_b)):
            near = jnp.where(place < 0, west, jnp.where(place < LANES, own, east))
            near = jnp.where(place < 2 * LANES, near, 0.0)
            far = jnp.where(place >= 2 * LANES, own, 0.0)
            if part:
                near = jnp.where(halo, near, 0.0)
                far = jnp.where(halo, far, 0.0)
            t1_ref[pl.ds(part + 8 * slot, 8), :] = near
            t2_ref[pl.ds(part + 8 * slot, 8), :] = far
    for g in range(8):
        for m in range(8):
            fold_ref[pl.ds(8 * g + m, 1), :] = t1_ref[pl.ds(8 * g + 7 - m, 1), :]
            next_ref[pl.ds(8 * g + m, 1), :] = t2_ref[pl.ds(8 * g + 7 - m, 1), :]


GROUPS = ROWS // 8 + 2


def basis_kernel(x_ref, fw_ref, fe_ref, fs_ref, fn_ref, ff_ref, basis_ref, sums_ref,
                 depth, side, inv, coef, acc):
    lane = lanes_of(8)
    zero = jnp.zeros((8, LANES), F32)
    targets = (
        lambda t: depth.at[t],
        lambda t: (basis_ref if t == 0 else side).at[STEPS + 1],
        lambda t: (basis_ref if t == 0 else side).at[0],
    )
    for q in range(3):
        own, rim = targets[q](0), targets[q](1)
        for g in range(ROWS // 8):
            own[pl.ds(16 + 8 * g, 8), :] = x_ref[q, pl.ds(8 * g, 8), :]
            blk, v = 8 * g // BLK, (8 * g % BLK) // 8
            rim[pl.ds(16 + 8 * g, 8), :] = unpack_halo(fw_ref, fe_ref, q, blk, v, lane)
        for t, ref in ((0, own), (1, rim)):
            at = 32 * t + 8 * q
            ref[pl.ds(8, 8), :] = fs_ref[pl.ds(at, 8), :]
            ref[pl.ds(EXT - 16, 8), :] = fn_ref[pl.ds(at, 8), :] + ff_ref[pl.ds(at, 8), :]
            if q == 0:
                at = 32 * t + 24
                ref[pl.ds(0, 8), :] = fs_ref[pl.ds(at, 8), :]
                ref[pl.ds(EXT - 8, 8), :] = fn_ref[pl.ds(at, 8), :] + ff_ref[pl.ds(at, 8), :]
            else:
                ref[pl.ds(0, 8), :] = zero
                ref[pl.ds(EXT - 8, 8), :] = zero
    for k in list(range(1, STEPS + 1)) + list(range(STEPS + 2, VECTORS)):
        for ref in (basis_ref, side):
            ref[k, pl.ds(0, 8), :] = zero
            ref[k, pl.ds(EXT - 8, 8), :] = zero
    for t in range(2):
        inv[t, pl.ds(0, 8), :] = zero
        inv[t, pl.ds(EXT - 8, 8), :] = zero

    def root_of(g, carry):
        at = 8 + 8 * g
        vert, mid, wet_mid, deep = [], [], [], []
        for t in range(2):
            down = depth[t, pl.ds(at - 1, 8), :]
            here = depth[t, pl.ds(at, 8), :]
            up = depth[t, pl.ds(at + 1, 8), :]
            wet = jnp.where(here > 0.0, 1.0, 0.0)
            wets = jnp.where(down > 0.0, 1.0, 0.0) + jnp.where(up > 0.0, 1.0, 0.0)
            vert.append((down + up, wets))
            mid.append((here + 0.5 * (down + up), wet + 0.5 * wets))
            deep.append(here)
            wet_mid.append(wet)
        sums = []
        for c in range(2):
            ea, eb = shift_east(mid[0][c], mid[1][c], lane)
            wa, wb = shift_west(mid[0][c], mid[1][c], lane)
            sums.append((vert[0][c] + (ea + wa), vert[1][c] + (eb + wb)))
        for t in range(2):
            links = 0.5 * (deep[t] * sums[1][t] + sums[0][t])
            diagonal = wet_mid[t] * (deep[t] / (REACH * REACH) + links) + (1.0 - wet_mid[t])
            inv[t, pl.ds(at, 8), :] = lax.rsqrt(diagonal) * wet_mid[t]
        return carry

    lax.fori_loop(0, GROUPS, root_of, 0, unroll=2)

    def coefs_of(g, carry):
        at = 8 + 8 * g
        d = [[depth[t, pl.ds(at + s, 8), :] for s in (-1, 0, 1)] for t in range(2)]
        r = [[inv[t, pl.ds(at + s, 8), :] for s in (-1, 0, 1)] for t in range(2)]
        de, re = shift_east(d[0][1], d[1][1], lane), shift_east(r[0][1], r[1][1], lane)
        dw, rw = shift_west(d[0][1], d[1][1], lane), shift_west(r[0][1], r[1][1], lane)
        for t in range(2):
            for base, (dc, rc) in enumerate(((d[t][1], r[t][1]), (de[t], re[t]), (dw[t], rw[t]))):
                for s in range(3):
                    if base == 0 and s == 1:
                        continue
                    whole = base == 0 or s == 1
                    c = (dc + d[t][s]) * (rc * r[t][s])
                    coef[t, 3 * base + s, pl.ds(at, 8), :] = c * (-1.0 if whole else -0.5)
        return carry

    lax.fori_loop(0, GROUPS, coefs_of, 0, unroll=2)

    def twice_applied(k, at, tiles, weights):
        parts = []
        for t in range(2):
            ref = basis_ref if t == 0 else side
            down, here, up = (ref[k, pl.ds(at + s, 8), :] for s in (-1, 0, 1))
            w = weights[t]
            straight = w[0] * down + w[2] * up
            toward_w = (w[3] * down + w[5] * up) + w[4] * here
            toward_e = (w[6] * down + w[8] * up) + w[7] * here
            parts.append((straight, toward_w, toward_e, here))
        wa, wb = shift_west(parts[0][1], parts[1][1], lane)
        ea, eb = shift_east(parts[0][2], parts[1][2], lane)
        return ((parts[0][0] + (wa + ea), parts[1][0] + (wb + eb))[:tiles], parts[0][3])

    def weights_at(at):
        return [[None if i == 1 else coef[t, i, pl.ds(at, 8), :] for i in range(9)] for t in range(2)]

    def step(k, first, last):
        total = [zero] * 6
        tiles = 1 if last else 2
        for g in range(1, GROUPS - 1) if last else range(GROUPS):
            at = 8 + 8 * g
            w = weights_at(at)
            now, new = [], []
            for base in ((0,) if last else (0, STEPS + 1)):
                out, here = twice_applied(base + k, at, tiles, w)
                now.append(here)
                for t in range(tiles):
                    ref = basis_ref if t == 0 else side
                    value = 0.5 * out[t] if first else out[t] - ref[base + k - 1, pl.ds(at, 8), :]
                    ref[base + k + 1, pl.ds(at, 8), :] = value
                    if t == 0:
                        new.append(value)
            if last:
                now.append(basis_ref[STEPS + 1 + k, pl.ds(at, 8), :])
            if 1 <= g <= ROWS // 8:
                p, r = now
                total[0] += p * p
                total[1] += p * new[0]
                total[2] += r * r
                total[3] += new[0] * new[0] if last else r * new[1]
                total[4] += p * r
                total[5] += new[0] * r
        for i in range(6):
            acc[k, i, :, :] = total[i]
        acc[k, 6, :, :] = zero
        acc[k, 7, :, :] = zero

    step(0, True, False)

    def middle(k, carry):
        step(k, False, False)
        return carry

    lax.fori_loop(1, STEPS - 1, middle, 0)
    step(STEPS - 1, False, True)

    flat = jnp.sum(acc[...].reshape(8 * STEPS, 8, LANES), axis=1)
    flat = jnp.concatenate([flat, jnp.zeros_like(flat)], axis=0)
    row = lax.dot_general(
        jnp.ones((8, LANES), F32), flat, (((1,), (1,)), ((), ())),
        precision=lax.Precision.HIGHEST, preferred_element_type=F32,
    )
    for g in range(sums_ref.shape[0] // 8):
        sums_ref[pl.ds(8 * g, 8), :] = row


def middle_kernel(in_ref, out_ref):
    out_ref[...] = jnp.broadcast_to(jnp.sum(in_ref[...], axis=0, keepdims=True), out_ref.shape)


def final_kernel(sum_ref, basis_ref, height_ref, residual_ref):
    held = jnp.broadcast_to(jnp.sum(sum_ref[...], axis=0, keepdims=True), (8, LANES))
    row = lax.broadcasted_iota(jnp.int32, (24, LANES), 0)
    col = lax.broadcasted_iota(jnp.int32, (24, LANES), 1)
    half = STEPS + 1
    i = jnp.where(row < half, row, row - half)
    j = jnp.where(col < half, col, col - half)
    row_p, col_p = row < half, col < half
    inside = (row < VECTORS) & (col < VECTORS)
    total, apart = i + j, jnp.abs(i - j)
    even = (total & 1) == 0
    slot = jnp.where(row_p & col_p, 0, jnp.where(row_p | col_p, 4, 2))
    slot = slot + jnp.where(even, 0, 1)

    def gathered(index):
        index = jnp.where(inside, index, 6)
        parts = [
            jnp.take_along_axis(held, index[8 * g : 8 * g + 8], axis=1, mode="promise_in_bounds")
            for g in range(3)
        ]
        return jnp.concatenate(parts, axis=0)

    high = jnp.where(total == 2 * STEPS, 8 * (STEPS - 1) + 3, 8 * (total >> 1) + slot)
    gram = gathered(high) + gathered(8 * (apart >> 1) + slot) - gathered(slot)

    lead_r = (row == 0) | (row == half)
    tail_r = (row == STEPS) | (row >= VECTORS - 1)
    same = (row_p == col_p) & inside & ~tail_r
    h_turned = jnp.where(same & (row == col), 1.0, 0.0)
    h_turned = h_turned + jnp.where(same & (col == row + 1), jnp.where(lead_r, 1.0, 0.5), 0.0)
    h_turned = h_turned + jnp.where(same & (col == row - 1) & ~lead_r, 0.5, 0.0)
    keep = jnp.where(tail_r, 0.0, 1.0)
    to_next = jnp.where(tail_r, 0.0, jnp.where(lead_r, 1.0, 0.5))
    to_last = jnp.where(tail_r | lead_r, 0.0, 0.5)

    def as_row(matrix, column):
        return jnp.sum(matrix * column, axis=0, keepdims=True)

    def dot(a, b):
        return jnp.sum(a * b, axis=1, keepdims=True)

    xc = jnp.zeros((24, LANES), F32)
    pc, rc = jnp.where(row == 0, 1.0, 0.0), jnp.where(row == half, 1.0, 0.0)
    pr, rr_row = jnp.where(col[:1] == 0, 1.0, 0.0), jnp.where(col[:1] == half, 1.0, 0.0)
    norm = dot(as_row(gram, rc), rr_row)
    for _ in range(STEPS):
        q_row = as_row(h_turned, pc)
        q_col = keep * pc + pltpu.roll(to_next * pc, 1, 0) + pltpu.roll(to_last * pc, 23, 0)
        t = norm / dot(as_row(gram, pc), q_row)
        xc = xc + t * pc
        rc = rc - t * q_col
        rr_row = rr_row - t * q_row
        new = dot(as_row(gram, rc), rr_row)
        ratio = new / norm
        pc = rc + ratio * pc
        norm = new
    xs = [jnp.broadcast_to(xc[k : k + 1, :], (8, LANES)) for k in range(VECTORS)]
    rs = [jnp.broadcast_to(rc[k : k + 1, :], (8, LANES)) for k in range(VECTORS)]
    for g in range(ROWS // 8):
        first = second = None
        for k in range(VECTORS):
            tile = basis_ref[k, pl.ds(16 + 8 * g, 8), :]
            first = xs[k] * tile if first is None else first + xs[k] * tile
            second = rs[k] * tile if second is None else second + rs[k] * tile
        height_ref[pl.ds(8 * g, 8), :] = first
        residual_ref[pl.ds(8 * g, 8), :] = second


def shape(*dims):
    return jax.ShapeDtypeStruct(dims, F32)


def per_device(forcing, search_direction, ocean_depth, land_mask, fold_map):
    lat_count, lon_count = lax.axis_size("lat"), lax.axis_size(LON)
    call = functools.partial(pl.pallas_call, compiler_params=pltpu.CompilerParams())
    fields, to_east, to_west = call(
        pack_kernel, name="pack",
        out_shape=(shape(3, ROWS, LANES), shape(BLK + 32, LANES), shape(BLK + 32, LANES)),
    )(forcing, search_direction, ocean_depth, land_mask)
    up = [(i, (i + 1) % lon_count) for i in range(lon_count)]
    from_west = lax.ppermute(to_east, LON, up)
    from_east = lax.ppermute(to_west, LON, [(b, a) for a, b in up])

    pivot = fold_map[0]
    offset = (pivot - 8) % (2 * LANES)
    reach = offset + 8
    pairing = ((pivot - reach) // (2 * LANES)) % (lon_count // 2)
    split = (reach + EDGE >= 2 * LANES).astype(jnp.int32)
    to_north, to_south, across, across_next = call(
        turn_kernel, name="turn",
        in_specs=[pl.BlockSpec(memory_space=pltpu.SMEM)] + [pl.BlockSpec(memory_space=pltpu.VMEM)] * 3,
        out_shape=(shape(64, LANES),) * 4,
        scratch_shapes=[pltpu.VMEM((64, LANES), F32)] * 2,
    )(reach.reshape(1), fields, from_west, from_east)

    from_south = lax.ppermute(to_north, "lat", [(i, i + 1) for i in range(lat_count - 1)])
    from_north = lax.ppermute(to_south, "lat", [(i + 1, i) for i in range(lat_count - 1)])
    top = (lat_count - 1) * lon_count

    def over_fold(value, pairing):
        pairs = [(top + i, top + (2 * pairing - i) % lon_count) for i in range(lon_count)]
        return lax.ppermute(value, ("lat",) + LON, pairs)

    def branch(index):
        if index % 2 == 0:
            return lambda near, far: over_fold(near, index // 2)
        return lambda near, far: over_fold(near, index // 2) + over_fold(far, index // 2 + 1)

    folded = lax.switch(2 * pairing + split, [branch(i) for i in range(lon_count)], across, across_next)

    basis, sums = call(
        basis_kernel, name="basis",
        out_shape=(shape(VECTORS, EXT, LANES), shape(lon_count, LANES)),
        scratch_shapes=[
            pltpu.VMEM((2, EXT, LANES), F32),
            pltpu.VMEM((VECTORS, EXT, LANES), F32),
            pltpu.VMEM((2, EXT, LANES), F32),
            pltpu.VMEM((2, 9, EXT, LANES), F32),
            pltpu.VMEM((STEPS, 8, 8, LANES), F32),
        ],
    )(fields, from_west, from_east, from_south, from_north, folded)
    sums = lax.all_to_all(sums, LON, split_axis=0, concat_axis=0, tiled=True)
    sums = call(middle_kernel, name="middle", out_shape=shape(lat_count, LANES))(sums)
    sums = lax.all_to_all(sums, "lat", split_axis=0, concat_axis=0, tiled=True)
    return call(
        final_kernel, name="final", out_shape=(shape(ROWS, LANES), shape(ROWS, LANES)),
    )(sums, basis)


def solution(mesh):
    lon = mesh.shape["lon"]
    split = Mesh(mesh.devices.reshape(mesh.shape["lat"], lon // 4, 4), ("lat", "lon_0", "lon_1"))
    return jax.shard_map(
        per_device,
        mesh=split,
        in_specs=(P("lat", LON), P("lat", LON), P("lat", LON), P("lat", LON), P()),
        out_specs=(P("lat", LON), P("lat", LON)),
        check_vma=False,
    )
```

```python
import functools

import jax
import jax.numpy as jnp
from jax import lax
from jax.experimental import pallas as pl
from jax.experimental.pallas import tpu as pltpu
from jax.sharding import Mesh
from jax.sharding import PartitionSpec as P

STEPS = 8
REACH = 256
ROWS = 160
LANES = 128
EXT = ROWS + 32
EDGE = 9
BLK = 40
LON = ("lon_0", "lon_1")
VECTORS = 2 * STEPS + 1
F32 = jnp.float32


def lanes_of(rows):
    return lax.broadcasted_iota(jnp.int32, (rows, LANES), 1)


def shift_east(a, b, lane):
    ra, rb = pltpu.roll(a, 1, 1), pltpu.roll(b, 1, 1)
    first = lane == 0
    return jnp.where(first, rb, ra), jnp.where(first, ra, rb)


def shift_west(a, b, lane):
    ra, rb = pltpu.roll(a, LANES - 1, 1), pltpu.roll(b, LANES - 1, 1)
    last = lane == LANES - 1
    return jnp.where(last, rb, ra), jnp.where(last, ra, rb)


def pack_kernel(pairs, f_hbm, p_hbm, d_hbm, m_hbm, map_hbm, x_ref, east_ref, west_ref, reach_ref, choice_ref,
                f_ref, p_ref, d_ref, m_ref, pivot, sems):
    copies = [
        pltpu.make_async_copy(source, target, sems.at[i])
        for i, (source, target) in enumerate((
            (m_hbm, m_ref), (d_hbm, d_ref), (f_hbm, f_ref), (p_hbm, p_ref), (map_hbm.at[pl.ds(0, LANES)], pivot),
        ))
    ]
    for copy in copies:
        copy.start()
    for copy in copies:
        copy.wait()
    for g in range(ROWS // 8):
        rows = pl.ds(8 * g, 8)
        flag = m_ref[rows, :].astype(F32)
        x_ref[0, rows, :] = d_ref[rows, :] * flag
        x_ref[1, rows, :] = f_ref[rows, :] * flag
        x_ref[2, rows, :] = p_ref[rows, :] * flag
    lane = lanes_of(8)
    for v in range(BLK // 8):
        east = jnp.zeros((8, LANES), F32)
        west = jnp.zeros((8, LANES), F32)
        for q in range(3):
            for blk in range(4):
                at = EDGE * (4 * q + blk)
                tile = x_ref[q, pl.ds(BLK * blk + 8 * v, 8), :]
                inside = (lane >= at) & (lane < at + EDGE)
                west = jnp.where(inside, pltpu.roll(tile, at, 1) if at else tile, west)
                east = jnp.where(inside, pltpu.roll(tile, (at + EDGE) % LANES, 1), east)
        east_ref[pl.ds(8 * v, 8), :] = east
        west_ref[pl.ds(8 * v, 8), :] = west
    for slot, (q, row) in enumerate(((0, ROWS - 8), (1, ROWS - 8), (2, ROWS - 8), (0, ROWS - 16))):
        tile = x_ref[q, pl.ds(row, 8), :]
        east_ref[pl.ds(BLK + 8 * slot, 8), :] = tile
        west_ref[pl.ds(BLK + 8 * slot, 8), :] = tile
    past = pivot[0] + (2 * pairs * LANES - 8)
    reach = past % (2 * LANES) + 8
    reach_ref[0] = reach
    split = jnp.where(reach + EDGE >= 2 * LANES, 1, 0)
    choice_ref[0] = 2 * ((past // (2 * LANES)) % pairs) + split


def unpack_halo(from_west, from_east, q, blk, v, lane):
    at = EDGE * (4 * q + blk)
    right = from_east[pl.ds(8 * v, 8), :]
    left = from_west[pl.ds(8 * v, 8), :]
    right = pltpu.roll(right, LANES - at, 1) if at else right
    left = pltpu.roll(left, (2 * LANES - EDGE - at) % LANES, 1)
    return jnp.where(lane < EDGE, right, jnp.where(lane >= LANES - EDGE, left, 0.0))


def turn_kernel(r_ref, x_ref, fw_ref, fe_ref, north_ref, south_ref, fold_ref, next_ref, t1_ref, t2_ref):
    lane = lanes_of(8)
    top, low = ROWS // 8 - 1, 0
    for slot, (q, g) in enumerate(((0, top), (1, top), (2, top), (0, top - 1))):
        north_ref[pl.ds(8 * slot, 8), :] = x_ref[q, pl.ds(8 * g, 8), :]
        blk, v = 8 * g // BLK, (8 * g % BLK) // 8
        north_ref[pl.ds(32 + 8 * slot, 8), :] = unpack_halo(fw_ref, fe_ref, q, blk, v, lane)
    for slot, (q, g) in enumerate(((0, low), (1, low), (2, low), (0, low + 1))):
        south_ref[pl.ds(8 * slot, 8), :] = x_ref[q, pl.ds(8 * g, 8), :]
        blk, v = 8 * g // BLK, (8 * g % BLK) // 8
        south_ref[pl.ds(32 + 8 * slot, 8), :] = unpack_halo(fw_ref, fe_ref, q, blk, v, lane)
    reach = r_ref[0]
    along = reach - lane
    pick = along & (LANES - 1)
    place_a = along
    place_b = jnp.where(lane < EDGE, along - LANES, along + LANES)
    halo = (lane < EDGE) | (lane >= LANES - EDGE)
    for slot in range(4):
        rows = pl.ds(8 * slot, 8)
        own = jnp.take_along_axis(north_ref[rows, :], pick, axis=1, mode="promise_in_bounds")
        west = jnp.take_along_axis(fw_ref[pl.ds(BLK + 8 * slot, 8), :], pick, axis=1, mode="promise_in_bounds")
        east = jnp.take_along_axis(fe_ref[pl.ds(BLK + 8 * slot, 8), :], pick, axis=1, mode="promise_in_bounds")
        for part, place in ((0, place_a), (32, place_b)):
            near = jnp.where(place < 0, west, jnp.where(place < LANES, own, east))
            near = jnp.where(place < 2 * LANES, near, 0.0)
            far = jnp.where(place >= 2 * LANES, own, 0.0)
            if part:
                near = jnp.where(halo, near, 0.0)
                far = jnp.where(halo, far, 0.0)
            t1_ref[pl.ds(part + 8 * slot, 8), :] = near
            t2_ref[pl.ds(part + 8 * slot, 8), :] = far
    for g in range(8):
        for m in range(8):
            fold_ref[pl.ds(8 * g + m, 1), :] = t1_ref[pl.ds(8 * g + 7 - m, 1), :]
            next_ref[pl.ds(8 * g + m, 1), :] = t2_ref[pl.ds(8 * g + 7 - m, 1), :]


GROUPS = ROWS // 8 + 2


def basis_kernel(x_ref, fw_ref, fe_ref, fs_hbm, fn_hbm, ff_hbm, basis_ref, sums_ref,
                 depth, side, inv, coef, acc, fs_ref, fn_ref, ff_ref, sems):
    copies = [
        pltpu.make_async_copy(source, target, sems.at[i])
        for i, (source, target) in enumerate(((fs_hbm, fs_ref), (fn_hbm, fn_ref), (ff_hbm, ff_ref)))
    ]
    for copy in copies:
        copy.start()
    lane = lanes_of(8)
    zero = jnp.zeros((8, LANES), F32)
    targets = (
        lambda t: depth.at[t],
        lambda t: (basis_ref if t == 0 else side).at[STEPS + 1],
        lambda t: (basis_ref if t == 0 else side).at[0],
    )
    for q in range(3):
        own, rim = targets[q](0), targets[q](1)
        for g in range(ROWS // 8):
            own[pl.ds(16 + 8 * g, 8), :] = x_ref[q, pl.ds(8 * g, 8), :]
            blk, v = 8 * g // BLK, (8 * g % BLK) // 8
            rim[pl.ds(16 + 8 * g, 8), :] = unpack_halo(fw_ref, fe_ref, q, blk, v, lane)
    for copy in copies:
        copy.wait()
    for q in range(3):
        own, rim = targets[q](0), targets[q](1)
        for t, ref in ((0, own), (1, rim)):
            at = 32 * t + 8 * q
            ref[pl.ds(8, 8), :] = fs_ref[pl.ds(at, 8), :]
            ref[pl.ds(EXT - 16, 8), :] = fn_ref[pl.ds(at, 8), :] + ff_ref[pl.ds(at, 8), :]
            if q == 0:
                at = 32 * t + 24
                ref[pl.ds(0, 8), :] = fs_ref[pl.ds(at, 8), :]
                ref[pl.ds(EXT - 8, 8), :] = fn_ref[pl.ds(at, 8), :] + ff_ref[pl.ds(at, 8), :]
            else:
                ref[pl.ds(0, 8), :] = zero
                ref[pl.ds(EXT - 8, 8), :] = zero
    for k in list(range(1, STEPS + 1)) + list(range(STEPS + 2, VECTORS)):
        for ref in (basis_ref, side):
            ref[k, pl.ds(0, 8), :] = zero
            ref[k, pl.ds(EXT - 8, 8), :] = zero
    for t in range(2):
        inv[t, pl.ds(0, 8), :] = zero
        inv[t, pl.ds(EXT - 8, 8), :] = zero

    def root_of(g, carry):
        at = 8 + 8 * g
        vert, mid, wet_mid, deep = [], [], [], []
        for t in range(2):
            down = depth[t, pl.ds(at - 1, 8), :]
            here = depth[t, pl.ds(at, 8), :]
            up = depth[t, pl.ds(at + 1, 8), :]
            wet = jnp.where(here > 0.0, 1.0, 0.0)
            wets = jnp.where(down > 0.0, 1.0, 0.0) + jnp.where(up > 0.0, 1.0, 0.0)
            vert.append((down + up, wets))
            mid.append((here + 0.5 * (down + up), wet + 0.5 * wets))
            deep.append(here)
            wet_mid.append(wet)
        sums = []
        for c in range(2):
            ea, eb = shift_east(mid[0][c], mid[1][c], lane)
            wa, wb = shift_west(mid[0][c], mid[1][c], lane)
            sums.append((vert[0][c] + (ea + wa), vert[1][c] + (eb + wb)))
        for t in range(2):
            links = 0.5 * (deep[t] * sums[1][t] + sums[0][t])
            diagonal = wet_mid[t] * (deep[t] / (REACH * REACH) + links) + (1.0 - wet_mid[t])
            inv[t, pl.ds(at, 8), :] = lax.rsqrt(diagonal) * wet_mid[t]
        return carry

    lax.fori_loop(0, GROUPS, root_of, 0, unroll=2)

    def coefs_of(g, carry):
        at = 8 + 8 * g
        d = [[depth[t, pl.ds(at + s, 8), :] for s in (-1, 0, 1)] for t in range(2)]
        r = [[inv[t, pl.ds(at + s, 8), :] for s in (-1, 0, 1)] for t in range(2)]
        de, re = shift_east(d[0][1], d[1][1], lane), shift_east(r[0][1], r[1][1], lane)
        dw, rw = shift_west(d[0][1], d[1][1], lane), shift_west(r[0][1], r[1][1], lane)
        for t in range(2):
            for base, (dc, rc) in enumerate(((d[t][1], r[t][1]), (de[t], re[t]), (dw[t], rw[t]))):
                for s in range(3):
                    if base == 0 and s == 1:
                        continue
                    whole = base == 0 or s == 1
                    c = (dc + d[t][s]) * (rc * r[t][s])
                    coef[t, 3 * base + s, pl.ds(at, 8), :] = c * (-1.0 if whole else -0.5)
        return carry

    lax.fori_loop(0, GROUPS, coefs_of, 0, unroll=2)

    def twice_applied(k, at, tiles, weights):
        parts = []
        for t in range(2):
            ref = basis_ref if t == 0 else side
            down, here, up = (ref[k, pl.ds(at + s, 8), :] for s in (-1, 0, 1))
            w = weights[t]
            straight = w[0] * down + w[2] * up
            toward_w = (w[3] * down + w[5] * up) + w[4] * here
            toward_e = (w[6] * down + w[8] * up) + w[7] * here
            parts.append((straight, toward_w, toward_e, here))
        wa, wb = shift_west(parts[0][1], parts[1][1], lane)
        ea, eb = shift_east(parts[0][2], parts[1][2], lane)
        return ((parts[0][0] + (wa + ea), parts[1][0] + (wb + eb))[:tiles], parts[0][3])

    def weights_at(at):
        return [[None if i == 1 else coef[t, i, pl.ds(at, 8), :] for i in range(9)] for t in range(2)]

    def step(k, first, last):
        total = [zero] * 6
        tiles = 1 if last else 2
        for g in range(1, GROUPS - 1) if last else range(GROUPS):
            at = 8 + 8 * g
            w = weights_at(at)
            now, new = [], []
            for base in ((0,) if last else (0, STEPS + 1)):
                out, here = twice_applied(base + k, at, tiles, w)
                now.append(here)
                for t in range(tiles):
                    ref = basis_ref if t == 0 else side
                    value = 0.5 * out[t] if first else out[t] - ref[base + k - 1, pl.ds(at, 8), :]
                    ref[base + k + 1, pl.ds(at, 8), :] = value
                    if t == 0:
                        new.append(value)
            if last:
                now.append(basis_ref[STEPS + 1 + k, pl.ds(at, 8), :])
            if 1 <= g <= ROWS // 8:
                p, r = now
                total[0] += p * p
                total[1] += p * new[0]
                total[2] += r * r
                total[3] += new[0] * new[0] if last else r * new[1]
                total[4] += p * r
                total[5] += new[0] * r
        for i in range(6):
            acc[k, i, :, :] = total[i]
        acc[k, 6, :, :] = zero
        acc[k, 7, :, :] = zero

    step(0, True, False)

    def middle(k, carry):
        step(k, False, False)
        return carry

    lax.fori_loop(1, STEPS - 1, middle, 0)
    step(STEPS - 1, False, True)

    flat = jnp.sum(acc[...].reshape(8 * STEPS, 8, LANES), axis=1)
    flat = jnp.concatenate([flat, jnp.zeros_like(flat)], axis=0)
    row = lax.dot_general(
        jnp.ones((8, LANES), F32), flat, (((1,), (1,)), ((), ())),
        precision=lax.Precision.HIGHEST, preferred_element_type=F32,
    )
    for g in range(sums_ref.shape[0] // 8):
        sums_ref[pl.ds(8 * g, 8), :] = row


def middle_kernel(in_ref, out_ref):
    out_ref[...] = jnp.broadcast_to(jnp.sum(in_ref[...], axis=0, keepdims=True), out_ref.shape)


def final_kernel(sum_ref, basis_ref, height_ref, residual_ref):
    products = jnp.broadcast_to(jnp.sum(sum_ref[...], axis=0, keepdims=True), (8, LANES))
    row = lax.broadcasted_iota(jnp.int32, (24, LANES), 0)
    col = lax.broadcasted_iota(jnp.int32, (24, LANES), 1)
    half = STEPS + 1
    i = jnp.where(row < half, row, row - half)
    j = jnp.where(col < half, col, col - half)
    row_p, col_p = row < half, col < half
    inside = (row < VECTORS) & (col < VECTORS)
    total, apart = i + j, jnp.abs(i - j)
    even = (total & 1) == 0
    slot = jnp.where(row_p & col_p, 0, jnp.where(row_p | col_p, 4, 2))
    slot = slot + jnp.where(even, 0, 1)

    def gathered(index):
        index = jnp.where(inside, index, 6)
        parts = [
            jnp.take_along_axis(products, index[8 * g : 8 * g + 8], axis=1, mode="promise_in_bounds")
            for g in range(3)
        ]
        return jnp.concatenate(parts, axis=0)

    high = jnp.where(total == 2 * STEPS, 8 * (STEPS - 1) + 3, 8 * (total >> 1) + slot)
    gram = gathered(high) + gathered(8 * (apart >> 1) + slot) - gathered(slot)

    lead_r = (row == 0) | (row == half)
    tail_r = (row == STEPS) | (row >= VECTORS - 1)
    same = (row_p == col_p) & inside & ~tail_r
    h_turned = jnp.where(same & (row == col), 1.0, 0.0)
    h_turned = h_turned + jnp.where(same & (col == row + 1), jnp.where(lead_r, 1.0, 0.5), 0.0)
    h_turned = h_turned + jnp.where(same & (col == row - 1) & ~lead_r, 0.5, 0.0)
    keep = jnp.where(tail_r, 0.0, 1.0)
    to_next = jnp.where(tail_r, 0.0, jnp.where(lead_r, 1.0, 0.5))
    to_last = jnp.where(tail_r | lead_r, 0.0, 0.5)

    def as_row(matrix, column):
        return jnp.sum(matrix * column, axis=0, keepdims=True)

    def dot(a, b):
        return jnp.sum(a * b, axis=1, keepdims=True)

    xc = jnp.zeros((24, LANES), F32)
    pc, rc = jnp.where(row == 0, 1.0, 0.0), jnp.where(row == half, 1.0, 0.0)
    pr, rr_row = jnp.where(col[:1] == 0, 1.0, 0.0), jnp.where(col[:1] == half, 1.0, 0.0)
    norm = dot(as_row(gram, rc), rr_row)
    for _ in range(STEPS):
        q_row = as_row(h_turned, pc)
        q_col = keep * pc + pltpu.roll(to_next * pc, 1, 0) + pltpu.roll(to_last * pc, 23, 0)
        t = norm / dot(as_row(gram, pc), q_row)
        xc = xc + t * pc
        rc = rc - t * q_col
        rr_row = rr_row - t * q_row
        new = dot(as_row(gram, rc), rr_row)
        ratio = new / norm
        pc = rc + ratio * pc
        norm = new
    xs = [jnp.broadcast_to(xc[k : k + 1, :], (8, LANES)) for k in range(VECTORS)]
    rs = [jnp.broadcast_to(rc[k : k + 1, :], (8, LANES)) for k in range(VECTORS)]
    for g in range(ROWS // 8):
        first = second = None
        for k in range(VECTORS):
            tile = basis_ref[k, pl.ds(16 + 8 * g, 8), :]
            first = xs[k] * tile if first is None else first + xs[k] * tile
            second = rs[k] * tile if second is None else second + rs[k] * tile
        height_ref[pl.ds(8 * g, 8), :] = first
        residual_ref[pl.ds(8 * g, 8), :] = second


def shape(*dims):
    return pltpu.VMEM(dims, F32)


def held(*values, space=pltpu.VMEM):
    return tuple(pltpu.with_memory_space_constraint(v, space) for v in values)


def limit(mib):
    return pltpu.CompilerParams(vmem_limit_bytes=mib << 20)


def per_device(forcing, search_direction, ocean_depth, land_mask, fold_map):
    lat_count, lon_count = lax.axis_size("lat"), lax.axis_size(LON)
    call = pl.pallas_call
    fields, to_east, to_west, reach, choice = call(
        functools.partial(pack_kernel, lon_count // 2), name="pack",
        in_specs=[pl.BlockSpec(memory_space=pl.ANY)] * 5,
        out_specs=[pl.BlockSpec(memory_space=pltpu.VMEM)] * 3 + [pl.BlockSpec(memory_space=pltpu.SMEM)] * 2,
        out_shape=(shape(3, ROWS, LANES), shape(BLK + 32, LANES), shape(BLK + 32, LANES),
                   pltpu.SMEM((1,), jnp.int32), pltpu.SMEM((1,), jnp.int32)),
        scratch_shapes=[pltpu.VMEM((ROWS, LANES), F32)] * 3 + [
            pltpu.VMEM((ROWS, LANES), jnp.int32), pltpu.SMEM((LANES,), jnp.int32), pltpu.SemaphoreType.DMA((5,)),
        ],
        compiler_params=limit(4),
    )(*held(forcing, search_direction, ocean_depth, land_mask, fold_map, space=pltpu.HBM))
    up = [(i, (i + 1) % lon_count) for i in range(lon_count)]
    from_west = lax.ppermute(to_east, LON, up)
    from_east = lax.ppermute(to_west, LON, [(b, a) for a, b in up])

    to_north, to_south, across, across_next = call(
        turn_kernel, name="turn",
        in_specs=[pl.BlockSpec(memory_space=pltpu.SMEM)] + [pl.BlockSpec(memory_space=pltpu.VMEM)] * 3,
        out_shape=(shape(64, LANES),) * 4,
        scratch_shapes=[pltpu.VMEM((64, LANES), F32)] * 2,
        compiler_params=limit(4),
    )(reach, *held(fields, from_west, from_east))

    top = (lat_count - 1) * lon_count

    def over_fold(value, pairing):
        pairs = [(top + i, top + (2 * pairing - i) % lon_count) for i in range(lon_count)]
        return lax.ppermute(value, ("lat",) + LON, pairs)

    def branch(index):
        def exchange(near, far, to_north, to_south):
            folded = over_fold(near, index // 2)
            if index % 2:
                folded = folded + over_fold(far, index // 2 + 1)
            from_south = lax.ppermute(to_north, "lat", [(i, i + 1) for i in range(lat_count - 1)])
            from_north = lax.ppermute(to_south, "lat", [(i + 1, i) for i in range(lat_count - 1)])
            return folded, from_south, from_north

        return exchange

    folded, from_south, from_north = lax.switch(
        choice[0], [branch(i) for i in range(lon_count)], across, across_next, to_north, to_south
    )

    basis, sums = call(
        basis_kernel, name="basis",
        out_shape=(shape(VECTORS, EXT, LANES), shape(lon_count, LANES)),
        scratch_shapes=[
            pltpu.VMEM((2, EXT, LANES), F32),
            pltpu.VMEM((VECTORS, EXT, LANES), F32),
            pltpu.VMEM((2, EXT, LANES), F32),
            pltpu.VMEM((2, 9, EXT, LANES), F32),
            pltpu.VMEM((STEPS, 8, 8, LANES), F32),
        ] + [pltpu.VMEM((64, LANES), F32)] * 3 + [pltpu.SemaphoreType.DMA((3,))],
        in_specs=[pl.BlockSpec(memory_space=pltpu.VMEM)] * 3 + [pl.BlockSpec(memory_space=pl.ANY)] * 3,
        compiler_params=limit(12),
    )(*held(fields, from_west, from_east), *held(from_south, from_north, folded, space=pltpu.HBM))
    sums = lax.all_to_all(sums, LON, split_axis=0, concat_axis=0, tiled=True)
    sums = call(middle_kernel, name="middle", out_shape=shape(lat_count, LANES), compiler_params=limit(2))(*held(sums))
    sums = lax.all_to_all(sums, "lat", split_axis=0, concat_axis=0, tiled=True)
    return call(
        final_kernel, name="final", out_shape=(jax.ShapeDtypeStruct((ROWS, LANES), F32),) * 2,
        compiler_params=limit(4),
    )(*held(sums, basis))


def solution(mesh):
    lon = mesh.shape["lon"]
    split = Mesh(mesh.devices.reshape(mesh.shape["lat"], lon // 4, 4), ("lat", "lon_0", "lon_1"))
    return jax.shard_map(
        per_device,
        mesh=split,
        in_specs=(P("lat", LON), P("lat", LON), P("lat", LON), P("lat", LON), P()),
        out_specs=(P("lat", LON), P("lat", LON)),
        check_vma=False,
    )
```

```python
import functools

import jax
import jax.numpy as jnp
from jax import lax
from jax.experimental import pallas as pl
from jax.experimental.pallas import tpu as pltpu
from jax.sharding import Mesh
from jax.sharding import PartitionSpec as P

STEPS = 8
REACH = 256
ROWS = 160
LANES = 128
EXT = ROWS + 32
EDGE = 9
BLK = 40
LON = ("lon_0", "lon_1")
VECTORS = 2 * STEPS + 1
F32 = jnp.float32


def lanes_of(rows):
    return lax.broadcasted_iota(jnp.int32, (rows, LANES), 1)


def shift_east(a, b, lane):
    ra, rb = pltpu.roll(a, 1, 1), pltpu.roll(b, 1, 1)
    first = lane == 0
    return jnp.where(first, rb, ra), jnp.where(first, ra, rb)


def shift_west(a, b, lane):
    ra, rb = pltpu.roll(a, LANES - 1, 1), pltpu.roll(b, LANES - 1, 1)
    last = lane == LANES - 1
    return jnp.where(last, rb, ra), jnp.where(last, ra, rb)


def pack_kernel(pairs, f_hbm, p_hbm, d_hbm, m_hbm, map_hbm, x_ref, first_ref, second_ref, reach_ref, choice_ref,
                f_ref, p_ref, d_ref, m_ref, pivot, sems):
    even = lax.axis_index(LON) % 2 == 0
    copies = [
        pltpu.make_async_copy(source, target, sems.at[i])
        for i, (source, target) in enumerate((
            (m_hbm, m_ref), (d_hbm, d_ref), (f_hbm, f_ref), (p_hbm, p_ref), (map_hbm.at[pl.ds(0, LANES)], pivot),
        ))
    ]
    for copy in copies:
        copy.start()
    for copy in copies:
        copy.wait()
    for g in range(ROWS // 8):
        rows = pl.ds(8 * g, 8)
        flag = m_ref[rows, :].astype(F32)
        x_ref[0, rows, :] = d_ref[rows, :] * flag
        x_ref[1, rows, :] = f_ref[rows, :] * flag
        x_ref[2, rows, :] = p_ref[rows, :] * flag
    lane = lanes_of(8)
    for v in range(BLK // 8):
        east = jnp.zeros((8, LANES), F32)
        west = jnp.zeros((8, LANES), F32)
        for q in range(3):
            for blk in range(4):
                at = EDGE * (4 * q + blk)
                tile = x_ref[q, pl.ds(BLK * blk + 8 * v, 8), :]
                inside = (lane >= at) & (lane < at + EDGE)
                west = jnp.where(inside, pltpu.roll(tile, at, 1) if at else tile, west)
                east = jnp.where(inside, pltpu.roll(tile, (at + EDGE) % LANES, 1), east)
        first_ref[pl.ds(8 * v, 8), :] = jnp.where(even, east, west)
        second_ref[pl.ds(8 * v, 8), :] = jnp.where(even, west, east)
    for slot, (q, row) in enumerate(((0, ROWS - 8), (1, ROWS - 8), (2, ROWS - 8), (0, ROWS - 16))):
        tile = x_ref[q, pl.ds(row, 8), :]
        first_ref[pl.ds(BLK + 8 * slot, 8), :] = tile
        second_ref[pl.ds(BLK + 8 * slot, 8), :] = tile
    past = pivot[0] + (2 * pairs * LANES - 8)
    reach = past % (2 * LANES) + 8
    reach_ref[0] = reach
    split = jnp.where(reach + EDGE >= 2 * LANES, 1, 0)
    choice_ref[0] = 2 * ((past // (2 * LANES)) % pairs) + split


def unpack_halo(from_west, from_east, q, blk, v, lane):
    at = EDGE * (4 * q + blk)
    right = from_east[pl.ds(8 * v, 8), :]
    left = from_west[pl.ds(8 * v, 8), :]
    right = pltpu.roll(right, LANES - at, 1) if at else right
    left = pltpu.roll(left, (2 * LANES - EDGE - at) % LANES, 1)
    return jnp.where(lane < EDGE, right, jnp.where(lane >= LANES - EDGE, left, 0.0))


def sort_partners(axis, first, second, before, after):
    even = lax.axis_index(axis) % 2 == 0
    for g in range(first.shape[0] // 8):
        rows = pl.ds(8 * g, 8)
        a, b = first[rows, :], second[rows, :]
        before[rows, :] = jnp.where(even, b, a)
        after[rows, :] = jnp.where(even, a, b)


def turn_kernel(tops, r_ref, x_ref, first_ref, second_ref, one_ref, two_ref, next_ref,
                fw_ref, fe_ref, north_ref, south_ref, t1_ref, t2_ref):
    lane = lanes_of(8)
    lat = lax.axis_index("lat")
    even, top_row = lat % 2 == 0, lat == tops
    sort_partners(LON, first_ref, second_ref, fw_ref, fe_ref)
    top, low = ROWS // 8 - 1, 0
    for ref, rows in (
        (north_ref, ((0, top), (1, top), (2, top), (0, top - 1))),
        (south_ref, ((0, low), (1, low), (2, low), (0, low + 1))),
    ):
        for slot, (q, g) in enumerate(rows):
            ref[pl.ds(8 * slot, 8), :] = x_ref[q, pl.ds(8 * g, 8), :]
            blk, v = 8 * g // BLK, (8 * g % BLK) // 8
            ref[pl.ds(32 + 8 * slot, 8), :] = unpack_halo(fw_ref, fe_ref, q, blk, v, lane)
    for g in range(8):
        rows = pl.ds(8 * g, 8)
        north, south = north_ref[rows, :], south_ref[rows, :]
        one_ref[rows, :] = jnp.where(even, north, south)
        two_ref[rows, :] = jnp.where(even, south, north)
        next_ref[rows, :] = jnp.zeros((8, LANES), F32)

    @pl.when(top_row)
    def _():
        across_fold(r_ref[0], lane, north_ref, fw_ref, fe_ref, two_ref, next_ref, t1_ref, t2_ref)


def across_fold(reach, lane, north_ref, fw_ref, fe_ref, fold_ref, next_ref, t1_ref, t2_ref):
    along = reach - lane
    pick = along & (LANES - 1)
    place_a = along
    place_b = jnp.where(lane < EDGE, along - LANES, along + LANES)
    halo = (lane < EDGE) | (lane >= LANES - EDGE)
    for slot in range(4):
        rows = pl.ds(8 * slot, 8)
        own = jnp.take_along_axis(north_ref[rows, :], pick, axis=1, mode="promise_in_bounds")
        west = jnp.take_along_axis(fw_ref[pl.ds(BLK + 8 * slot, 8), :], pick, axis=1, mode="promise_in_bounds")
        east = jnp.take_along_axis(fe_ref[pl.ds(BLK + 8 * slot, 8), :], pick, axis=1, mode="promise_in_bounds")
        for part, place in ((0, place_a), (32, place_b)):
            near = jnp.where(place < 0, west, jnp.where(place < LANES, own, east))
            near = jnp.where(place < 2 * LANES, near, 0.0)
            far = jnp.where(place >= 2 * LANES, own, 0.0)
            if part:
                near = jnp.where(halo, near, 0.0)
                far = jnp.where(halo, far, 0.0)
            t1_ref[pl.ds(part + 8 * slot, 8), :] = near
            t2_ref[pl.ds(part + 8 * slot, 8), :] = far
    for g in range(8):
        for m in range(8):
            fold_ref[pl.ds(8 * g + m, 1), :] = t1_ref[pl.ds(8 * g + 7 - m, 1), :]
            next_ref[pl.ds(8 * g + m, 1), :] = t2_ref[pl.ds(8 * g + 7 - m, 1), :]


GROUPS = ROWS // 8 + 2


def basis_kernel(x_ref, first_ref, second_ref, one_ref, two_hbm, basis_ref, sums_ref,
                 depth, side, inv, coef, acc, fw_ref, fe_ref, fs_ref, fn_ref, two_ref, sem):
    copy = pltpu.make_async_copy(two_hbm, two_ref, sem)
    copy.start()
    sort_partners(LON, first_ref, second_ref, fw_ref, fe_ref)
    lane = lanes_of(8)
    zero = jnp.zeros((8, LANES), F32)
    targets = (
        lambda t: depth.at[t],
        lambda t: (basis_ref if t == 0 else side).at[STEPS + 1],
        lambda t: (basis_ref if t == 0 else side).at[0],
    )
    for q in range(3):
        own, rim = targets[q](0), targets[q](1)
        for g in range(ROWS // 8):
            own[pl.ds(16 + 8 * g, 8), :] = x_ref[q, pl.ds(8 * g, 8), :]
            blk, v = 8 * g // BLK, (8 * g % BLK) // 8
            rim[pl.ds(16 + 8 * g, 8), :] = unpack_halo(fw_ref, fe_ref, q, blk, v, lane)
    copy.wait()
    sort_partners("lat", one_ref, two_ref, fs_ref, fn_ref)
    for q in range(3):
        own, rim = targets[q](0), targets[q](1)
        for t, ref in ((0, own), (1, rim)):
            at = 32 * t + 8 * q
            ref[pl.ds(8, 8), :] = fs_ref[pl.ds(at, 8), :]
            ref[pl.ds(EXT - 16, 8), :] = fn_ref[pl.ds(at, 8), :]
            if q == 0:
                at = 32 * t + 24
                ref[pl.ds(0, 8), :] = fs_ref[pl.ds(at, 8), :]
                ref[pl.ds(EXT - 8, 8), :] = fn_ref[pl.ds(at, 8), :]
            else:
                ref[pl.ds(0, 8), :] = zero
                ref[pl.ds(EXT - 8, 8), :] = zero
    for k in list(range(1, STEPS + 1)) + list(range(STEPS + 2, VECTORS)):
        for ref in (basis_ref, side):
            ref[k, pl.ds(0, 8), :] = zero
            ref[k, pl.ds(EXT - 8, 8), :] = zero
    for t in range(2):
        inv[t, pl.ds(0, 8), :] = zero
        inv[t, pl.ds(EXT - 8, 8), :] = zero

    def root_of(g, carry):
        at = 8 + 8 * g
        vert, mid, wet_mid, deep = [], [], [], []
        for t in range(2):
            down = depth[t, pl.ds(at - 1, 8), :]
            here = depth[t, pl.ds(at, 8), :]
            up = depth[t, pl.ds(at + 1, 8), :]
            wet = jnp.where(here > 0.0, 1.0, 0.0)
            wets = jnp.where(down > 0.0, 1.0, 0.0) + jnp.where(up > 0.0, 1.0, 0.0)
            vert.append((down + up, wets))
            mid.append((here + 0.5 * (down + up), wet + 0.5 * wets))
            deep.append(here)
            wet_mid.append(wet)
        sums = []
        for c in range(2):
            ea, eb = shift_east(mid[0][c], mid[1][c], lane)
            wa, wb = shift_west(mid[0][c], mid[1][c], lane)
            sums.append((vert[0][c] + (ea + wa), vert[1][c] + (eb + wb)))
        for t in range(2):
            links = 0.5 * (deep[t] * sums[1][t] + sums[0][t])
            diagonal = wet_mid[t] * (deep[t] / (REACH * REACH) + links) + (1.0 - wet_mid[t])
            inv[t, pl.ds(at, 8), :] = lax.rsqrt(diagonal) * wet_mid[t]
        return carry

    lax.fori_loop(0, GROUPS, root_of, 0, unroll=2)

    def coefs_of(g, carry):
        at = 8 + 8 * g
        d = [[depth[t, pl.ds(at + s, 8), :] for s in (-1, 0, 1)] for t in range(2)]
        r = [[inv[t, pl.ds(at + s, 8), :] for s in (-1, 0, 1)] for t in range(2)]
        de, re = shift_east(d[0][1], d[1][1], lane), shift_east(r[0][1], r[1][1], lane)
        dw, rw = shift_west(d[0][1], d[1][1], lane), shift_west(r[0][1], r[1][1], lane)
        for t in range(2):
            for base, (dc, rc) in enumerate(((d[t][1], r[t][1]), (de[t], re[t]), (dw[t], rw[t]))):
                for s in range(3):
                    if base == 0 and s == 1:
                        continue
                    whole = base == 0 or s == 1
                    c = (dc + d[t][s]) * (rc * r[t][s])
                    coef[t, 3 * base + s, pl.ds(at, 8), :] = c * (-1.0 if whole else -0.5)
        return carry

    lax.fori_loop(0, GROUPS, coefs_of, 0, unroll=2)

    def twice_applied(k, at, tiles, weights):
        parts = []
        for t in range(2):
            ref = basis_ref if t == 0 else side
            down, here, up = (ref[k, pl.ds(at + s, 8), :] for s in (-1, 0, 1))
            w = weights[t]
            straight = w[0] * down + w[2] * up
            toward_w = (w[3] * down + w[5] * up) + w[4] * here
            toward_e = (w[6] * down + w[8] * up) + w[7] * here
            parts.append((straight, toward_w, toward_e, here))
        wa, wb = shift_west(parts[0][1], parts[1][1], lane)
        ea, eb = shift_east(parts[0][2], parts[1][2], lane)
        return ((parts[0][0] + (wa + ea), parts[1][0] + (wb + eb))[:tiles], parts[0][3])

    def weights_at(at):
        return [[None if i == 1 else coef[t, i, pl.ds(at, 8), :] for i in range(9)] for t in range(2)]

    def step(k, first, last):
        total = [zero] * 6
        tiles = 1 if last else 2
        for g in range(1, GROUPS - 1) if last else range(GROUPS):
            at = 8 + 8 * g
            w = weights_at(at)
            now, new = [], []
            for base in ((0,) if last else (0, STEPS + 1)):
                out, here = twice_applied(base + k, at, tiles, w)
                now.append(here)
                for t in range(tiles):
                    ref = basis_ref if t == 0 else side
                    value = 0.5 * out[t] if first else out[t] - ref[base + k - 1, pl.ds(at, 8), :]
                    ref[base + k + 1, pl.ds(at, 8), :] = value
                    if t == 0:
                        new.append(value)
            if last:
                now.append(basis_ref[STEPS + 1 + k, pl.ds(at, 8), :])
            if 1 <= g <= ROWS // 8:
                p, r = now
                total[0] += p * p
                total[1] += p * new[0]
                total[2] += r * r
                total[3] += new[0] * new[0] if last else r * new[1]
                total[4] += p * r
                total[5] += new[0] * r
        for i in range(6):
            acc[k, i, :, :] = total[i]
        acc[k, 6, :, :] = zero
        acc[k, 7, :, :] = zero

    step(0, True, False)

    def middle(k, carry):
        step(k, False, False)
        return carry

    lax.fori_loop(1, STEPS - 1, middle, 0)
    step(STEPS - 1, False, True)

    flat = jnp.sum(acc[...].reshape(8 * STEPS, 8, LANES), axis=1)
    flat = jnp.concatenate([flat, jnp.zeros_like(flat)], axis=0)
    row = lax.dot_general(
        jnp.ones((8, LANES), F32), flat, (((1,), (1,)), ((), ())),
        precision=lax.Precision.HIGHEST, preferred_element_type=F32,
    )
    for g in range(sums_ref.shape[0] // 8):
        sums_ref[pl.ds(8 * g, 8), :] = row


def middle_kernel(in_ref, out_ref):
    out_ref[...] = jnp.broadcast_to(jnp.sum(in_ref[...], axis=0, keepdims=True), out_ref.shape)


def final_kernel(sum_ref, basis_ref, height_ref, residual_ref):
    products = jnp.broadcast_to(jnp.sum(sum_ref[...], axis=0, keepdims=True), (8, LANES))
    row = lax.broadcasted_iota(jnp.int32, (24, LANES), 0)
    col = lax.broadcasted_iota(jnp.int32, (24, LANES), 1)
    half = STEPS + 1
    i = jnp.where(row < half, row, row - half)
    j = jnp.where(col < half, col, col - half)
    row_p, col_p = row < half, col < half
    inside = (row < VECTORS) & (col < VECTORS)
    total, apart = i + j, jnp.abs(i - j)
    even = (total & 1) == 0
    slot = jnp.where(row_p & col_p, 0, jnp.where(row_p | col_p, 4, 2))
    slot = slot + jnp.where(even, 0, 1)

    def gathered(index):
        index = jnp.where(inside, index, 6)
        parts = [
            jnp.take_along_axis(products, index[8 * g : 8 * g + 8], axis=1, mode="promise_in_bounds")
            for g in range(3)
        ]
        return jnp.concatenate(parts, axis=0)

    high = jnp.where(total == 2 * STEPS, 8 * (STEPS - 1) + 3, 8 * (total >> 1) + slot)
    gram = gathered(high) + gathered(8 * (apart >> 1) + slot) - gathered(slot)

    lead_r = (row == 0) | (row == half)
    tail_r = (row == STEPS) | (row >= VECTORS - 1)
    same = (row_p == col_p) & inside & ~tail_r
    h_turned = jnp.where(same & (row == col), 1.0, 0.0)
    h_turned = h_turned + jnp.where(same & (col == row + 1), jnp.where(lead_r, 1.0, 0.5), 0.0)
    h_turned = h_turned + jnp.where(same & (col == row - 1) & ~lead_r, 0.5, 0.0)
    keep = jnp.where(tail_r, 0.0, 1.0)
    to_next = jnp.where(tail_r, 0.0, jnp.where(lead_r, 1.0, 0.5))
    to_last = jnp.where(tail_r | lead_r, 0.0, 0.5)

    def as_row(matrix, column):
        return jnp.sum(matrix * column, axis=0, keepdims=True)

    def dot(a, b):
        return jnp.sum(a * b, axis=1, keepdims=True)

    xc = jnp.zeros((24, LANES), F32)
    pc, rc = jnp.where(row == 0, 1.0, 0.0), jnp.where(row == half, 1.0, 0.0)
    pr, rr_row = jnp.where(col[:1] == 0, 1.0, 0.0), jnp.where(col[:1] == half, 1.0, 0.0)
    norm = dot(as_row(gram, rc), rr_row)
    for _ in range(STEPS):
        q_row = as_row(h_turned, pc)
        q_col = keep * pc + pltpu.roll(to_next * pc, 1, 0) + pltpu.roll(to_last * pc, 23, 0)
        t = norm / dot(as_row(gram, pc), q_row)
        xc = xc + t * pc
        rc = rc - t * q_col
        rr_row = rr_row - t * q_row
        new = dot(as_row(gram, rc), rr_row)
        ratio = new / norm
        pc = rc + ratio * pc
        norm = new
    xs = [jnp.broadcast_to(xc[k : k + 1, :], (8, LANES)) for k in range(VECTORS)]
    rs = [jnp.broadcast_to(rc[k : k + 1, :], (8, LANES)) for k in range(VECTORS)]
    for g in range(ROWS // 8):
        first = second = None
        for k in range(VECTORS):
            tile = basis_ref[k, pl.ds(16 + 8 * g, 8), :]
            first = xs[k] * tile if first is None else first + xs[k] * tile
            second = rs[k] * tile if second is None else second + rs[k] * tile
        height_ref[pl.ds(8 * g, 8), :] = first
        residual_ref[pl.ds(8 * g, 8), :] = second


def shape(*dims):
    return pltpu.VMEM(dims, F32)


def held(*values, space=pltpu.VMEM):
    return tuple(pltpu.with_memory_space_constraint(v, space) for v in values)


def limit(mib):
    return pltpu.CompilerParams(vmem_limit_bytes=mib << 20)


def per_device(forcing, search_direction, ocean_depth, land_mask, fold_map):
    lat_count, lon_count = lax.axis_size("lat"), lax.axis_size(LON)
    call = pl.pallas_call
    fields, first, second, reach, choice = call(
        functools.partial(pack_kernel, lon_count // 2), name="pack",
        in_specs=[pl.BlockSpec(memory_space=pl.ANY)] * 5,
        out_specs=[pl.BlockSpec(memory_space=pltpu.VMEM)] * 3 + [pl.BlockSpec(memory_space=pltpu.SMEM)] * 2,
        out_shape=(shape(3, ROWS, LANES), shape(BLK + 32, LANES), shape(BLK + 32, LANES),
                   pltpu.SMEM((1,), jnp.int32), pltpu.SMEM((1,), jnp.int32)),
        scratch_shapes=[pltpu.VMEM((ROWS, LANES), F32)] * 3 + [
            pltpu.VMEM((ROWS, LANES), jnp.int32), pltpu.SMEM((LANES,), jnp.int32), pltpu.SemaphoreType.DMA((5,)),
        ],
        compiler_params=limit(4),
    )(*held(forcing, search_direction, ocean_depth, land_mask, fold_map, space=pltpu.HBM))
    evens, odds = range(0, lon_count, 2), range(1, lon_count, 2)
    first = lax.ppermute(first, LON, [(i, i + 1) for i in evens] + [(i + 1, i) for i in evens])
    wrap = [(i, (i + 1) % lon_count) for i in odds]
    second = lax.ppermute(second, LON, wrap + [(b, a) for a, b in wrap])

    one, two, two_next = call(
        functools.partial(turn_kernel, lat_count - 1), name="turn",
        in_specs=[pl.BlockSpec(memory_space=pltpu.SMEM)] + [pl.BlockSpec(memory_space=pltpu.VMEM)] * 3,
        out_shape=(shape(64, LANES),) * 3,
        scratch_shapes=[pltpu.VMEM((BLK + 32, LANES), F32)] * 2 + [pltpu.VMEM((64, LANES), F32)] * 4,
        compiler_params=limit(4),
    )(reach, *held(fields, first, second))

    evens, odds = range(0, lat_count, 2), range(1, lat_count - 1, 2)
    one = lax.ppermute(one, "lat", [(i, i + 1) for i in evens] + [(i + 1, i) for i in evens])
    swaps = [
        (i * lon_count + c, (i + s) * lon_count + c)
        for k in odds for i, s in ((k, 1), (k + 1, -1)) for c in range(lon_count)
    ]
    top = (lat_count - 1) * lon_count

    def second_round(value, pairing):
        fold = [(top + i, top + (2 * pairing - i) % lon_count) for i in range(lon_count)]
        return lax.ppermute(value, ("lat",) + LON, swaps + fold)

    def branch(index):
        if index % 2 == 0:
            return lambda near, far: second_round(near, index // 2)
        return lambda near, far: second_round(near, index // 2) + second_round(far, (index // 2 + 1) % (lon_count // 2))

    two = lax.switch(choice[0], [branch(i) for i in range(lon_count)], two, two_next)

    basis, sums = call(
        basis_kernel, name="basis",
        out_shape=(shape(VECTORS, EXT, LANES), shape(lon_count, LANES)),
        scratch_shapes=[
            pltpu.VMEM((2, EXT, LANES), F32),
            pltpu.VMEM((VECTORS, EXT, LANES), F32),
            pltpu.VMEM((2, EXT, LANES), F32),
            pltpu.VMEM((2, 9, EXT, LANES), F32),
            pltpu.VMEM((STEPS, 8, 8, LANES), F32),
        ] + [pltpu.VMEM((BLK + 32, LANES), F32)] * 2 + [pltpu.VMEM((64, LANES), F32)] * 3 + [
            pltpu.SemaphoreType.DMA,
        ],
        in_specs=[pl.BlockSpec(memory_space=pltpu.VMEM)] * 4 + [pl.BlockSpec(memory_space=pl.ANY)],
        compiler_params=limit(12),
    )(*held(fields, first, second, one), *held(two, space=pltpu.HBM))
    sums = lax.all_to_all(sums, LON, split_axis=0, concat_axis=0, tiled=True)
    sums = call(middle_kernel, name="middle", out_shape=shape(lat_count, LANES), compiler_params=limit(2))(*held(sums))
    sums = lax.all_to_all(sums, "lat", split_axis=0, concat_axis=0, tiled=True)
    return call(
        final_kernel, name="final", out_shape=(jax.ShapeDtypeStruct((ROWS, LANES), F32),) * 2,
        compiler_params=limit(4),
    )(*held(sums, basis))


def solution(mesh):
    lon = mesh.shape["lon"]
    split = Mesh(mesh.devices.reshape(mesh.shape["lat"], lon // 4, 4), ("lat", "lon_0", "lon_1"))
    return jax.shard_map(
        per_device,
        mesh=split,
        in_specs=(P("lat", LON), P("lat", LON), P("lat", LON), P("lat", LON), P()),
        out_specs=(P("lat", LON), P("lat", LON)),
        check_vma=False,
    )
```

```python
import functools

import jax
import jax.numpy as jnp
from jax import lax
from jax.experimental import pallas as pl
from jax.experimental.pallas import tpu as pltpu
from jax.sharding import Mesh
from jax.sharding import PartitionSpec as P

STEPS = 8
REACH = 256
ROWS = 160
LANES = 128
EXT = ROWS + 32
PITCH = 216
EDGE = 9
BLK = 40
LON = ("lon_0", "lon_1")
VECTORS = 2 * STEPS + 1
F32 = jnp.float32


def lanes_of(rows):
    return lax.broadcasted_iota(jnp.int32, (rows, LANES), 1)


def shift_east(a, b, lane):
    ra, rb = pltpu.roll(a, 1, 1), pltpu.roll(b, 1, 1)
    first = lane == 0
    return jnp.where(first, rb, ra), jnp.where(first, ra, rb)


def shift_west(a, b, lane):
    ra, rb = pltpu.roll(a, LANES - 1, 1), pltpu.roll(b, LANES - 1, 1)
    last = lane == LANES - 1
    return jnp.where(last, rb, ra), jnp.where(last, ra, rb)


def pack_kernel(pairs, f_hbm, p_hbm, d_hbm, m_hbm, map_hbm, x_ref, first_ref, second_ref, reach_ref, choice_ref,
                f_ref, p_ref, d_ref, m_ref, pivot, sems):
    even = lax.axis_index(LON) % 2 == 0
    copies = [
        pltpu.make_async_copy(source, target, sems.at[i])
        for i, (source, target) in enumerate((
            (m_hbm, m_ref), (d_hbm, d_ref), (f_hbm, f_ref), (p_hbm, p_ref), (map_hbm.at[pl.ds(0, LANES)], pivot),
        ))
    ]
    for copy in copies:
        copy.start()
    for copy in copies:
        copy.wait()
    for g in range(ROWS // 8):
        rows = pl.ds(8 * g, 8)
        flag = m_ref[rows, :].astype(F32)
        x_ref[0, rows, :] = d_ref[rows, :] * flag
        x_ref[1, rows, :] = f_ref[rows, :] * flag
        x_ref[2, rows, :] = p_ref[rows, :] * flag
    lane = lanes_of(8)
    for v in range(BLK // 8):
        east = jnp.zeros((8, LANES), F32)
        west = jnp.zeros((8, LANES), F32)
        for q in range(3):
            for blk in range(4):
                at = EDGE * (4 * q + blk)
                tile = x_ref[q, pl.ds(BLK * blk + 8 * v, 8), :]
                inside = (lane >= at) & (lane < at + EDGE)
                west = jnp.where(inside, pltpu.roll(tile, at, 1) if at else tile, west)
                east = jnp.where(inside, pltpu.roll(tile, (at + EDGE) % LANES, 1), east)
        first_ref[pl.ds(8 * v, 8), :] = jnp.where(even, east, west)
        second_ref[pl.ds(8 * v, 8), :] = jnp.where(even, west, east)
    for slot, (q, row) in enumerate(((0, ROWS - 8), (1, ROWS - 8), (2, ROWS - 8), (0, ROWS - 16))):
        tile = x_ref[q, pl.ds(row, 8), :]
        first_ref[pl.ds(BLK + 8 * slot, 8), :] = tile
        second_ref[pl.ds(BLK + 8 * slot, 8), :] = tile
    past = pivot[0] + (2 * pairs * LANES - 8)
    reach = past % (2 * LANES) + 8
    reach_ref[0] = reach
    split = jnp.where(reach + EDGE >= 2 * LANES, 1, 0)
    choice_ref[0] = 2 * ((past // (2 * LANES)) % pairs) + split


def unpack_halo(from_west, from_east, q, blk, v, lane):
    at = EDGE * (4 * q + blk)
    right = from_east[pl.ds(8 * v, 8), :]
    left = from_west[pl.ds(8 * v, 8), :]
    right = pltpu.roll(right, LANES - at, 1) if at else right
    left = pltpu.roll(left, (2 * LANES - EDGE - at) % LANES, 1)
    return jnp.where(lane < EDGE, right, jnp.where(lane >= LANES - EDGE, left, 0.0))


def sort_partners(axis, first, second, before, after):
    even = lax.axis_index(axis) % 2 == 0
    for g in range(first.shape[0] // 8):
        rows = pl.ds(8 * g, 8)
        a, b = first[rows, :], second[rows, :]
        before[rows, :] = jnp.where(even, b, a)
        after[rows, :] = jnp.where(even, a, b)


def turn_kernel(tops, r_ref, x_ref, first_ref, second_ref, one_ref, two_ref, next_ref,
                fw_ref, fe_ref, north_ref, south_ref, t1_ref, t2_ref):
    lane = lanes_of(8)
    lat = lax.axis_index("lat")
    even, top_row = lat % 2 == 0, lat == tops
    sort_partners(LON, first_ref, second_ref, fw_ref, fe_ref)
    top, low = ROWS // 8 - 1, 0
    for ref, rows in (
        (north_ref, ((0, top), (1, top), (2, top), (0, top - 1))),
        (south_ref, ((0, low), (1, low), (2, low), (0, low + 1))),
    ):
        for slot, (q, g) in enumerate(rows):
            ref[pl.ds(8 * slot, 8), :] = x_ref[q, pl.ds(8 * g, 8), :]
            blk, v = 8 * g // BLK, (8 * g % BLK) // 8
            ref[pl.ds(32 + 8 * slot, 8), :] = unpack_halo(fw_ref, fe_ref, q, blk, v, lane)
    for g in range(8):
        rows = pl.ds(8 * g, 8)
        north, south = north_ref[rows, :], south_ref[rows, :]
        one_ref[rows, :] = jnp.where(even, north, south)
        two_ref[rows, :] = jnp.where(even, south, north)
        next_ref[rows, :] = jnp.zeros((8, LANES), F32)

    @pl.when(top_row)
    def _():
        across_fold(r_ref[0], lane, north_ref, fw_ref, fe_ref, two_ref, next_ref, t1_ref, t2_ref)


def across_fold(reach, lane, north_ref, fw_ref, fe_ref, fold_ref, next_ref, t1_ref, t2_ref):
    along = reach - lane
    pick = along & (LANES - 1)
    place_a = along
    place_b = jnp.where(lane < EDGE, along - LANES, along + LANES)
    halo = (lane < EDGE) | (lane >= LANES - EDGE)
    for slot in range(4):
        rows = pl.ds(8 * slot, 8)
        own = jnp.take_along_axis(north_ref[rows, :], pick, axis=1, mode="promise_in_bounds")
        west = jnp.take_along_axis(fw_ref[pl.ds(BLK + 8 * slot, 8), :], pick, axis=1, mode="promise_in_bounds")
        east = jnp.take_along_axis(fe_ref[pl.ds(BLK + 8 * slot, 8), :], pick, axis=1, mode="promise_in_bounds")
        for part, place in ((0, place_a), (32, place_b)):
            near = jnp.where(place < 0, west, jnp.where(place < LANES, own, east))
            near = jnp.where(place < 2 * LANES, near, 0.0)
            far = jnp.where(place >= 2 * LANES, own, 0.0)
            if part:
                near = jnp.where(halo, near, 0.0)
                far = jnp.where(halo, far, 0.0)
            t1_ref[pl.ds(part + 8 * slot, 8), :] = near
            t2_ref[pl.ds(part + 8 * slot, 8), :] = far
    for g in range(8):
        for m in range(8):
            fold_ref[pl.ds(8 * g + m, 1), :] = t1_ref[pl.ds(8 * g + 7 - m, 1), :]
            next_ref[pl.ds(8 * g + m, 1), :] = t2_ref[pl.ds(8 * g + 7 - m, 1), :]


GROUPS = ROWS // 8 + 2


def land_kernel(in_ref, out_ref):
    out_ref[...] = in_ref[...]


def basis_kernel(x_ref, first_ref, second_ref, one_ref, two_ref, basis_ref, sums_ref,
                 depth, side, inv, coef, acc, fw_ref, fe_ref, fs_ref, fn_ref):
    sort_partners(LON, first_ref, second_ref, fw_ref, fe_ref)
    lane = lanes_of(8)
    zero = jnp.zeros((8, LANES), F32)
    targets = (
        lambda t: depth.at[t],
        lambda t: (basis_ref if t == 0 else side).at[STEPS + 1],
        lambda t: (basis_ref if t == 0 else side).at[0],
    )
    for q in range(3):
        own, rim = targets[q](0), targets[q](1)
        for g in range(ROWS // 8):
            own[pl.ds(16 + 8 * g, 8), :] = x_ref[q, pl.ds(8 * g, 8), :]
            blk, v = 8 * g // BLK, (8 * g % BLK) // 8
            rim[pl.ds(16 + 8 * g, 8), :] = unpack_halo(fw_ref, fe_ref, q, blk, v, lane)
    sort_partners("lat", one_ref, two_ref, fs_ref, fn_ref)
    for q in range(3):
        own, rim = targets[q](0), targets[q](1)
        for t, ref in ((0, own), (1, rim)):
            at = 32 * t + 8 * q
            ref[pl.ds(8, 8), :] = fs_ref[pl.ds(at, 8), :]
            ref[pl.ds(EXT - 16, 8), :] = fn_ref[pl.ds(at, 8), :]
            if q == 0:
                at = 32 * t + 24
                ref[pl.ds(0, 8), :] = fs_ref[pl.ds(at, 8), :]
                ref[pl.ds(EXT - 8, 8), :] = fn_ref[pl.ds(at, 8), :]
            else:
                ref[pl.ds(0, 8), :] = zero
                ref[pl.ds(EXT - 8, 8), :] = zero
    for k in list(range(1, STEPS + 1)) + list(range(STEPS + 2, VECTORS)):
        for ref in (basis_ref, side):
            ref[k, pl.ds(0, 8), :] = zero
            ref[k, pl.ds(EXT - 8, 8), :] = zero
    for t in range(2):
        inv[t, pl.ds(0, 8), :] = zero
        inv[t, pl.ds(EXT - 8, 8), :] = zero

    def root_of(g):
        at = 8 + 8 * g
        vert, mid, wet_mid, deep = [], [], [], []
        for t in range(2):
            down = depth[t, pl.ds(at - 1, 8), :]
            here = depth[t, pl.ds(at, 8), :]
            up = depth[t, pl.ds(at + 1, 8), :]
            wet = jnp.where(here > 0.0, 1.0, 0.0)
            wets = jnp.where(down > 0.0, 1.0, 0.0) + jnp.where(up > 0.0, 1.0, 0.0)
            vert.append((down + up, wets))
            mid.append((here + 0.5 * (down + up), wet + 0.5 * wets))
            deep.append(here)
            wet_mid.append(wet)
        sums = []
        for c in range(2):
            ea, eb = shift_east(mid[0][c], mid[1][c], lane)
            wa, wb = shift_west(mid[0][c], mid[1][c], lane)
            sums.append((vert[0][c] + (ea + wa), vert[1][c] + (eb + wb)))
        for t in range(2):
            links = 0.5 * (deep[t] * sums[1][t] + sums[0][t])
            diagonal = wet_mid[t] * (deep[t] / (REACH * REACH) + links) + (1.0 - wet_mid[t])
            inv[t, pl.ds(at, 8), :] = lax.rsqrt(diagonal) * wet_mid[t]

    def coefs_of(g):
        at = 8 + 8 * g
        d = [[depth[t, pl.ds(at + s, 8), :] for s in (-1, 0, 1)] for t in range(2)]
        r = [[inv[t, pl.ds(at + s, 8), :] for s in (-1, 0, 1)] for t in range(2)]
        de, re = shift_east(d[0][1], d[1][1], lane), shift_east(r[0][1], r[1][1], lane)
        dw, rw = shift_west(d[0][1], d[1][1], lane), shift_west(r[0][1], r[1][1], lane)
        for t in range(2):
            for base, (dc, rc) in enumerate(((d[t][1], r[t][1]), (de[t], re[t]), (dw[t], rw[t]))):
                for s in range(3):
                    if base == 0 and s == 1:
                        continue
                    whole = base == 0 or s == 1
                    c = (dc + d[t][s]) * (rc * r[t][s])
                    coef[t, 3 * base + s, pl.ds(at, 8), :] = c * (-1.0 if whole else -0.5)

    for g in range(GROUPS):
        root_of(g)
    for g in range(GROUPS):
        coefs_of(g)

    def twice_applied(k, at, tiles, weights):
        parts = []
        for t in range(2):
            ref = basis_ref if t == 0 else side
            down, here, up = (ref[k, pl.ds(at + s, 8), :] for s in (-1, 0, 1))
            w = weights[t]
            straight = w[0] * down + w[2] * up
            toward_w = (w[3] * down + w[5] * up) + w[4] * here
            toward_e = (w[6] * down + w[8] * up) + w[7] * here
            parts.append((straight, toward_w, toward_e, here))
        wa, wb = shift_west(parts[0][1], parts[1][1], lane)
        ea, eb = shift_east(parts[0][2], parts[1][2], lane)
        return ((parts[0][0] + (wa + ea), parts[1][0] + (wb + eb))[:tiles], parts[0][3])

    def weights_at(at):
        return [[None if i == 1 else coef[t, i, pl.ds(at, 8), :] for i in range(9)] for t in range(2)]

    def step(k, first, last):
        total = [zero] * 6
        tiles = 1 if last else 2
        for g in range(1, GROUPS - 1) if last else range(GROUPS):
            at = 8 + 8 * g
            w = weights_at(at)
            now, new = [], []
            for base in ((0,) if last else (0, STEPS + 1)):
                out, here = twice_applied(base + k, at, tiles, w)
                now.append(here)
                for t in range(tiles):
                    ref = basis_ref if t == 0 else side
                    value = 0.5 * out[t] if first else out[t] - ref[base + k - 1, pl.ds(at, 8), :]
                    ref[base + k + 1, pl.ds(at, 8), :] = value
                    if t == 0:
                        new.append(value)
            if last:
                now.append(basis_ref[STEPS + 1 + k, pl.ds(at, 8), :])
            if 1 <= g <= ROWS // 8:
                p, r = now
                total[0] += p * p
                total[1] += p * new[0]
                total[2] += r * r
                total[3] += new[0] * new[0] if last else r * new[1]
                total[4] += p * r
                total[5] += new[0] * r
        for i in range(6):
            acc[k, i, :, :] = total[i]
        acc[k, 6, :, :] = zero
        acc[k, 7, :, :] = zero

    step(0, True, False)

    def middle(k, carry):
        step(k, False, False)
        return carry

    lax.fori_loop(1, STEPS - 1, middle, 0)
    step(STEPS - 1, False, True)

    flat = jnp.sum(acc[...].reshape(8 * STEPS, 8, LANES), axis=1)
    flat = jnp.concatenate([flat, jnp.zeros_like(flat)], axis=0)
    row = lax.dot_general(
        jnp.ones((8, LANES), F32), flat, (((1,), (1,)), ((), ())),
        precision=lax.Precision.HIGHEST, preferred_element_type=F32,
    )
    for g in range(sums_ref.shape[0] // 8):
        sums_ref[pl.ds(8 * g, 8), :] = row


def middle_kernel(in_ref, out_ref):
    out_ref[...] = jnp.broadcast_to(jnp.sum(in_ref[...], axis=0, keepdims=True), out_ref.shape)


def final_kernel(sum_ref, basis_ref, height_ref, residual_ref):
    products = jnp.broadcast_to(jnp.sum(sum_ref[...], axis=0, keepdims=True), (8, LANES))
    row = lax.broadcasted_iota(jnp.int32, (24, LANES), 0)
    col = lax.broadcasted_iota(jnp.int32, (24, LANES), 1)
    half = STEPS + 1
    i = jnp.where(row < half, row, row - half)
    j = jnp.where(col < half, col, col - half)
    row_p, col_p = row < half, col < half
    inside = (row < VECTORS) & (col < VECTORS)
    total, apart = i + j, jnp.abs(i - j)
    even = (total & 1) == 0
    slot = jnp.where(row_p & col_p, 0, jnp.where(row_p | col_p, 4, 2))
    slot = slot + jnp.where(even, 0, 1)

    def gathered(index):
        index = jnp.where(inside, index, 6)
        parts = [
            jnp.take_along_axis(products, index[8 * g : 8 * g + 8], axis=1, mode="promise_in_bounds")
            for g in range(3)
        ]
        return jnp.concatenate(parts, axis=0)

    high = jnp.where(total == 2 * STEPS, 8 * (STEPS - 1) + 3, 8 * (total >> 1) + slot)
    gram = gathered(high) + gathered(8 * (apart >> 1) + slot) - gathered(slot)

    lead_r, lead_c = (row == 0) | (row == half), (col == 0) | (col == half)
    tail_r = (row == STEPS) | (row >= VECTORS - 1)
    tail_c = (col == STEPS) | (col >= VECTORS - 1)
    mapped = jnp.where(tail_c, 0.0, gram + jnp.where(lead_c, 1.0, 0.5) * pltpu.roll(gram, LANES - 1, 1)
                       + jnp.where(lead_c, 0.0, 0.5) * pltpu.roll(gram, 1, 1))
    same = (row_p == col_p) & inside & ~tail_r
    h_turned = jnp.where(same & (row == col), 1.0, 0.0)
    h_turned = h_turned + jnp.where(same & (col == row + 1), jnp.where(lead_r, 1.0, 0.5), 0.0)
    h_turned = h_turned + jnp.where(same & (col == row - 1) & ~lead_r, 0.5, 0.0)
    keep = jnp.where(tail_r, 0.0, 1.0)
    to_next = jnp.where(tail_r, 0.0, jnp.where(lead_r, 1.0, 0.5))
    to_last = jnp.where(tail_r | lead_r, 0.0, 0.5)

    def down(value):
        return jnp.sum(value, axis=0, keepdims=True)

    xc = jnp.zeros((24, LANES), F32)
    pc, rc = jnp.where(row == 0, 1.0, 0.0), jnp.where(row == half, 1.0, 0.0)
    p_row, r_row = jnp.where(col[:1] == 0, 1.0, 0.0), jnp.where(col[:1] == half, 1.0, 0.0)
    gr = jnp.broadcast_to(jnp.sum(gram * r_row, axis=1, keepdims=True), (24, LANES))
    norm = down(rc * gr)
    for _ in range(STEPS):
        z = jnp.broadcast_to(jnp.sum(mapped * p_row, axis=1, keepdims=True), (24, LANES))
        q_row = down(h_turned * pc)
        q_col = keep * pc + pltpu.roll(to_next * pc, 1, 0) + pltpu.roll(to_last * pc, 23, 0)
        t = norm / down(pc * z)
        xc = xc + t * pc
        rc = rc - t * q_col
        r_row = r_row - t * q_row
        gr = gr - t * z
        new = down(rc * gr)
        ratio = new / norm
        pc = rc + ratio * pc
        p_row = r_row + ratio * p_row
        norm = new
    xs = [jnp.broadcast_to(xc[k : k + 1, :], (8, LANES)) for k in range(VECTORS)]
    rs = [jnp.broadcast_to(rc[k : k + 1, :], (8, LANES)) for k in range(VECTORS)]
    for g in range(ROWS // 8):
        first = second = None
        for k in range(VECTORS):
            tile = basis_ref[k, pl.ds(16 + 8 * g, 8), :]
            first = xs[k] * tile if first is None else first + xs[k] * tile
            second = rs[k] * tile if second is None else second + rs[k] * tile
        height_ref[pl.ds(8 * g, 8), :] = first
        residual_ref[pl.ds(8 * g, 8), :] = second


def shape(*dims):
    return pltpu.VMEM(dims, F32)


def held(*values, space=pltpu.VMEM):
    return tuple(pltpu.with_memory_space_constraint(v, space) for v in values)


def limit(mib):
    return pltpu.CompilerParams(vmem_limit_bytes=mib << 20)


def per_device(forcing, search_direction, ocean_depth, land_mask, fold_map):
    lat_count, lon_count = lax.axis_size("lat"), lax.axis_size(LON)
    call = pl.pallas_call
    fields, first, second, reach, choice = call(
        functools.partial(pack_kernel, lon_count // 2), name="pack",
        in_specs=[pl.BlockSpec(memory_space=pl.ANY)] * 5,
        out_specs=[pl.BlockSpec(memory_space=pltpu.VMEM)] * 3 + [pl.BlockSpec(memory_space=pltpu.SMEM)] * 2,
        out_shape=(shape(3, ROWS, LANES), shape(BLK + 32, LANES), shape(BLK + 32, LANES),
                   pltpu.SMEM((1,), jnp.int32), pltpu.SMEM((1,), jnp.int32)),
        scratch_shapes=[pltpu.VMEM((ROWS, LANES), F32)] * 3 + [
            pltpu.VMEM((ROWS, LANES), jnp.int32), pltpu.SMEM((LANES,), jnp.int32), pltpu.SemaphoreType.DMA((5,)),
        ],
        compiler_params=limit(4),
    )(*held(forcing, search_direction, ocean_depth, land_mask, fold_map, space=pltpu.HBM))
    evens, odds = range(0, lon_count, 2), range(1, lon_count, 2)
    first = lax.ppermute(first, LON, [(i, i + 1) for i in evens] + [(i + 1, i) for i in evens])
    wrap = [(i, (i + 1) % lon_count) for i in odds]
    second = lax.ppermute(second, LON, wrap + [(b, a) for a, b in wrap])

    one, two, two_next = call(
        functools.partial(turn_kernel, lat_count - 1), name="turn",
        in_specs=[pl.BlockSpec(memory_space=pltpu.SMEM)] + [pl.BlockSpec(memory_space=pltpu.VMEM)] * 3,
        out_shape=(shape(64, LANES),) * 3,
        scratch_shapes=[pltpu.VMEM((BLK + 32, LANES), F32)] * 2 + [pltpu.VMEM((64, LANES), F32)] * 4,
        compiler_params=limit(4),
    )(reach, *held(fields, first, second))

    evens, odds = range(0, lat_count, 2), range(1, lat_count - 1, 2)
    one = lax.ppermute(one, "lat", [(i, i + 1) for i in evens] + [(i + 1, i) for i in evens])
    swaps = [
        (i * lon_count + c, (i + s) * lon_count + c)
        for k in odds for i, s in ((k, 1), (k + 1, -1)) for c in range(lon_count)
    ]
    top = (lat_count - 1) * lon_count

    def second_round(value, pairing):
        fold = [(top + i, top + (2 * pairing - i) % lon_count) for i in range(lon_count)]
        return lax.ppermute(value, ("lat",) + LON, swaps + fold)

    def branch(index):
        def exchange(near, far):
            value = second_round(near, index // 2)
            if index % 2:
                value = value + second_round(far, (index // 2 + 1) % (lon_count // 2))
            return call(land_kernel, name="land", out_shape=shape(64, LANES), compiler_params=limit(2))(*held(value))

        return exchange

    two = lax.switch(choice[0], [branch(i) for i in range(lon_count)], two, two_next)

    basis, sums = call(
        basis_kernel, name="basis",
        out_shape=(shape(VECTORS, PITCH, LANES), shape(lon_count, LANES)),
        scratch_shapes=[
            pltpu.VMEM((2, PITCH, LANES), F32),
            pltpu.VMEM((VECTORS, PITCH, LANES), F32),
            pltpu.VMEM((2, PITCH, LANES), F32),
            pltpu.VMEM((2, 9, PITCH, LANES), F32),
            pltpu.VMEM((STEPS, 8, 8, LANES), F32),
        ] + [pltpu.VMEM((BLK + 32, LANES), F32)] * 2 + [pltpu.VMEM((64, LANES), F32)] * 2,
        compiler_params=limit(12),
    )(*held(fields, first, second, one, two))
    sums = lax.all_to_all(sums, LON, split_axis=0, concat_axis=0, tiled=True)
    sums = call(middle_kernel, name="middle", out_shape=shape(lat_count, LANES), compiler_params=limit(2))(*held(sums))
    sums = lax.all_to_all(sums, "lat", split_axis=0, concat_axis=0, tiled=True)
    return call(
        final_kernel, name="final", out_shape=(jax.ShapeDtypeStruct((ROWS, LANES), F32),) * 2,
        compiler_params=limit(4),
    )(*held(sums, basis))


def solution(mesh):
    lon = mesh.shape["lon"]
    split = Mesh(mesh.devices.reshape(mesh.shape["lat"], lon // 4, 4), ("lat", "lon_0", "lon_1"))
    return jax.shard_map(
        per_device,
        mesh=split,
        in_specs=(P("lat", LON), P("lat", LON), P("lat", LON), P("lat", LON), P()),
        out_specs=(P("lat", LON), P("lat", LON)),
        check_vma=False,
    )
```

```python
import functools

import jax
import jax.numpy as jnp
from jax import lax
from jax.experimental import pallas as pl
from jax.experimental.pallas import tpu as pltpu
from jax.sharding import Mesh
from jax.sharding import PartitionSpec as P

STEPS = 8
REACH = 256
ROWS = 160
LANES = 128
EXT = ROWS + 32
PITCH = 216
EDGE = 9
BLK = 40
LON = ("lon_0", "lon_1")
VECTORS = 2 * STEPS + 1
F32 = jnp.float32


def lanes_of(rows):
    return lax.broadcasted_iota(jnp.int32, (rows, LANES), 1)


def shift_east(a, b, lane):
    ra, rb = pltpu.roll(a, 1, 1), pltpu.roll(b, 1, 1)
    first = lane == 0
    return jnp.where(first, rb, ra), jnp.where(first, ra, rb)


def shift_west(a, b, lane):
    ra, rb = pltpu.roll(a, LANES - 1, 1), pltpu.roll(b, LANES - 1, 1)
    last = lane == LANES - 1
    return jnp.where(last, rb, ra), jnp.where(last, ra, rb)


def pack_kernel(pairs, f_hbm, p_hbm, d_hbm, m_hbm, map_hbm, x_ref, first_ref, second_ref, reach_ref, choice_ref,
                f_ref, p_ref, d_ref, m_ref, pivot, sems):
    even = lax.axis_index(LON) % 2 == 0
    copies = [
        pltpu.make_async_copy(source, target, sems.at[i])
        for i, (source, target) in enumerate((
            (m_hbm, m_ref), (d_hbm, d_ref), (f_hbm, f_ref), (p_hbm, p_ref), (map_hbm.at[pl.ds(0, LANES)], pivot),
        ))
    ]
    for copy in copies:
        copy.start()
    for copy in copies:
        copy.wait()
    for g in range(ROWS // 8):
        rows = pl.ds(8 * g, 8)
        flag = m_ref[rows, :].astype(F32)
        x_ref[0, rows, :] = d_ref[rows, :] * flag
        x_ref[1, rows, :] = f_ref[rows, :] * flag
        x_ref[2, rows, :] = p_ref[rows, :] * flag
    lane = lanes_of(8)
    for v in range(BLK // 8):
        east = jnp.zeros((8, LANES), F32)
        west = jnp.zeros((8, LANES), F32)
        for q in range(3):
            for blk in range(4):
                at = EDGE * (4 * q + blk)
                tile = x_ref[q, pl.ds(BLK * blk + 8 * v, 8), :]
                inside = (lane >= at) & (lane < at + EDGE)
                west = jnp.where(inside, pltpu.roll(tile, at, 1) if at else tile, west)
                east = jnp.where(inside, pltpu.roll(tile, (at + EDGE) % LANES, 1), east)
        first_ref[pl.ds(8 * v, 8), :] = jnp.where(even, east, west)
        second_ref[pl.ds(8 * v, 8), :] = jnp.where(even, west, east)
    for slot, (q, row) in enumerate(((0, ROWS - 8), (1, ROWS - 8), (2, ROWS - 8), (0, ROWS - 16))):
        tile = x_ref[q, pl.ds(row, 8), :]
        first_ref[pl.ds(BLK + 8 * slot, 8), :] = tile
        second_ref[pl.ds(BLK + 8 * slot, 8), :] = tile
    past = pivot[0] + (2 * pairs * LANES - 8)
    reach = past % (2 * LANES) + 8
    reach_ref[0] = reach
    split = jnp.where(reach + EDGE >= 2 * LANES, 1, 0)
    choice_ref[0] = 2 * ((past // (2 * LANES)) % pairs) + split


def unpack_halo(from_west, from_east, q, blk, v, lane):
    at = EDGE * (4 * q + blk)
    right = from_east[pl.ds(8 * v, 8), :]
    left = from_west[pl.ds(8 * v, 8), :]
    right = pltpu.roll(right, LANES - at, 1) if at else right
    left = pltpu.roll(left, (2 * LANES - EDGE - at) % LANES, 1)
    return jnp.where(lane < EDGE, right, jnp.where(lane >= LANES - EDGE, left, 0.0))


def sort_partners(axis, first, second, before, after):
    even = lax.axis_index(axis) % 2 == 0
    for g in range(first.shape[0] // 8):
        rows = pl.ds(8 * g, 8)
        a, b = first[rows, :], second[rows, :]
        before[rows, :] = jnp.where(even, b, a)
        after[rows, :] = jnp.where(even, a, b)


def turn_kernel(tops, r_ref, x_ref, second_ref, first_ref, one_ref, two_ref, next_ref,
                fw_ref, fe_ref, north_ref, south_ref, t1_ref, t2_ref):
    lane = lanes_of(8)
    lat = lax.axis_index("lat")
    even, top_row = lat % 2 == 0, lat == tops
    sort_partners(LON, first_ref, second_ref, fw_ref, fe_ref)
    top, low = ROWS // 8 - 1, 0
    for ref, rows in (
        (north_ref, ((0, top), (1, top), (2, top), (0, top - 1))),
        (south_ref, ((0, low), (1, low), (2, low), (0, low + 1))),
    ):
        for slot, (q, g) in enumerate(rows):
            ref[pl.ds(8 * slot, 8), :] = x_ref[q, pl.ds(8 * g, 8), :]
            blk, v = 8 * g // BLK, (8 * g % BLK) // 8
            ref[pl.ds(32 + 8 * slot, 8), :] = unpack_halo(fw_ref, fe_ref, q, blk, v, lane)
    for g in range(8):
        rows = pl.ds(8 * g, 8)
        north, south = north_ref[rows, :], south_ref[rows, :]
        one_ref[rows, :] = jnp.where(even, north, south)
        two_ref[rows, :] = jnp.where(even, south, north)
        next_ref[rows, :] = jnp.zeros((8, LANES), F32)

    @pl.when(top_row)
    def _():
        across_fold(r_ref[0], lane, north_ref, fw_ref, fe_ref, two_ref, next_ref, t1_ref, t2_ref)


def across_fold(reach, lane, north_ref, fw_ref, fe_ref, fold_ref, next_ref, t1_ref, t2_ref):
    along = reach - lane
    pick = along & (LANES - 1)
    place_a = along
    place_b = jnp.where(lane < EDGE, along - LANES, along + LANES)
    halo = (lane < EDGE) | (lane >= LANES - EDGE)
    for slot in range(4):
        rows = pl.ds(8 * slot, 8)
        own = jnp.take_along_axis(north_ref[rows, :], pick, axis=1, mode="promise_in_bounds")
        west = jnp.take_along_axis(fw_ref[pl.ds(BLK + 8 * slot, 8), :], pick, axis=1, mode="promise_in_bounds")
        east = jnp.take_along_axis(fe_ref[pl.ds(BLK + 8 * slot, 8), :], pick, axis=1, mode="promise_in_bounds")
        for part, place in ((0, place_a), (32, place_b)):
            near = jnp.where(place < 0, west, jnp.where(place < LANES, own, east))
            near = jnp.where(place < 2 * LANES, near, 0.0)
            far = jnp.where(place >= 2 * LANES, own, 0.0)
            if part:
                near = jnp.where(halo, near, 0.0)
                far = jnp.where(halo, far, 0.0)
            t1_ref[pl.ds(part + 8 * slot, 8), :] = near
            t2_ref[pl.ds(part + 8 * slot, 8), :] = far
    for g in range(8):
        for m in range(8):
            fold_ref[pl.ds(8 * g + m, 1), :] = t1_ref[pl.ds(8 * g + 7 - m, 1), :]
            next_ref[pl.ds(8 * g + m, 1), :] = t2_ref[pl.ds(8 * g + 7 - m, 1), :]


GROUPS = ROWS // 8 + 2


def land_kernel(two_ref, one_ref, south_ref, north_ref):
    sort_partners("lat", one_ref, two_ref, south_ref, north_ref)


def basis_kernel(x_ref, second_ref, first_ref, fs_ref, fn_ref, basis_ref, sums_ref,
                 depth, side, inv, coef, acc, fw_ref, fe_ref):
    sort_partners(LON, first_ref, second_ref, fw_ref, fe_ref)
    lane = lanes_of(8)
    zero = jnp.zeros((8, LANES), F32)
    targets = (
        lambda t: depth.at[t],
        lambda t: (basis_ref if t == 0 else side).at[STEPS + 1],
        lambda t: (basis_ref if t == 0 else side).at[0],
    )
    for q in range(3):
        own, rim = targets[q](0), targets[q](1)
        for g in range(ROWS // 8):
            own[pl.ds(16 + 8 * g, 8), :] = x_ref[q, pl.ds(8 * g, 8), :]
            blk, v = 8 * g // BLK, (8 * g % BLK) // 8
            rim[pl.ds(16 + 8 * g, 8), :] = unpack_halo(fw_ref, fe_ref, q, blk, v, lane)
    for q in range(3):
        own, rim = targets[q](0), targets[q](1)
        for t, ref in ((0, own), (1, rim)):
            at = 32 * t + 8 * q
            ref[pl.ds(8, 8), :] = fs_ref[pl.ds(at, 8), :]
            ref[pl.ds(EXT - 16, 8), :] = fn_ref[pl.ds(at, 8), :]
            if q == 0:
                at = 32 * t + 24
                ref[pl.ds(0, 8), :] = fs_ref[pl.ds(at, 8), :]
                ref[pl.ds(EXT - 8, 8), :] = fn_ref[pl.ds(at, 8), :]
            else:
                ref[pl.ds(0, 8), :] = zero
                ref[pl.ds(EXT - 8, 8), :] = zero
    for k in list(range(1, STEPS + 1)) + list(range(STEPS + 2, VECTORS)):
        for ref in (basis_ref, side):
            ref[k, pl.ds(0, 8), :] = zero
            ref[k, pl.ds(EXT - 8, 8), :] = zero
    for t in range(2):
        inv[t, pl.ds(0, 8), :] = zero
        inv[t, pl.ds(EXT - 8, 8), :] = zero

    def root_of(g):
        at = 8 + 8 * g
        vert, mid, wet_mid, deep = [], [], [], []
        for t in range(2):
            down = depth[t, pl.ds(at - 1, 8), :]
            here = depth[t, pl.ds(at, 8), :]
            up = depth[t, pl.ds(at + 1, 8), :]
            wet = jnp.where(here > 0.0, 1.0, 0.0)
            wets = jnp.where(down > 0.0, 1.0, 0.0) + jnp.where(up > 0.0, 1.0, 0.0)
            vert.append((down + up, wets))
            mid.append((here + 0.5 * (down + up), wet + 0.5 * wets))
            deep.append(here)
            wet_mid.append(wet)
        sums = []
        for c in range(2):
            ea, eb = shift_east(mid[0][c], mid[1][c], lane)
            wa, wb = shift_west(mid[0][c], mid[1][c], lane)
            sums.append((vert[0][c] + (ea + wa), vert[1][c] + (eb + wb)))
        for t in range(2):
            links = 0.5 * (deep[t] * sums[1][t] + sums[0][t])
            diagonal = wet_mid[t] * (deep[t] / (REACH * REACH) + links) + (1.0 - wet_mid[t])
            inv[t, pl.ds(at, 8), :] = lax.rsqrt(diagonal) * wet_mid[t]

    def coefs_of(g):
        at = 8 + 8 * g
        d = [[depth[t, pl.ds(at + s, 8), :] for s in (-1, 0, 1)] for t in range(2)]
        r = [[inv[t, pl.ds(at + s, 8), :] for s in (-1, 0, 1)] for t in range(2)]
        de, re = shift_east(d[0][1], d[1][1], lane), shift_east(r[0][1], r[1][1], lane)
        dw, rw = shift_west(d[0][1], d[1][1], lane), shift_west(r[0][1], r[1][1], lane)
        for t in range(2):
            for base, (dc, rc) in enumerate(((d[t][1], r[t][1]), (de[t], re[t]), (dw[t], rw[t]))):
                for s in range(3):
                    if base == 0 and s == 1:
                        continue
                    whole = base == 0 or s == 1
                    c = (dc + d[t][s]) * (rc * r[t][s])
                    coef[t, 3 * base + s, pl.ds(at, 8), :] = c * (-1.0 if whole else -0.5)

    for g in range(GROUPS):
        root_of(g)
    for g in range(GROUPS):
        coefs_of(g)

    def twice_applied(k, at, tiles, weights):
        parts = []
        for t in range(2):
            ref = basis_ref if t == 0 else side
            down, here, up = (ref[k, pl.ds(at + s, 8), :] for s in (-1, 0, 1))
            w = weights[t]
            straight = w[0] * down + w[2] * up
            toward_w = (w[3] * down + w[5] * up) + w[4] * here
            toward_e = (w[6] * down + w[8] * up) + w[7] * here
            parts.append((straight, toward_w, toward_e, here))
        wa, wb = shift_west(parts[0][1], parts[1][1], lane)
        ea, eb = shift_east(parts[0][2], parts[1][2], lane)
        return ((parts[0][0] + (wa + ea), parts[1][0] + (wb + eb))[:tiles], parts[0][3])

    def weights_at(at):
        return [[None if i == 1 else coef[t, i, pl.ds(at, 8), :] for i in range(9)] for t in range(2)]

    def step(k, first, last):
        total = [zero] * 6
        tiles = 1 if last else 2
        for g in range(1, GROUPS - 1) if last else range(GROUPS):
            at = 8 + 8 * g
            w = weights_at(at)
            now, new = [], []
            for base in ((0,) if last else (0, STEPS + 1)):
                out, here = twice_applied(base + k, at, tiles, w)
                now.append(here)
                for t in range(tiles):
                    ref = basis_ref if t == 0 else side
                    value = 0.5 * out[t] if first else out[t] - ref[base + k - 1, pl.ds(at, 8), :]
                    ref[base + k + 1, pl.ds(at, 8), :] = value
                    if t == 0:
                        new.append(value)
            if last:
                now.append(basis_ref[STEPS + 1 + k, pl.ds(at, 8), :])
            if 1 <= g <= ROWS // 8:
                p, r = now
                total[0] += p * p
                total[1] += p * new[0]
                total[2] += r * r
                total[3] += new[0] * new[0] if last else r * new[1]
                total[4] += p * r
                total[5] += new[0] * r
        for i in range(6):
            acc[k, i, :, :] = total[i]
        acc[k, 6, :, :] = zero
        acc[k, 7, :, :] = zero

    step(0, True, False)

    def middle(k, carry):
        step(k, False, False)
        return carry

    lax.fori_loop(1, STEPS - 1, middle, 0)
    step(STEPS - 1, False, True)

    flat = jnp.sum(acc[...].reshape(8 * STEPS, 8, LANES), axis=1)
    flat = jnp.concatenate([flat, jnp.zeros_like(flat)], axis=0)
    row = lax.dot_general(
        jnp.ones((8, LANES), F32), flat, (((1,), (1,)), ((), ())),
        precision=lax.Precision.HIGHEST, preferred_element_type=F32,
    )
    for g in range(sums_ref.shape[0] // 8):
        sums_ref[pl.ds(8 * g, 8), :] = row


def middle_kernel(in_ref, out_ref):
    out_ref[...] = jnp.broadcast_to(jnp.sum(in_ref[...], axis=0, keepdims=True), out_ref.shape)


def final_kernel(sum_ref, basis_ref, height_ref, residual_ref):
    products = jnp.broadcast_to(jnp.sum(sum_ref[...], axis=0, keepdims=True), (8, LANES))
    row = lax.broadcasted_iota(jnp.int32, (24, LANES), 0)
    col = lax.broadcasted_iota(jnp.int32, (24, LANES), 1)
    half = STEPS + 1
    i = jnp.where(row < half, row, row - half)
    j = jnp.where(col < half, col, col - half)
    row_p, col_p = row < half, col < half
    inside = (row < VECTORS) & (col < VECTORS)
    total, apart = i + j, jnp.abs(i - j)
    even = (total & 1) == 0
    slot = jnp.where(row_p & col_p, 0, jnp.where(row_p | col_p, 4, 2))
    slot = slot + jnp.where(even, 0, 1)

    def gathered(index):
        index = jnp.where(inside, index, 6)
        parts = [
            jnp.take_along_axis(products, index[8 * g : 8 * g + 8], axis=1, mode="promise_in_bounds")
            for g in range(3)
        ]
        return jnp.concatenate(parts, axis=0)

    high = jnp.where(total == 2 * STEPS, 8 * (STEPS - 1) + 3, 8 * (total >> 1) + slot)
    gram = gathered(high) + gathered(8 * (apart >> 1) + slot) - gathered(slot)

    lead_r, lead_c = (row == 0) | (row == half), (col == 0) | (col == half)
    tail_r = (row == STEPS) | (row >= VECTORS - 1)
    tail_c = (col == STEPS) | (col >= VECTORS - 1)
    mapped = jnp.where(tail_c, 0.0, gram + jnp.where(lead_c, 1.0, 0.5) * pltpu.roll(gram, LANES - 1, 1)
                       + jnp.where(lead_c, 0.0, 0.5) * pltpu.roll(gram, 1, 1))
    same = (row_p == col_p) & inside & ~tail_r
    h_turned = jnp.where(same & (row == col), 1.0, 0.0)
    h_turned = h_turned + jnp.where(same & (col == row + 1), jnp.where(lead_r, 1.0, 0.5), 0.0)
    h_turned = h_turned + jnp.where(same & (col == row - 1) & ~lead_r, 0.5, 0.0)
    keep = jnp.where(tail_r, 0.0, 1.0)
    to_next = jnp.where(tail_r, 0.0, jnp.where(lead_r, 1.0, 0.5))
    to_last = jnp.where(tail_r | lead_r, 0.0, 0.5)

    def down(value):
        return jnp.sum(value, axis=0, keepdims=True)

    xc = jnp.zeros((24, LANES), F32)
    pc, rc = jnp.where(row == 0, 1.0, 0.0), jnp.where(row == half, 1.0, 0.0)
    p_row, r_row = jnp.where(col[:1] == 0, 1.0, 0.0), jnp.where(col[:1] == half, 1.0, 0.0)
    gr = jnp.broadcast_to(jnp.sum(gram * r_row, axis=1, keepdims=True), (24, LANES))
    norm = down(rc * gr)
    for _ in range(STEPS):
        z = jnp.broadcast_to(jnp.sum(mapped * p_row, axis=1, keepdims=True), (24, LANES))
        q_row = down(h_turned * pc)
        q_col = keep * pc + pltpu.roll(to_next * pc, 1, 0) + pltpu.roll(to_last * pc, 23, 0)
        t = norm / down(pc * z)
        xc = xc + t * pc
        rc = rc - t * q_col
        r_row = r_row - t * q_row
        gr = gr - t * z
        new = down(rc * gr)
        ratio = new / norm
        pc = rc + ratio * pc
        p_row = r_row + ratio * p_row
        norm = new
    xs = [jnp.broadcast_to(xc[k : k + 1, :], (8, LANES)) for k in range(VECTORS)]
    rs = [jnp.broadcast_to(rc[k : k + 1, :], (8, LANES)) for k in range(VECTORS)]
    for g in range(ROWS // 8):
        first = second = None
        for k in range(VECTORS):
            tile = basis_ref[k, pl.ds(16 + 8 * g, 8), :]
            first = xs[k] * tile if first is None else first + xs[k] * tile
            second = rs[k] * tile if second is None else second + rs[k] * tile
        height_ref[pl.ds(8 * g, 8), :] = first
        residual_ref[pl.ds(8 * g, 8), :] = second


def shape(*dims):
    return pltpu.VMEM(dims, F32)


def held(*values, space=pltpu.VMEM):
    return tuple(pltpu.with_memory_space_constraint(v, space) for v in values)


def limit(mib):
    return pltpu.CompilerParams(vmem_limit_bytes=mib << 20)


def per_device(forcing, search_direction, ocean_depth, land_mask, fold_map):
    lat_count, lon_count = lax.axis_size("lat"), lax.axis_size(LON)
    call = pl.pallas_call
    fields, first, second, reach, choice = call(
        functools.partial(pack_kernel, lon_count // 2), name="pack",
        in_specs=[pl.BlockSpec(memory_space=pl.ANY)] * 5,
        out_specs=[pl.BlockSpec(memory_space=pltpu.VMEM)] * 3 + [pl.BlockSpec(memory_space=pltpu.SMEM)] * 2,
        out_shape=(shape(3, ROWS, LANES), shape(BLK + 32, LANES), shape(BLK + 32, LANES),
                   pltpu.SMEM((1,), jnp.int32), pltpu.SMEM((1,), jnp.int32)),
        scratch_shapes=[pltpu.VMEM((ROWS, LANES), F32)] * 3 + [
            pltpu.VMEM((ROWS, LANES), jnp.int32), pltpu.SMEM((LANES,), jnp.int32), pltpu.SemaphoreType.DMA((5,)),
        ],
        compiler_params=limit(4),
    )(*held(forcing, search_direction, ocean_depth, land_mask, fold_map, space=pltpu.HBM))
    evens, odds = range(0, lon_count, 2), range(1, lon_count, 2)
    wrap = [(i, (i + 1) % lon_count) for i in odds]
    second = lax.ppermute(second, LON, wrap + [(b, a) for a, b in wrap])
    first = lax.ppermute(first, LON, [(i, i + 1) for i in evens] + [(i + 1, i) for i in evens])

    one, two, two_next = call(
        functools.partial(turn_kernel, lat_count - 1), name="turn",
        in_specs=[pl.BlockSpec(memory_space=pltpu.SMEM)] + [pl.BlockSpec(memory_space=pltpu.VMEM)] * 3,
        out_shape=(shape(64, LANES),) * 3,
        scratch_shapes=[pltpu.VMEM((BLK + 32, LANES), F32)] * 2 + [pltpu.VMEM((64, LANES), F32)] * 4,
        compiler_params=limit(4),
    )(reach, *held(fields, second, first))

    evens, odds = range(0, lat_count, 2), range(1, lat_count - 1, 2)
    pairs = [(i, i + 1) for i in evens] + [(i + 1, i) for i in evens]
    swaps = [
        (i * lon_count + c, (i + s) * lon_count + c)
        for k in odds for i, s in ((k, 1), (k + 1, -1)) for c in range(lon_count)
    ]
    top = (lat_count - 1) * lon_count

    def second_round(value, pairing):
        fold = [(top + i, top + (2 * pairing - i) % lon_count) for i in range(lon_count)]
        return lax.ppermute(value, ("lat",) + LON, swaps + fold)

    def branch(index):
        def exchange(one, near, far):
            value = second_round(near, index // 2)
            if index % 2:
                value = value + second_round(far, (index // 2 + 1) % (lon_count // 2))
            one = lax.ppermute(one, "lat", pairs)
            return call(
                land_kernel, name="land", out_shape=(shape(64, LANES),) * 2, compiler_params=limit(2),
            )(*held(value, one))

        return exchange

    south, north = lax.switch(choice[0], [branch(i) for i in range(lon_count)], one, two, two_next)

    basis, sums = call(
        basis_kernel, name="basis",
        out_shape=(shape(VECTORS, PITCH, LANES), shape(lon_count, LANES)),
        scratch_shapes=[
            pltpu.VMEM((2, PITCH, LANES), F32),
            pltpu.VMEM((VECTORS, PITCH, LANES), F32),
            pltpu.VMEM((2, PITCH, LANES), F32),
            pltpu.VMEM((2, 9, PITCH, LANES), F32),
            pltpu.VMEM((STEPS, 8, 8, LANES), F32),
        ] + [pltpu.VMEM((BLK + 32, LANES), F32)] * 2,
        compiler_params=limit(12),
    )(*held(fields, second, first, south, north))
    sums = lax.all_to_all(sums, LON, split_axis=0, concat_axis=0, tiled=True)
    sums = call(middle_kernel, name="middle", out_shape=shape(lat_count, LANES), compiler_params=limit(2))(*held(sums))
    sums = lax.all_to_all(sums, "lat", split_axis=0, concat_axis=0, tiled=True)
    return call(
        final_kernel, name="final", out_shape=(jax.ShapeDtypeStruct((ROWS, LANES), F32),) * 2,
        compiler_params=limit(4),
    )(*held(sums, basis))


def solution(mesh):
    lon = mesh.shape["lon"]
    split = Mesh(mesh.devices.reshape(mesh.shape["lat"], lon // 4, 4), ("lat", "lon_0", "lon_1"))
    return jax.shard_map(
        per_device,
        mesh=split,
        in_specs=(P("lat", LON), P("lat", LON), P("lat", LON), P("lat", LON), P()),
        out_specs=(P("lat", LON), P("lat", LON)),
        check_vma=False,
    )
```

```python
import functools

import jax
import jax.numpy as jnp
from jax import lax
from jax.experimental import pallas as pl
from jax.experimental.pallas import tpu as pltpu
from jax.sharding import Mesh
from jax.sharding import PartitionSpec as P

STEPS = 8
REACH = 256
ROWS = 160
LANES = 128
EXT = ROWS + 32
PITCH = 216
EDGE = 9
BLK = 40
LON = ("lon_0", "lon_1")
VECTORS = 2 * STEPS + 1
F32 = jnp.float32


def lanes_of(rows):
    return lax.broadcasted_iota(jnp.int32, (rows, LANES), 1)


def shift_east(a, b, lane):
    ra, rb = pltpu.roll(a, 1, 1), pltpu.roll(b, 1, 1)
    first = lane == 0
    return jnp.where(first, rb, ra), jnp.where(first, ra, rb)


def shift_west(a, b, lane):
    ra, rb = pltpu.roll(a, LANES - 1, 1), pltpu.roll(b, LANES - 1, 1)
    last = lane == LANES - 1
    return jnp.where(last, rb, ra), jnp.where(last, ra, rb)


def pack_kernel(pairs, f_hbm, p_hbm, d_hbm, m_hbm, map_hbm, x_ref, first_ref, second_ref, reach_ref, choice_ref,
                f_ref, p_ref, d_ref, m_ref, pivot, sems):
    even = lax.axis_index(LON) % 2 == 0
    copies = [
        pltpu.make_async_copy(source, target, sems.at[i])
        for i, (source, target) in enumerate((
            (m_hbm, m_ref), (d_hbm, d_ref), (f_hbm, f_ref), (p_hbm, p_ref), (map_hbm.at[pl.ds(0, LANES)], pivot),
        ))
    ]
    for copy in copies:
        copy.start()
    for copy in copies:
        copy.wait()
    for g in range(ROWS // 8):
        rows = pl.ds(8 * g, 8)
        flag = m_ref[rows, :].astype(F32)
        x_ref[0, rows, :] = d_ref[rows, :] * flag
        x_ref[1, rows, :] = f_ref[rows, :] * flag
        x_ref[2, rows, :] = p_ref[rows, :] * flag
    lane = lanes_of(8)
    for v in range(BLK // 8):
        east = jnp.zeros((8, LANES), F32)
        west = jnp.zeros((8, LANES), F32)
        for q in range(3):
            for blk in range(4):
                at = EDGE * (4 * q + blk)
                tile = x_ref[q, pl.ds(BLK * blk + 8 * v, 8), :]
                inside = (lane >= at) & (lane < at + EDGE)
                west = jnp.where(inside, pltpu.roll(tile, at, 1) if at else tile, west)
                east = jnp.where(inside, pltpu.roll(tile, (at + EDGE) % LANES, 1), east)
        first_ref[pl.ds(8 * v, 8), :] = jnp.where(even, east, west)
        second_ref[pl.ds(8 * v, 8), :] = jnp.where(even, west, east)
    for slot, (q, row) in enumerate(((0, ROWS - 8), (1, ROWS - 8), (2, ROWS - 8), (0, ROWS - 16))):
        tile = x_ref[q, pl.ds(row, 8), :]
        first_ref[pl.ds(BLK + 8 * slot, 8), :] = tile
        second_ref[pl.ds(BLK + 8 * slot, 8), :] = tile
    past = pivot[0] + (2 * pairs * LANES - 8)
    reach = past % (2 * LANES) + 8
    reach_ref[0] = reach
    split = jnp.where(reach + EDGE >= 2 * LANES, 1, 0)
    choice_ref[0] = 2 * ((past // (2 * LANES)) % pairs) + split


def unpack_halo(from_west, from_east, q, blk, v, lane):
    at = EDGE * (4 * q + blk)
    right = from_east[pl.ds(8 * v, 8), :]
    left = from_west[pl.ds(8 * v, 8), :]
    right = pltpu.roll(right, LANES - at, 1) if at else right
    left = pltpu.roll(left, (2 * LANES - EDGE - at) % LANES, 1)
    return jnp.where(lane < EDGE, right, jnp.where(lane >= LANES - EDGE, left, 0.0))


def sort_partners(axis, first, second, before, after):
    even = lax.axis_index(axis) % 2 == 0
    for g in range(first.shape[0] // 8):
        rows = pl.ds(8 * g, 8)
        a, b = first[rows, :], second[rows, :]
        before[rows, :] = jnp.where(even, b, a)
        after[rows, :] = jnp.where(even, a, b)


def turn_kernel(tops, r_ref, x_ref, second_ref, first_ref, one_ref, two_ref, next_ref,
                fw_ref, fe_ref, north_ref, south_ref, t1_ref, t2_ref):
    lane = lanes_of(8)
    lat = lax.axis_index("lat")
    even, top_row = lat % 2 == 0, lat == tops
    sort_partners(LON, first_ref, second_ref, fw_ref, fe_ref)
    top, low = ROWS // 8 - 1, 0
    for ref, rows in (
        (north_ref, ((0, top), (1, top), (2, top), (0, top - 1))),
        (south_ref, ((0, low), (1, low), (2, low), (0, low + 1))),
    ):
        for slot, (q, g) in enumerate(rows):
            ref[pl.ds(8 * slot, 8), :] = x_ref[q, pl.ds(8 * g, 8), :]
            blk, v = 8 * g // BLK, (8 * g % BLK) // 8
            ref[pl.ds(32 + 8 * slot, 8), :] = unpack_halo(fw_ref, fe_ref, q, blk, v, lane)
    for g in range(8):
        rows = pl.ds(8 * g, 8)
        north, south = north_ref[rows, :], south_ref[rows, :]
        one_ref[rows, :] = jnp.where(even, north, south)
        two_ref[rows, :] = jnp.where(even, south, north)
        next_ref[rows, :] = jnp.zeros((8, LANES), F32)

    @pl.when(top_row)
    def _():
        across_fold(r_ref[0], lane, north_ref, fw_ref, fe_ref, two_ref, next_ref, t1_ref, t2_ref)


def across_fold(reach, lane, north_ref, fw_ref, fe_ref, fold_ref, next_ref, t1_ref, t2_ref):
    along = reach - lane
    pick = along & (LANES - 1)
    place_a = along
    place_b = jnp.where(lane < EDGE, along - LANES, along + LANES)
    halo = (lane < EDGE) | (lane >= LANES - EDGE)
    for slot in range(4):
        rows = pl.ds(8 * slot, 8)
        own = jnp.take_along_axis(north_ref[rows, :], pick, axis=1, mode="promise_in_bounds")
        west = jnp.take_along_axis(fw_ref[pl.ds(BLK + 8 * slot, 8), :], pick, axis=1, mode="promise_in_bounds")
        east = jnp.take_along_axis(fe_ref[pl.ds(BLK + 8 * slot, 8), :], pick, axis=1, mode="promise_in_bounds")
        for part, place in ((0, place_a), (32, place_b)):
            near = jnp.where(place < 0, west, jnp.where(place < LANES, own, east))
            near = jnp.where(place < 2 * LANES, near, 0.0)
            far = jnp.where(place >= 2 * LANES, own, 0.0)
            if part:
                near = jnp.where(halo, near, 0.0)
                far = jnp.where(halo, far, 0.0)
            t1_ref[pl.ds(part + 8 * slot, 8), :] = near
            t2_ref[pl.ds(part + 8 * slot, 8), :] = far
    for g in range(8):
        for m in range(8):
            fold_ref[pl.ds(8 * g + m, 1), :] = t1_ref[pl.ds(8 * g + 7 - m, 1), :]
            next_ref[pl.ds(8 * g + m, 1), :] = t2_ref[pl.ds(8 * g + 7 - m, 1), :]


GROUPS = ROWS // 8 + 2


def root_of(depth, inv, at, lane):
    vert, mid, wet_mid, deep = [], [], [], []
    for t in range(2):
        down = depth[t, pl.ds(at - 1, 8), :]
        here = depth[t, pl.ds(at, 8), :]
        up = depth[t, pl.ds(at + 1, 8), :]
        wet = jnp.where(here > 0.0, 1.0, 0.0)
        wets = jnp.where(down > 0.0, 1.0, 0.0) + jnp.where(up > 0.0, 1.0, 0.0)
        vert.append((down + up, wets))
        mid.append((here + 0.5 * (down + up), wet + 0.5 * wets))
        deep.append(here)
        wet_mid.append(wet)
    sums = []
    for c in range(2):
        ea, eb = shift_east(mid[0][c], mid[1][c], lane)
        wa, wb = shift_west(mid[0][c], mid[1][c], lane)
        sums.append((vert[0][c] + (ea + wa), vert[1][c] + (eb + wb)))
    for t in range(2):
        links = 0.5 * (deep[t] * sums[1][t] + sums[0][t])
        diagonal = wet_mid[t] * (deep[t] / (REACH * REACH) + links) + (1.0 - wet_mid[t])
        inv[t, pl.ds(at, 8), :] = lax.rsqrt(diagonal) * wet_mid[t]


def coefs_of(depth, inv, coef, at, lane):
    d = [[depth[t, pl.ds(at + s, 8), :] for s in (-1, 0, 1)] for t in range(2)]
    r = [[inv[t, pl.ds(at + s, 8), :] for s in (-1, 0, 1)] for t in range(2)]
    de, re = shift_east(d[0][1], d[1][1], lane), shift_east(r[0][1], r[1][1], lane)
    dw, rw = shift_west(d[0][1], d[1][1], lane), shift_west(r[0][1], r[1][1], lane)
    for t in range(2):
        for base, (dc, rc) in enumerate(((d[t][1], r[t][1]), (de[t], re[t]), (dw[t], rw[t]))):
            for s in range(3):
                if base == 0 and s == 1:
                    continue
                whole = base == 0 or s == 1
                c = (dc + d[t][s]) * (rc * r[t][s])
                coef[t, 3 * base + s, pl.ds(at, 8), :] = c * (-1.0 if whole else -0.5)


def prepare_kernel(x_ref, second_ref, first_ref, depth, side, inv, coef, fw_ref, fe_ref):
    sort_partners(LON, first_ref, second_ref, fw_ref, fe_ref)
    lane = lanes_of(8)

    def unpack(v, carry):
        for q, ref in ((0, depth.at[1]), (1, side.at[1]), (2, side.at[0])):
            for blk in range(4):
                rows = pl.ds(pl.multiple_of(16 + BLK * blk + 8 * v, 8), 8)
                ref[rows, :] = unpack_halo(fw_ref, fe_ref, q, blk, v, lane)
        return carry

    for g in range(ROWS // 8):
        depth[0, pl.ds(16 + 8 * g, 8), :] = x_ref[0, pl.ds(8 * g, 8), :]
    lax.fori_loop(0, BLK // 8, unpack, 0)

    def roots(i, carry):
        for g in range(6):
            root_of(depth, inv, pl.multiple_of(24 + 48 * i, 8) + 8 * g, lane)
        return carry

    def coefs(i, carry):
        for g in range(4):
            coefs_of(depth, inv, coef, pl.multiple_of(32 + 32 * i, 8) + 8 * g, lane)
        return carry

    lax.fori_loop(0, 3, roots, 0)
    lax.fori_loop(0, 4, coefs, 0)


def land_kernel(two_ref, one_ref, south_ref, north_ref):
    sort_partners("lat", one_ref, two_ref, south_ref, north_ref)


def basis_kernel(x_ref, side_ref, _depth, _inv, _coef, fs_ref, fn_ref, basis_ref, sums_ref, depth, inv, coef,
                 side, acc):
    lane = lanes_of(8)
    zero = jnp.zeros((8, LANES), F32)
    for q, k in ((1, STEPS + 1), (2, 0)):
        for g in range(ROWS // 8):
            rows = pl.ds(16 + 8 * g, 8)
            basis_ref[k, rows, :] = x_ref[q, pl.ds(8 * g, 8), :]
            side[k, rows, :] = side_ref[2 - q, rows, :]
    targets = (
        lambda t: depth.at[t],
        lambda t: (basis_ref if t == 0 else side).at[STEPS + 1],
        lambda t: (basis_ref if t == 0 else side).at[0],
    )
    for q in range(3):
        own, rim = targets[q](0), targets[q](1)
        for t, ref in ((0, own), (1, rim)):
            at = 32 * t + 8 * q
            ref[pl.ds(8, 8), :] = fs_ref[pl.ds(at, 8), :]
            ref[pl.ds(EXT - 16, 8), :] = fn_ref[pl.ds(at, 8), :]
            if q == 0:
                at = 32 * t + 24
                ref[pl.ds(0, 8), :] = fs_ref[pl.ds(at, 8), :]
                ref[pl.ds(EXT - 8, 8), :] = fn_ref[pl.ds(at, 8), :]
            else:
                ref[pl.ds(0, 8), :] = zero
                ref[pl.ds(EXT - 8, 8), :] = zero
    for k in list(range(1, STEPS + 1)) + list(range(STEPS + 2, VECTORS)):
        for ref in (basis_ref, side):
            ref[k, pl.ds(0, 8), :] = zero
            ref[k, pl.ds(EXT - 8, 8), :] = zero
    for t in range(2):
        inv[t, pl.ds(0, 8), :] = zero
        inv[t, pl.ds(EXT - 8, 8), :] = zero

    for g in (0, 1, GROUPS - 2, GROUPS - 1):
        root_of(depth, inv, 8 + 8 * g, lane)
    for g in (0, 1, 2, GROUPS - 3, GROUPS - 2, GROUPS - 1):
        coefs_of(depth, inv, coef, 8 + 8 * g, lane)

    def twice_applied(k, at, tiles, weights):
        parts = []
        for t in range(2):
            ref = basis_ref if t == 0 else side
            down, here, up = (ref[k, pl.ds(at + s, 8), :] for s in (-1, 0, 1))
            w = weights[t]
            straight = w[0] * down + w[2] * up
            toward_w = (w[3] * down + w[5] * up) + w[4] * here
            toward_e = (w[6] * down + w[8] * up) + w[7] * here
            parts.append((straight, toward_w, toward_e, here))
        wa, wb = shift_west(parts[0][1], parts[1][1], lane)
        ea, eb = shift_east(parts[0][2], parts[1][2], lane)
        return ((parts[0][0] + (wa + ea), parts[1][0] + (wb + eb))[:tiles], parts[0][3])

    def weights_at(at):
        return [[None if i == 1 else coef[t, i, pl.ds(at, 8), :] for i in range(9)] for t in range(2)]

    def step(k, first, last):
        total = [zero] * 6
        tiles = 1 if last else 2
        for g in range(1, GROUPS - 1) if last else range(GROUPS):
            at = 8 + 8 * g
            w = weights_at(at)
            now, new = [], []
            for base in ((0,) if last else (0, STEPS + 1)):
                out, here = twice_applied(base + k, at, tiles, w)
                now.append(here)
                for t in range(tiles):
                    ref = basis_ref if t == 0 else side
                    value = 0.5 * out[t] if first else out[t] - ref[base + k - 1, pl.ds(at, 8), :]
                    ref[base + k + 1, pl.ds(at, 8), :] = value
                    if t == 0:
                        new.append(value)
            if last:
                now.append(basis_ref[STEPS + 1 + k, pl.ds(at, 8), :])
            if 1 <= g <= ROWS // 8:
                p, r = now
                total[0] += p * p
                total[1] += p * new[0]
                total[2] += r * r
                total[3] += new[0] * new[0] if last else r * new[1]
                total[4] += p * r
                total[5] += new[0] * r
        for i in range(6):
            acc[k, i, :, :] = total[i]
        acc[k, 6, :, :] = zero
        acc[k, 7, :, :] = zero

    step(0, True, False)

    def middle(k, carry):
        step(k, False, False)
        return carry

    lax.fori_loop(1, STEPS - 1, middle, 0)
    step(STEPS - 1, False, True)

    flat = jnp.sum(acc[...].reshape(8 * STEPS, 8, LANES), axis=1)
    flat = jnp.concatenate([flat, jnp.zeros_like(flat)], axis=0)
    row = lax.dot_general(
        jnp.ones((8, LANES), F32), flat, (((1,), (1,)), ((), ())),
        precision=lax.Precision.HIGHEST, preferred_element_type=F32,
    )
    for g in range(sums_ref.shape[0] // 8):
        sums_ref[pl.ds(8 * g, 8), :] = row


def middle_kernel(in_ref, out_ref):
    out_ref[...] = jnp.broadcast_to(jnp.sum(in_ref[...], axis=0, keepdims=True), out_ref.shape)


def final_kernel(sum_ref, basis_ref, height_ref, residual_ref):
    products = jnp.broadcast_to(jnp.sum(sum_ref[...], axis=0, keepdims=True), (8, LANES))
    row = lax.broadcasted_iota(jnp.int32, (24, LANES), 0)
    col = lax.broadcasted_iota(jnp.int32, (24, LANES), 1)
    half = STEPS + 1
    i = jnp.where(row < half, row, row - half)
    j = jnp.where(col < half, col, col - half)
    row_p, col_p = row < half, col < half
    inside = (row < VECTORS) & (col < VECTORS)
    total, apart = i + j, jnp.abs(i - j)
    even = (total & 1) == 0
    slot = jnp.where(row_p & col_p, 0, jnp.where(row_p | col_p, 4, 2))
    slot = slot + jnp.where(even, 0, 1)

    def gathered(index):
        index = jnp.where(inside, index, 6)
        parts = [
            jnp.take_along_axis(products, index[8 * g : 8 * g + 8], axis=1, mode="promise_in_bounds")
            for g in range(3)
        ]
        return jnp.concatenate(parts, axis=0)

    high = jnp.where(total == 2 * STEPS, 8 * (STEPS - 1) + 3, 8 * (total >> 1) + slot)
    gram = gathered(high) + gathered(8 * (apart >> 1) + slot) - gathered(slot)

    lead_r, lead_c = (row == 0) | (row == half), (col == 0) | (col == half)
    tail_r = (row == STEPS) | (row >= VECTORS - 1)
    tail_c = (col == STEPS) | (col >= VECTORS - 1)
    mapped = jnp.where(tail_c, 0.0, gram + jnp.where(lead_c, 1.0, 0.5) * pltpu.roll(gram, LANES - 1, 1)
                       + jnp.where(lead_c, 0.0, 0.5) * pltpu.roll(gram, 1, 1))
    same = (row_p == col_p) & inside & ~tail_r
    h_turned = jnp.where(same & (row == col), 1.0, 0.0)
    h_turned = h_turned + jnp.where(same & (col == row + 1), jnp.where(lead_r, 1.0, 0.5), 0.0)
    h_turned = h_turned + jnp.where(same & (col == row - 1) & ~lead_r, 0.5, 0.0)
    keep = jnp.where(tail_r, 0.0, 1.0)
    to_next = jnp.where(tail_r, 0.0, jnp.where(lead_r, 1.0, 0.5))
    to_last = jnp.where(tail_r | lead_r, 0.0, 0.5)

    def down(value):
        return jnp.sum(value, axis=0, keepdims=True)

    xc = jnp.zeros((24, LANES), F32)
    pc, rc = jnp.where(row == 0, 1.0, 0.0), jnp.where(row == half, 1.0, 0.0)
    p_row, r_row = jnp.where(col[:1] == 0, 1.0, 0.0), jnp.where(col[:1] == half, 1.0, 0.0)
    gr = jnp.broadcast_to(jnp.sum(gram * r_row, axis=1, keepdims=True), (24, LANES))
    norm = down(rc * gr)
    for _ in range(STEPS):
        z = jnp.broadcast_to(jnp.sum(mapped * p_row, axis=1, keepdims=True), (24, LANES))
        q_row = down(h_turned * pc)
        q_col = keep * pc + pltpu.roll(to_next * pc, 1, 0) + pltpu.roll(to_last * pc, 23, 0)
        t = norm / down(pc * z)
        xc = xc + t * pc
        rc = rc - t * q_col
        r_row = r_row - t * q_row
        gr = gr - t * z
        new = down(rc * gr)
        ratio = new / norm
        pc = rc + ratio * pc
        p_row = r_row + ratio * p_row
        norm = new
    xs = [jnp.broadcast_to(xc[k : k + 1, :], (8, LANES)) for k in range(VECTORS)]
    rs = [jnp.broadcast_to(rc[k : k + 1, :], (8, LANES)) for k in range(VECTORS)]
    for g in range(ROWS // 8):
        first = second = None
        for k in range(VECTORS):
            tile = basis_ref[k, pl.ds(16 + 8 * g, 8), :]
            first = xs[k] * tile if first is None else first + xs[k] * tile
            second = rs[k] * tile if second is None else second + rs[k] * tile
        height_ref[pl.ds(8 * g, 8), :] = first
        residual_ref[pl.ds(8 * g, 8), :] = second


def shape(*dims):
    return pltpu.VMEM(dims, F32)


def held(*values, space=pltpu.VMEM):
    return tuple(pltpu.with_memory_space_constraint(v, space) for v in values)


def limit(mib):
    return pltpu.CompilerParams(vmem_limit_bytes=mib << 20)


def per_device(forcing, search_direction, ocean_depth, land_mask, fold_map):
    lat_count, lon_count = lax.axis_size("lat"), lax.axis_size(LON)
    call = pl.pallas_call
    fields, first, second, reach, choice = call(
        functools.partial(pack_kernel, lon_count // 2), name="pack",
        in_specs=[pl.BlockSpec(memory_space=pl.ANY)] * 5,
        out_specs=[pl.BlockSpec(memory_space=pltpu.VMEM)] * 3 + [pl.BlockSpec(memory_space=pltpu.SMEM)] * 2,
        out_shape=(shape(3, ROWS, LANES), shape(BLK + 32, LANES), shape(BLK + 32, LANES),
                   pltpu.SMEM((1,), jnp.int32), pltpu.SMEM((1,), jnp.int32)),
        scratch_shapes=[pltpu.VMEM((ROWS, LANES), F32)] * 3 + [
            pltpu.VMEM((ROWS, LANES), jnp.int32), pltpu.SMEM((LANES,), jnp.int32), pltpu.SemaphoreType.DMA((5,)),
        ],
        compiler_params=limit(4),
    )(*held(forcing, search_direction, ocean_depth, land_mask, fold_map, space=pltpu.HBM))
    evens, odds = range(0, lon_count, 2), range(1, lon_count, 2)
    wrap = [(i, (i + 1) % lon_count) for i in odds]
    second = lax.ppermute(second, LON, wrap + [(b, a) for a, b in wrap])
    first = lax.ppermute(first, LON, [(i, i + 1) for i in evens] + [(i + 1, i) for i in evens])

    one, two, two_next = call(
        functools.partial(turn_kernel, lat_count - 1), name="turn",
        in_specs=[pl.BlockSpec(memory_space=pltpu.SMEM)] + [pl.BlockSpec(memory_space=pltpu.VMEM)] * 3,
        out_shape=(shape(64, LANES),) * 3,
        scratch_shapes=[pltpu.VMEM((BLK + 32, LANES), F32)] * 2 + [pltpu.VMEM((64, LANES), F32)] * 4,
        compiler_params=limit(4),
    )(reach, *held(fields, second, first))

    evens, odds = range(0, lat_count, 2), range(1, lat_count - 1, 2)
    pairs = [(i, i + 1) for i in evens] + [(i + 1, i) for i in evens]
    swaps = [
        (i * lon_count + c, (i + s) * lon_count + c)
        for k in odds for i, s in ((k, 1), (k + 1, -1)) for c in range(lon_count)
    ]
    top = (lat_count - 1) * lon_count

    def second_round(value, pairing):
        fold = [(top + i, top + (2 * pairing - i) % lon_count) for i in range(lon_count)]
        return lax.ppermute(value, ("lat",) + LON, swaps + fold)

    def branch(index):
        def exchange(one, near, far, fields, second, first):
            value = second_round(near, index // 2)
            if index % 2:
                value = value + second_round(far, (index // 2 + 1) % (lon_count // 2))
            one = lax.ppermute(one, "lat", pairs)
            ready = call(
                prepare_kernel, name="prepare",
                out_shape=(shape(2, PITCH, LANES), shape(2, PITCH, LANES), shape(2, PITCH, LANES),
                           shape(2, 9, PITCH, LANES)),
                scratch_shapes=[pltpu.VMEM((BLK + 32, LANES), F32)] * 2,
                compiler_params=limit(4),
                cost_estimate=pl.CostEstimate(flops=4_000_000, transcendentals=0, bytes_accessed=0),
            )(*held(fields, second, first))
            landed = call(
                land_kernel, name="land", out_shape=(shape(64, LANES),) * 2, compiler_params=limit(2),
            )(*held(value, one))
            return *ready, *landed

        return exchange

    depth, side, inv, coef, south, north = lax.switch(
        choice[0], [branch(i) for i in range(lon_count)], one, two, two_next, fields, second, first
    )

    basis, sums, *_ = call(
        basis_kernel, name="basis",
        out_shape=(shape(VECTORS, PITCH, LANES), shape(lon_count, LANES), shape(2, PITCH, LANES),
                   shape(2, PITCH, LANES), shape(2, 9, PITCH, LANES)),
        scratch_shapes=[
            pltpu.VMEM((VECTORS, PITCH, LANES), F32),
            pltpu.VMEM((STEPS, 8, 8, LANES), F32),
        ],
        input_output_aliases={2: 2, 3: 3, 4: 4},
        compiler_params=limit(12),
    )(*held(fields, side, depth, inv, coef, south, north))
    sums = lax.all_to_all(sums, LON, split_axis=0, concat_axis=0, tiled=True)
    sums = call(middle_kernel, name="middle", out_shape=shape(lat_count, LANES), compiler_params=limit(2))(*held(sums))
    sums = lax.all_to_all(sums, "lat", split_axis=0, concat_axis=0, tiled=True)
    return call(
        final_kernel, name="final", out_shape=(jax.ShapeDtypeStruct((ROWS, LANES), F32),) * 2,
        compiler_params=limit(4),
    )(*held(sums, basis))


def solution(mesh):
    lon = mesh.shape["lon"]
    split = Mesh(mesh.devices.reshape(mesh.shape["lat"], lon // 4, 4), ("lat", "lon_0", "lon_1"))
    return jax.shard_map(
        per_device,
        mesh=split,
        in_specs=(P("lat", LON), P("lat", LON), P("lat", LON), P("lat", LON), P()),
        out_specs=(P("lat", LON), P("lat", LON)),
        check_vma=False,
    )
```

```python
import functools

import jax
import jax.numpy as jnp
from jax import lax
from jax.experimental import pallas as pl
from jax.experimental.pallas import tpu as pltpu
from jax.sharding import Mesh
from jax.sharding import PartitionSpec as P

STEPS = 8
REACH = 256
ROWS = 160
LANES = 128
EXT = ROWS + 32
PITCH = 216
EDGE = 9
BLK = 40
LON = ("lon_0", "lon_1")
VECTORS = 2 * STEPS + 1
F32 = jnp.float32


def lanes_of(rows):
    return lax.broadcasted_iota(jnp.int32, (rows, LANES), 1)


def shift_east(a, b, lane):
    ra, rb = pltpu.roll(a, 1, 1), pltpu.roll(b, 1, 1)
    first = lane == 0
    return jnp.where(first, rb, ra), jnp.where(first, ra, rb)


def shift_west(a, b, lane):
    ra, rb = pltpu.roll(a, LANES - 1, 1), pltpu.roll(b, LANES - 1, 1)
    last = lane == LANES - 1
    return jnp.where(last, rb, ra), jnp.where(last, ra, rb)


def pack_kernel(pairs, f_hbm, p_hbm, d_hbm, m_hbm, map_hbm, x_ref, first_ref, second_ref, reach_ref, choice_ref,
                f_ref, p_ref, d_ref, m_ref, pivot, sems):
    even = lax.axis_index(LON) % 2 == 0
    copies = [
        pltpu.make_async_copy(source, target, sems.at[i])
        for i, (source, target) in enumerate((
            (m_hbm, m_ref), (d_hbm, d_ref), (f_hbm, f_ref), (p_hbm, p_ref), (map_hbm.at[pl.ds(0, LANES)], pivot),
        ))
    ]
    for copy in copies:
        copy.start()
    for copy in copies:
        copy.wait()
    for g in range(ROWS // 8):
        rows = pl.ds(8 * g, 8)
        flag = m_ref[rows, :].astype(F32)
        x_ref[0, rows, :] = d_ref[rows, :] * flag
        x_ref[1, rows, :] = f_ref[rows, :] * flag
        x_ref[2, rows, :] = p_ref[rows, :] * flag
    lane = lanes_of(8)
    for v in range(BLK // 8):
        east = jnp.zeros((8, LANES), F32)
        west = jnp.zeros((8, LANES), F32)
        for q in range(3):
            for blk in range(4):
                at = EDGE * (4 * q + blk)
                tile = x_ref[q, pl.ds(BLK * blk + 8 * v, 8), :]
                inside = (lane >= at) & (lane < at + EDGE)
                west = jnp.where(inside, pltpu.roll(tile, at, 1) if at else tile, west)
                east = jnp.where(inside, pltpu.roll(tile, (at + EDGE) % LANES, 1), east)
        first_ref[pl.ds(8 * v, 8), :] = jnp.where(even, east, west)
        second_ref[pl.ds(8 * v, 8), :] = jnp.where(even, west, east)
    for slot, (q, row) in enumerate(((0, ROWS - 8), (1, ROWS - 8), (2, ROWS - 8), (0, ROWS - 16))):
        tile = x_ref[q, pl.ds(row, 8), :]
        first_ref[pl.ds(BLK + 8 * slot, 8), :] = tile
        second_ref[pl.ds(BLK + 8 * slot, 8), :] = tile
    past = pivot[0] + (2 * pairs * LANES - 8)
    reach = past % (2 * LANES) + 8
    reach_ref[0] = reach
    split = jnp.where(reach + EDGE >= 2 * LANES, 1, 0)
    choice_ref[0] = 2 * ((past // (2 * LANES)) % pairs) + split


def unpack_halo(from_west, from_east, q, blk, v, lane):
    at = EDGE * (4 * q + blk)
    right = from_east[pl.ds(8 * v, 8), :]
    left = from_west[pl.ds(8 * v, 8), :]
    right = pltpu.roll(right, LANES - at, 1) if at else right
    left = pltpu.roll(left, (2 * LANES - EDGE - at) % LANES, 1)
    return jnp.where(lane < EDGE, right, jnp.where(lane >= LANES - EDGE, left, 0.0))


def sort_partners(axis, first, second, before, after):
    even = lax.axis_index(axis) % 2 == 0
    for g in range(first.shape[0] // 8):
        rows = pl.ds(8 * g, 8)
        a, b = first[rows, :], second[rows, :]
        before[rows, :] = jnp.where(even, b, a)
        after[rows, :] = jnp.where(even, a, b)


def turn_kernel(tops, r_ref, x_ref, second_ref, first_ref, one_ref, two_ref, next_ref,
                fw_ref, fe_ref, north_ref, south_ref, t1_ref, t2_ref):
    lane = lanes_of(8)
    lat = lax.axis_index("lat")
    even, top_row = lat % 2 == 0, lat == tops
    sort_partners(LON, first_ref, second_ref, fw_ref, fe_ref)
    top, low = ROWS // 8 - 1, 0
    for ref, rows in (
        (north_ref, ((0, top), (1, top), (2, top), (0, top - 1))),
        (south_ref, ((0, low), (1, low), (2, low), (0, low + 1))),
    ):
        for slot, (q, g) in enumerate(rows):
            ref[pl.ds(8 * slot, 8), :] = x_ref[q, pl.ds(8 * g, 8), :]
            blk, v = 8 * g // BLK, (8 * g % BLK) // 8
            ref[pl.ds(32 + 8 * slot, 8), :] = unpack_halo(fw_ref, fe_ref, q, blk, v, lane)
    for g in range(8):
        rows = pl.ds(8 * g, 8)
        north, south = north_ref[rows, :], south_ref[rows, :]
        one_ref[rows, :] = jnp.where(even, north, south)
        two_ref[rows, :] = jnp.where(even, south, north)
        next_ref[rows, :] = jnp.zeros((8, LANES), F32)

    @pl.when(top_row)
    def _():
        across_fold(r_ref[0], lane, north_ref, fw_ref, fe_ref, two_ref, next_ref, t1_ref, t2_ref)


def across_fold(reach, lane, north_ref, fw_ref, fe_ref, fold_ref, next_ref, t1_ref, t2_ref):
    along = reach - lane
    pick = along & (LANES - 1)
    place_a = along
    place_b = jnp.where(lane < EDGE, along - LANES, along + LANES)
    halo = (lane < EDGE) | (lane >= LANES - EDGE)
    for slot in range(4):
        rows = pl.ds(8 * slot, 8)
        own = jnp.take_along_axis(north_ref[rows, :], pick, axis=1, mode="promise_in_bounds")
        west = jnp.take_along_axis(fw_ref[pl.ds(BLK + 8 * slot, 8), :], pick, axis=1, mode="promise_in_bounds")
        east = jnp.take_along_axis(fe_ref[pl.ds(BLK + 8 * slot, 8), :], pick, axis=1, mode="promise_in_bounds")
        for part, place in ((0, place_a), (32, place_b)):
            near = jnp.where(place < 0, west, jnp.where(place < LANES, own, east))
            near = jnp.where(place < 2 * LANES, near, 0.0)
            far = jnp.where(place >= 2 * LANES, own, 0.0)
            if part:
                near = jnp.where(halo, near, 0.0)
                far = jnp.where(halo, far, 0.0)
            t1_ref[pl.ds(part + 8 * slot, 8), :] = near
            t2_ref[pl.ds(part + 8 * slot, 8), :] = far
    for g in range(8):
        for m in range(8):
            fold_ref[pl.ds(8 * g + m, 1), :] = t1_ref[pl.ds(8 * g + 7 - m, 1), :]
            next_ref[pl.ds(8 * g + m, 1), :] = t2_ref[pl.ds(8 * g + 7 - m, 1), :]


GROUPS = ROWS // 8 + 2


def root_of(depth, inv, at, lane):
    vert, mid, wet_mid, deep = [], [], [], []
    for t in range(2):
        down = depth[t, pl.ds(at - 1, 8), :]
        here = depth[t, pl.ds(at, 8), :]
        up = depth[t, pl.ds(at + 1, 8), :]
        wet = jnp.where(here > 0.0, 1.0, 0.0)
        wets = jnp.where(down > 0.0, 1.0, 0.0) + jnp.where(up > 0.0, 1.0, 0.0)
        vert.append((down + up, wets))
        mid.append((here + 0.5 * (down + up), wet + 0.5 * wets))
        deep.append(here)
        wet_mid.append(wet)
    sums = []
    for c in range(2):
        ea, eb = shift_east(mid[0][c], mid[1][c], lane)
        wa, wb = shift_west(mid[0][c], mid[1][c], lane)
        sums.append((vert[0][c] + (ea + wa), vert[1][c] + (eb + wb)))
    for t in range(2):
        links = 0.5 * (deep[t] * sums[1][t] + sums[0][t])
        diagonal = wet_mid[t] * (deep[t] / (REACH * REACH) + links) + (1.0 - wet_mid[t])
        inv[t, pl.ds(at, 8), :] = lax.rsqrt(diagonal) * wet_mid[t]


def coefs_of(depth, inv, coef, at, lane):
    d = [[depth[t, pl.ds(at + s, 8), :] for s in (-1, 0, 1)] for t in range(2)]
    r = [[inv[t, pl.ds(at + s, 8), :] for s in (-1, 0, 1)] for t in range(2)]
    de, re = shift_east(d[0][1], d[1][1], lane), shift_east(r[0][1], r[1][1], lane)
    dw, rw = shift_west(d[0][1], d[1][1], lane), shift_west(r[0][1], r[1][1], lane)
    for t in range(2):
        for base, (dc, rc) in enumerate(((d[t][1], r[t][1]), (de[t], re[t]), (dw[t], rw[t]))):
            for s in range(3):
                if base == 0 and s == 1:
                    continue
                whole = base == 0 or s == 1
                c = (dc + d[t][s]) * (rc * r[t][s])
                coef[t, 3 * base + s, pl.ds(at, 8), :] = c * (-1.0 if whole else -0.5)


def prepare_kernel(x_ref, second_ref, first_ref, depth, side, inv, coef, fw_ref, fe_ref):
    sort_partners(LON, first_ref, second_ref, fw_ref, fe_ref)
    lane = lanes_of(8)

    def unpack(v, carry):
        for q, ref in ((0, depth.at[1]), (1, side.at[1]), (2, side.at[0])):
            for blk in range(4):
                rows = pl.ds(pl.multiple_of(16 + BLK * blk + 8 * v, 8), 8)
                ref[rows, :] = unpack_halo(fw_ref, fe_ref, q, blk, v, lane)
        return carry

    for g in range(ROWS // 8):
        depth[0, pl.ds(16 + 8 * g, 8), :] = x_ref[0, pl.ds(8 * g, 8), :]
    lax.fori_loop(0, BLK // 8, unpack, 0)

    def roots(i, carry):
        for g in range(6):
            root_of(depth, inv, pl.multiple_of(24 + 48 * i, 8) + 8 * g, lane)
        return carry

    def coefs(i, carry):
        for g in range(4):
            coefs_of(depth, inv, coef, pl.multiple_of(32 + 32 * i, 8) + 8 * g, lane)
        return carry

    lax.fori_loop(0, 3, roots, 0)
    lax.fori_loop(0, 4, coefs, 0)


def land_kernel(two_ref, one_ref, south_ref, north_ref):
    sort_partners("lat", one_ref, two_ref, south_ref, north_ref)


def basis_kernel(x_ref, side_ref, _depth, _inv, _coef, fs_ref, fn_ref, basis_ref, sums_ref, depth, inv, coef,
                 side, acc):
    lane = lanes_of(8)
    zero = jnp.zeros((8, LANES), F32)
    for q, k in ((1, STEPS + 1), (2, 0)):
        for g in range(ROWS // 8):
            rows = pl.ds(16 + 8 * g, 8)
            basis_ref[k, rows, :] = x_ref[q, pl.ds(8 * g, 8), :]
            side[k, rows, :] = side_ref[2 - q, rows, :]
    targets = (
        lambda t: depth.at[t],
        lambda t: (basis_ref if t == 0 else side).at[STEPS + 1],
        lambda t: (basis_ref if t == 0 else side).at[0],
    )
    for q in range(3):
        own, rim = targets[q](0), targets[q](1)
        for t, ref in ((0, own), (1, rim)):
            at = 32 * t + 8 * q
            ref[pl.ds(8, 8), :] = fs_ref[pl.ds(at, 8), :]
            ref[pl.ds(EXT - 16, 8), :] = fn_ref[pl.ds(at, 8), :]
            if q == 0:
                at = 32 * t + 24
                ref[pl.ds(0, 8), :] = fs_ref[pl.ds(at, 8), :]
                ref[pl.ds(EXT - 8, 8), :] = fn_ref[pl.ds(at, 8), :]
            else:
                ref[pl.ds(0, 8), :] = zero
                ref[pl.ds(EXT - 8, 8), :] = zero
    for k in list(range(1, STEPS + 1)) + list(range(STEPS + 2, VECTORS)):
        for ref in (basis_ref, side):
            ref[k, pl.ds(0, 8), :] = zero
            ref[k, pl.ds(EXT - 8, 8), :] = zero
    for t in range(2):
        inv[t, pl.ds(0, 8), :] = zero
        inv[t, pl.ds(EXT - 8, 8), :] = zero

    for g in (0, 1, GROUPS - 2, GROUPS - 1):
        root_of(depth, inv, 8 + 8 * g, lane)
    for g in (0, 1, 2, GROUPS - 3, GROUPS - 2, GROUPS - 1):
        coefs_of(depth, inv, coef, 8 + 8 * g, lane)

    def twice_applied(k, at, tiles, weights):
        parts = []
        for t in range(2):
            ref = basis_ref if t == 0 else side
            down, here, up = (ref[k, pl.ds(at + s, 8), :] for s in (-1, 0, 1))
            w = weights[t]
            straight = w[0] * down + w[2] * up
            toward_w = (w[3] * down + w[5] * up) + w[4] * here
            toward_e = (w[6] * down + w[8] * up) + w[7] * here
            parts.append((straight, toward_w, toward_e, here))
        wa, wb = shift_west(parts[0][1], parts[1][1], lane)
        ea, eb = shift_east(parts[0][2], parts[1][2], lane)
        return ((parts[0][0] + (wa + ea), parts[1][0] + (wb + eb))[:tiles], parts[0][3])

    def weights_at(at):
        return [[None if i == 1 else coef[t, i, pl.ds(at, 8), :] for i in range(9)] for t in range(2)]

    def step(k, first, last):
        total = [zero] * 6
        tiles = 1 if last else 2
        for g in range(1, GROUPS - 1) if last else range(GROUPS):
            at = 8 + 8 * g
            w = weights_at(at)
            now, new = [], []
            for base in ((0,) if last else (0, STEPS + 1)):
                out, here = twice_applied(base + k, at, tiles, w)
                now.append(here)
                for t in range(tiles):
                    ref = basis_ref if t == 0 else side
                    value = 0.5 * out[t] if first else out[t] - ref[base + k - 1, pl.ds(at, 8), :]
                    ref[base + k + 1, pl.ds(at, 8), :] = value
                    if t == 0:
                        new.append(value)
            if last:
                now.append(basis_ref[STEPS + 1 + k, pl.ds(at, 8), :])
            if 1 <= g <= ROWS // 8:
                p, r = now
                total[0] += p * p
                total[1] += p * new[0]
                total[2] += r * r
                total[3] += new[0] * new[0] if last else r * new[1]
                total[4] += p * r
                total[5] += new[0] * r
        for i in range(6):
            acc[k, i, :, :] = total[i]
        acc[k, 6, :, :] = zero
        acc[k, 7, :, :] = zero

    step(0, True, False)

    def middle(k, carry):
        step(k, False, False)
        return carry

    lax.fori_loop(1, STEPS - 1, middle, 0)
    step(STEPS - 1, False, True)

    flat = jnp.sum(acc[...].reshape(8 * STEPS, 8, LANES), axis=1)
    flat = jnp.concatenate([flat, jnp.zeros_like(flat)], axis=0)
    row = lax.dot_general(
        jnp.ones((8, LANES), F32), flat, (((1,), (1,)), ((), ())),
        precision=lax.Precision.HIGHEST, preferred_element_type=F32,
    )
    for g in range(sums_ref.shape[0] // 8):
        sums_ref[pl.ds(8 * g, 8), :] = row


def middle_kernel(in_ref, out_ref):
    out_ref[...] = jnp.broadcast_to(jnp.sum(in_ref[...], axis=0, keepdims=True), out_ref.shape)


def final_kernel(sum_ref, basis_ref, height_ref, residual_ref):
    products = jnp.broadcast_to(jnp.sum(sum_ref[...], axis=0, keepdims=True), (8, LANES))
    row = lax.broadcasted_iota(jnp.int32, (24, LANES), 0)
    first = row == 0
    odd = row & 1

    def gathered(index):
        parts = [
            jnp.take_along_axis(products, index[8 * g : 8 * g + 8], axis=1, mode="promise_in_bounds")
            for g in range(3)
        ]
        return jnp.concatenate(parts, axis=0)

    def moments(slot, count):
        index = jnp.where(row < count, 8 * (row >> 1) + odd + slot, 6)
        if count > 2 * STEPS:
            index = jnp.where(row == 2 * STEPS, 8 * (STEPS - 1) + 3, index)
        return 2.0 * gathered(index) - gathered(jnp.where(row < count, odd + slot, 6))

    def raised(v):
        up = pltpu.roll(v, 23, 0)
        return v + 0.5 * (up + jnp.where(first, up, pltpu.roll(v, 1, 0)))

    def mapped(v):
        down = pltpu.roll(jnp.where(first, v, 0.5 * v), 1, 0)
        return v + down + pltpu.roll(jnp.where(first, 0.0, 0.5 * v), 23, 0)

    def dot(u, v):
        return jnp.sum(u[0] * v[0] + u[1] * v[1], axis=0, keepdims=True)

    pair = (0, 1)
    unit, zero = jnp.where(first, 1.0, 0.0), jnp.zeros((24, LANES), F32)
    pp, rr, pr = moments(0, 2 * STEPS + 1), moments(2, 2 * STEPS - 1), moments(4, 2 * STEPS)
    xc, pc, rc = (zero, zero), (unit, zero), (zero, unit)
    with_r, with_q = (pr, rr), (raised(pp), raised(pr))
    norm = dot(rc, with_r)
    for _ in range(STEPS):
        t = norm / dot(pc, with_q)
        inverse = 1.0 / norm
        with_r = [with_r[i] - t * with_q[i] for i in pair]
        rc, xc = [rc[i] - t * mapped(pc[i]) for i in pair], [xc[i] + t * pc[i] for i in pair]
        norm = dot(rc, with_r)
        ratio = norm * inverse
        with_q = [raised(with_r[i]) + ratio * with_q[i] for i in pair]
        pc = [rc[i] + ratio * pc[i] for i in pair]
    spots = [(0, k) for k in range(STEPS + 1)] + [(1, k) for k in range(STEPS)]
    xs = [jnp.broadcast_to(xc[i][k : k + 1, :], (8, LANES)) for i, k in spots]
    rs = [jnp.broadcast_to(rc[i][k : k + 1, :], (8, LANES)) for i, k in spots]
    for g in range(ROWS // 8):
        first = second = None
        for k in range(VECTORS):
            tile = basis_ref[k, pl.ds(16 + 8 * g, 8), :]
            first = xs[k] * tile if first is None else first + xs[k] * tile
            second = rs[k] * tile if second is None else second + rs[k] * tile
        height_ref[pl.ds(8 * g, 8), :] = first
        residual_ref[pl.ds(8 * g, 8), :] = second


def shape(*dims):
    return pltpu.VMEM(dims, F32)


def held(*values, space=pltpu.VMEM):
    return tuple(pltpu.with_memory_space_constraint(v, space) for v in values)


def limit(mib):
    return pltpu.CompilerParams(vmem_limit_bytes=mib << 20)


def per_device(forcing, search_direction, ocean_depth, land_mask, fold_map):
    lat_count, lon_count = lax.axis_size("lat"), lax.axis_size(LON)
    call = pl.pallas_call
    fields, first, second, reach, choice = call(
        functools.partial(pack_kernel, lon_count // 2), name="pack",
        in_specs=[pl.BlockSpec(memory_space=pl.ANY)] * 5,
        out_specs=[pl.BlockSpec(memory_space=pltpu.VMEM)] * 3 + [pl.BlockSpec(memory_space=pltpu.SMEM)] * 2,
        out_shape=(shape(3, ROWS, LANES), shape(BLK + 32, LANES), shape(BLK + 32, LANES),
                   pltpu.SMEM((1,), jnp.int32), pltpu.SMEM((1,), jnp.int32)),
        scratch_shapes=[pltpu.VMEM((ROWS, LANES), F32)] * 3 + [
            pltpu.VMEM((ROWS, LANES), jnp.int32), pltpu.SMEM((LANES,), jnp.int32), pltpu.SemaphoreType.DMA((5,)),
        ],
        compiler_params=limit(4),
    )(*held(forcing, search_direction, ocean_depth, land_mask, fold_map, space=pltpu.HBM))
    evens, odds = range(0, lon_count, 2), range(1, lon_count, 2)
    wrap = [(i, (i + 1) % lon_count) for i in odds]
    second = lax.ppermute(second, LON, wrap + [(b, a) for a, b in wrap])
    first = lax.ppermute(first, LON, [(i, i + 1) for i in evens] + [(i + 1, i) for i in evens])

    one, two, two_next = call(
        functools.partial(turn_kernel, lat_count - 1), name="turn",
        in_specs=[pl.BlockSpec(memory_space=pltpu.SMEM)] + [pl.BlockSpec(memory_space=pltpu.VMEM)] * 3,
        out_shape=(shape(64, LANES),) * 3,
        scratch_shapes=[pltpu.VMEM((BLK + 32, LANES), F32)] * 2 + [pltpu.VMEM((64, LANES), F32)] * 4,
        compiler_params=limit(4),
    )(reach, *held(fields, second, first))

    evens, odds = range(0, lat_count, 2), range(1, lat_count - 1, 2)
    pairs = [(i, i + 1) for i in evens] + [(i + 1, i) for i in evens]
    swaps = [
        (i * lon_count + c, (i + s) * lon_count + c)
        for k in odds for i, s in ((k, 1), (k + 1, -1)) for c in range(lon_count)
    ]
    top = (lat_count - 1) * lon_count

    def second_round(value, pairing):
        fold = [(top + i, top + (2 * pairing - i) % lon_count) for i in range(lon_count)]
        return lax.ppermute(value, ("lat",) + LON, swaps + fold)

    def branch(index):
        def exchange(one, near, far, fields, second, first):
            value = second_round(near, index // 2)
            if index % 2:
                value = value + second_round(far, (index // 2 + 1) % (lon_count // 2))
            one = lax.ppermute(one, "lat", pairs)
            ready = call(
                prepare_kernel, name="prepare",
                out_shape=(shape(2, PITCH, LANES), shape(2, PITCH, LANES), shape(2, PITCH, LANES),
                           shape(2, 9, PITCH, LANES)),
                scratch_shapes=[pltpu.VMEM((BLK + 32, LANES), F32)] * 2,
                compiler_params=limit(4),
                cost_estimate=pl.CostEstimate(flops=4_000_000, transcendentals=0, bytes_accessed=0),
            )(*held(fields, second, first))
            landed = call(
                land_kernel, name="land", out_shape=(shape(64, LANES),) * 2, compiler_params=limit(2),
            )(*held(value, one))
            return *ready, *landed

        return exchange

    depth, side, inv, coef, south, north = lax.switch(
        choice[0], [branch(i) for i in range(lon_count)], one, two, two_next, fields, second, first
    )

    basis, sums, *_ = call(
        basis_kernel, name="basis",
        out_shape=(shape(VECTORS, PITCH, LANES), shape(lon_count, LANES), shape(2, PITCH, LANES),
                   shape(2, PITCH, LANES), shape(2, 9, PITCH, LANES)),
        scratch_shapes=[
            pltpu.VMEM((VECTORS, PITCH, LANES), F32),
            pltpu.VMEM((STEPS, 8, 8, LANES), F32),
        ],
        input_output_aliases={2: 2, 3: 3, 4: 4},
        compiler_params=limit(12),
    )(*held(fields, side, depth, inv, coef, south, north))
    sums = lax.all_to_all(sums, LON, split_axis=0, concat_axis=0, tiled=True)
    sums = call(middle_kernel, name="middle", out_shape=shape(lat_count, LANES), compiler_params=limit(2))(*held(sums))
    sums = lax.all_to_all(sums, "lat", split_axis=0, concat_axis=0, tiled=True)
    return call(
        final_kernel, name="final", out_shape=(jax.ShapeDtypeStruct((ROWS, LANES), F32),) * 2,
        compiler_params=limit(4),
    )(*held(sums, basis))


def solution(mesh):
    lon = mesh.shape["lon"]
    split = Mesh(mesh.devices.reshape(mesh.shape["lat"], lon // 4, 4), ("lat", "lon_0", "lon_1"))
    return jax.shard_map(
        per_device,
        mesh=split,
        in_specs=(P("lat", LON), P("lat", LON), P("lat", LON), P("lat", LON), P()),
        out_specs=(P("lat", LON), P("lat", LON)),
        check_vma=False,
    )
```

```python
import functools

import jax
import jax.numpy as jnp
from jax import lax
from jax.experimental import pallas as pl
from jax.experimental.pallas import tpu as pltpu
from jax.sharding import Mesh
from jax.sharding import PartitionSpec as P

STEPS = 8
REACH = 256
ROWS = 160
LANES = 128
EXT = ROWS + 32
PITCH = 216
EDGE = 9
BLK = 32
LON = ("lon_0", "lon_1")
VECTORS = 2 * STEPS + 1
F32 = jnp.float32


def edge_of(q, blk):
    return 25 * blk + (0, 9, 17)[q], (9, 8, 8)[q]


def lanes_of(rows):
    return lax.broadcasted_iota(jnp.int32, (rows, LANES), 1)


def shift_east(a, b, lane):
    ra, rb = pltpu.roll(a, 1, 1), pltpu.roll(b, 1, 1)
    first = lane == 0
    return jnp.where(first, rb, ra), jnp.where(first, ra, rb)


def shift_west(a, b, lane):
    ra, rb = pltpu.roll(a, LANES - 1, 1), pltpu.roll(b, LANES - 1, 1)
    last = lane == LANES - 1
    return jnp.where(last, rb, ra), jnp.where(last, ra, rb)


def pack_kernel(pairs, f_hbm, p_hbm, d_hbm, m_hbm, map_hbm, x_ref, first_ref, second_ref, reach_ref, choice_ref,
                f_ref, p_ref, d_ref, m_ref, pivot, sems):
    even = lax.axis_index(LON) % 2 == 0
    copies = [
        pltpu.make_async_copy(source, target, sems.at[i])
        for i, (source, target) in enumerate((
            (m_hbm, m_ref), (d_hbm, d_ref), (f_hbm, f_ref), (p_hbm, p_ref), (map_hbm.at[pl.ds(0, LANES)], pivot),
        ))
    ]
    for copy in copies:
        copy.start()
    for copy in copies:
        copy.wait()
    for g in range(ROWS // 8):
        rows = pl.ds(8 * g, 8)
        flag = m_ref[rows, :].astype(F32)
        x_ref[0, rows, :] = d_ref[rows, :] * flag
        x_ref[1, rows, :] = f_ref[rows, :] * flag
        x_ref[2, rows, :] = p_ref[rows, :] * flag
    lane = lanes_of(8)
    for v in range(BLK // 8):
        east = jnp.zeros((8, LANES), F32)
        west = jnp.zeros((8, LANES), F32)
        for q in range(3):
            for blk in range(ROWS // BLK):
                at, width = edge_of(q, blk)
                tile = x_ref[q, pl.ds(BLK * blk + 8 * v, 8), :]
                inside = (lane >= at) & (lane < at + width)
                west = jnp.where(inside, pltpu.roll(tile, at, 1) if at else tile, west)
                east = jnp.where(inside, pltpu.roll(tile, (at + width) % LANES, 1), east)
        first_ref[pl.ds(8 * v, 8), :] = jnp.where(even, east, west)
        second_ref[pl.ds(8 * v, 8), :] = jnp.where(even, west, east)
    for slot, (q, row) in enumerate(((0, ROWS - 8), (1, ROWS - 8), (2, ROWS - 8), (0, ROWS - 16))):
        tile = x_ref[q, pl.ds(row, 8), :]
        first_ref[pl.ds(BLK + 8 * slot, 8), :] = tile
        second_ref[pl.ds(BLK + 8 * slot, 8), :] = tile
    past = pivot[0] + (2 * pairs * LANES - 8)
    reach = past % (2 * LANES) + 8
    reach_ref[0] = reach
    split = jnp.where(reach + EDGE >= 2 * LANES, 1, 0)
    choice_ref[0] = 2 * ((past // (2 * LANES)) % pairs) + split


def unpack_halo(from_west, from_east, q, blk, v, lane):
    at, width = edge_of(q, blk)
    right = from_east[pl.ds(8 * v, 8), :]
    left = from_west[pl.ds(8 * v, 8), :]
    right = pltpu.roll(right, LANES - at, 1) if at else right
    left = pltpu.roll(left, (2 * LANES - width - at) % LANES, 1)
    return jnp.where(lane < EDGE, right, jnp.where(lane >= LANES - EDGE, left, 0.0))


def sort_partners(axis, first, second, before, after):
    even = lax.axis_index(axis) % 2 == 0
    for g in range(first.shape[0] // 8):
        rows = pl.ds(8 * g, 8)
        a, b = first[rows, :], second[rows, :]
        before[rows, :] = jnp.where(even, b, a)
        after[rows, :] = jnp.where(even, a, b)


def turn_kernel(tops, r_ref, x_ref, second_ref, first_ref, one_ref, two_ref, next_ref,
                fw_ref, fe_ref, north_ref, south_ref, t1_ref, t2_ref):
    lane = lanes_of(8)
    lat = lax.axis_index("lat")
    even, top_row = lat % 2 == 0, lat == tops
    sort_partners(LON, first_ref, second_ref, fw_ref, fe_ref)
    top, low = ROWS // 8 - 1, 0
    for ref, rows in (
        (north_ref, ((0, top), (1, top), (2, top), (0, top - 1))),
        (south_ref, ((0, low), (1, low), (2, low), (0, low + 1))),
    ):
        for slot, (q, g) in enumerate(rows):
            ref[pl.ds(8 * slot, 8), :] = x_ref[q, pl.ds(8 * g, 8), :]
            blk, v = 8 * g // BLK, (8 * g % BLK) // 8
            ref[pl.ds(32 + 8 * slot, 8), :] = unpack_halo(fw_ref, fe_ref, q, blk, v, lane)
    for g in range(8):
        rows = pl.ds(8 * g, 8)
        north, south = north_ref[rows, :], south_ref[rows, :]
        one_ref[rows, :] = jnp.where(even, north, south)
        two_ref[rows, :] = jnp.where(even, south, north)
        next_ref[rows, :] = jnp.zeros((8, LANES), F32)

    @pl.when(top_row)
    def _():
        across_fold(r_ref[0], lane, north_ref, fw_ref, fe_ref, two_ref, next_ref, t1_ref, t2_ref)


def across_fold(reach, lane, north_ref, fw_ref, fe_ref, fold_ref, next_ref, t1_ref, t2_ref):
    along = reach - lane
    pick = along & (LANES - 1)
    place_a = along
    place_b = jnp.where(lane < EDGE, along - LANES, along + LANES)
    halo = (lane < EDGE) | (lane >= LANES - EDGE)
    for slot in range(4):
        rows = pl.ds(8 * slot, 8)
        own = jnp.take_along_axis(north_ref[rows, :], pick, axis=1, mode="promise_in_bounds")
        west = jnp.take_along_axis(fw_ref[pl.ds(BLK + 8 * slot, 8), :], pick, axis=1, mode="promise_in_bounds")
        east = jnp.take_along_axis(fe_ref[pl.ds(BLK + 8 * slot, 8), :], pick, axis=1, mode="promise_in_bounds")
        for part, place in ((0, place_a), (32, place_b)):
            near = jnp.where(place < 0, west, jnp.where(place < LANES, own, east))
            near = jnp.where(place < 2 * LANES, near, 0.0)
            far = jnp.where(place >= 2 * LANES, own, 0.0)
            if part:
                near = jnp.where(halo, near, 0.0)
                far = jnp.where(halo, far, 0.0)
            t1_ref[pl.ds(part + 8 * slot, 8), :] = near
            t2_ref[pl.ds(part + 8 * slot, 8), :] = far
    for g in range(8):
        for m in range(8):
            fold_ref[pl.ds(8 * g + m, 1), :] = t1_ref[pl.ds(8 * g + 7 - m, 1), :]
            next_ref[pl.ds(8 * g + m, 1), :] = t2_ref[pl.ds(8 * g + 7 - m, 1), :]


GROUPS = ROWS // 8 + 2


def root_of(depth, inv, at, lane):
    vert, mid, wet_mid, deep = [], [], [], []
    for t in range(2):
        down = depth[t, pl.ds(at - 1, 8), :]
        here = depth[t, pl.ds(at, 8), :]
        up = depth[t, pl.ds(at + 1, 8), :]
        wet = jnp.where(here > 0.0, 1.0, 0.0)
        wets = jnp.where(down > 0.0, 1.0, 0.0) + jnp.where(up > 0.0, 1.0, 0.0)
        vert.append((down + up, wets))
        mid.append((here + 0.5 * (down + up), wet + 0.5 * wets))
        deep.append(here)
        wet_mid.append(wet)
    sums = []
    for c in range(2):
        ea, eb = shift_east(mid[0][c], mid[1][c], lane)
        wa, wb = shift_west(mid[0][c], mid[1][c], lane)
        sums.append((vert[0][c] + (ea + wa), vert[1][c] + (eb + wb)))
    for t in range(2):
        links = 0.5 * (deep[t] * sums[1][t] + sums[0][t])
        diagonal = wet_mid[t] * (deep[t] / (REACH * REACH) + links) + (1.0 - wet_mid[t])
        inv[t, pl.ds(at, 8), :] = lax.rsqrt(diagonal) * wet_mid[t]


def coefs_of(depth, inv, coef, at, lane):
    d = [[depth[t, pl.ds(at + s, 8), :] for s in (-1, 0, 1)] for t in range(2)]
    r = [[inv[t, pl.ds(at + s, 8), :] for s in (-1, 0, 1)] for t in range(2)]
    de, re = shift_east(d[0][1], d[1][1], lane), shift_east(r[0][1], r[1][1], lane)
    dw, rw = shift_west(d[0][1], d[1][1], lane), shift_west(r[0][1], r[1][1], lane)
    for t in range(2):
        for base, (dc, rc) in enumerate(((d[t][1], r[t][1]), (de[t], re[t]), (dw[t], rw[t]))):
            for s in range(3):
                if base == 0 and s == 1:
                    continue
                whole = base == 0 or s == 1
                c = (dc + d[t][s]) * (rc * r[t][s])
                coef[t, 3 * base + s, pl.ds(at, 8), :] = c * (-1.0 if whole else -0.5)


def prepare_kernel(x_ref, second_ref, first_ref, depth, side, inv, coef, fw_ref, fe_ref):
    sort_partners(LON, first_ref, second_ref, fw_ref, fe_ref)
    lane = lanes_of(8)

    def unpack(v, carry):
        for q, ref in ((0, depth.at[1]), (1, side.at[1]), (2, side.at[0])):
            for blk in range(ROWS // BLK):
                rows = pl.ds(pl.multiple_of(16 + BLK * blk + 8 * v, 8), 8)
                ref[rows, :] = unpack_halo(fw_ref, fe_ref, q, blk, v, lane)
        return carry

    for g in range(ROWS // 8):
        depth[0, pl.ds(16 + 8 * g, 8), :] = x_ref[0, pl.ds(8 * g, 8), :]
    lax.fori_loop(0, BLK // 8, unpack, 0)

    def roots(i, carry):
        for g in range(6):
            root_of(depth, inv, pl.multiple_of(24 + 48 * i, 8) + 8 * g, lane)
        return carry

    def coefs(i, carry):
        for g in range(4):
            coefs_of(depth, inv, coef, pl.multiple_of(32 + 32 * i, 8) + 8 * g, lane)
        return carry

    lax.fori_loop(0, 3, roots, 0)
    lax.fori_loop(0, 4, coefs, 0)


def land_kernel(two_ref, one_ref, south_ref, north_ref):
    sort_partners("lat", one_ref, two_ref, south_ref, north_ref)


def basis_kernel(x_ref, side_ref, _depth, _inv, _coef, fs_ref, fn_ref, basis_ref, sums_ref, depth, inv, coef,
                 side, acc):
    lane = lanes_of(8)
    zero = jnp.zeros((8, LANES), F32)
    for q, k in ((1, STEPS + 1), (2, 0)):
        for g in range(ROWS // 8):
            rows = pl.ds(16 + 8 * g, 8)
            basis_ref[k, rows, :] = x_ref[q, pl.ds(8 * g, 8), :]
            side[k, rows, :] = side_ref[2 - q, rows, :]
    targets = (
        lambda t: depth.at[t],
        lambda t: (basis_ref if t == 0 else side).at[STEPS + 1],
        lambda t: (basis_ref if t == 0 else side).at[0],
    )
    for q in range(3):
        own, rim = targets[q](0), targets[q](1)
        for t, ref in ((0, own), (1, rim)):
            at = 32 * t + 8 * q
            ref[pl.ds(8, 8), :] = fs_ref[pl.ds(at, 8), :]
            ref[pl.ds(EXT - 16, 8), :] = fn_ref[pl.ds(at, 8), :]
            if q == 0:
                at = 32 * t + 24
                ref[pl.ds(0, 8), :] = fs_ref[pl.ds(at, 8), :]
                ref[pl.ds(EXT - 8, 8), :] = fn_ref[pl.ds(at, 8), :]
            else:
                ref[pl.ds(0, 8), :] = zero
                ref[pl.ds(EXT - 8, 8), :] = zero
    for k in list(range(1, STEPS + 1)) + list(range(STEPS + 2, VECTORS)):
        for ref in (basis_ref, side):
            ref[k, pl.ds(0, 8), :] = zero
            ref[k, pl.ds(EXT - 8, 8), :] = zero
    for t in range(2):
        inv[t, pl.ds(0, 8), :] = zero
        inv[t, pl.ds(EXT - 8, 8), :] = zero

    for g in (0, 1, GROUPS - 2, GROUPS - 1):
        root_of(depth, inv, 8 + 8 * g, lane)
    for g in (0, 1, 2, GROUPS - 3, GROUPS - 2, GROUPS - 1):
        coefs_of(depth, inv, coef, 8 + 8 * g, lane)

    def twice_applied(k, at, tiles, weights):
        parts = []
        for t in range(2):
            ref = basis_ref if t == 0 else side
            down, here, up = (ref[k, pl.ds(at + s, 8), :] for s in (-1, 0, 1))
            w = weights[t]
            straight = w[0] * down + w[2] * up
            toward_w = (w[3] * down + w[5] * up) + w[4] * here
            toward_e = (w[6] * down + w[8] * up) + w[7] * here
            parts.append((straight, toward_w, toward_e, here))
        wa, wb = shift_west(parts[0][1], parts[1][1], lane)
        ea, eb = shift_east(parts[0][2], parts[1][2], lane)
        return ((parts[0][0] + (wa + ea), parts[1][0] + (wb + eb))[:tiles], parts[0][3])

    def weights_at(at):
        return [[None if i == 1 else coef[t, i, pl.ds(at, 8), :] for i in range(9)] for t in range(2)]

    def step(k, first, last):
        total = [zero] * 6
        tiles = 1 if last else 2
        for g in range(1, GROUPS - 1) if last else range(GROUPS):
            at = 8 + 8 * g
            w = weights_at(at)
            now, new = [], []
            for base in ((0,) if last else (0, STEPS + 1)):
                out, here = twice_applied(base + k, at, tiles, w)
                now.append(here)
                for t in range(tiles):
                    ref = basis_ref if t == 0 else side
                    value = 0.5 * out[t] if first else out[t] - ref[base + k - 1, pl.ds(at, 8), :]
                    ref[base + k + 1, pl.ds(at, 8), :] = value
                    if t == 0:
                        new.append(value)
            if last:
                now.append(basis_ref[STEPS + 1 + k, pl.ds(at, 8), :])
            if 1 <= g <= ROWS // 8:
                p, r = now
                total[0] += p * p
                total[1] += p * new[0]
                total[2] += r * r
                total[3] += new[0] * new[0] if last else r * new[1]
                total[4] += p * r
                total[5] += new[0] * r
        for i in range(6):
            acc[6 * k + i, :, :] = total[i]

    step(0, True, False)

    def middle(k, carry):
        step(k, False, False)
        return carry

    lax.fori_loop(1, STEPS - 1, middle, 0)
    step(STEPS - 1, False, True)

    flat = jnp.sum(acc[...], axis=1)
    flat = jnp.concatenate([flat, jnp.zeros((LANES - 6 * STEPS, LANES), F32)], axis=0)
    row = jnp.broadcast_to(jnp.sum(flat.T, axis=0, keepdims=True), (8, LANES))
    for g in range(sums_ref.shape[0] // 8):
        sums_ref[pl.ds(8 * g, 8), :] = row


def middle_kernel(in_ref, out_ref):
    out_ref[...] = jnp.broadcast_to(jnp.sum(in_ref[...], axis=0, keepdims=True), out_ref.shape)


def final_kernel(sum_ref, basis_ref, height_hbm, residual_hbm, height_ref, residual_ref, sems):
    products = jnp.broadcast_to(jnp.sum(sum_ref[...], axis=0, keepdims=True), (8, LANES))
    row = lax.broadcasted_iota(jnp.int32, (24, LANES), 0)
    first = row == 0
    odd = row & 1

    def gathered(index):
        parts = [
            jnp.take_along_axis(products, index[8 * g : 8 * g + 8], axis=1, mode="promise_in_bounds")
            for g in range(3)
        ]
        return jnp.concatenate(parts, axis=0)

    def moments(slot, count):
        index = jnp.where(row < count, 6 * (row >> 1) + odd + slot, LANES - 1)
        if count > 2 * STEPS:
            index = jnp.where(row == 2 * STEPS, 6 * (STEPS - 1) + 3, index)
        return 2.0 * gathered(index) - gathered(jnp.where(row < count, odd + slot, LANES - 1))

    def raised(v):
        up = pltpu.roll(v, 23, 0)
        return v + 0.5 * (up + jnp.where(first, up, pltpu.roll(v, 1, 0)))

    def mapped(v):
        down = pltpu.roll(jnp.where(first, v, 0.5 * v), 1, 0)
        return v + down + pltpu.roll(jnp.where(first, 0.0, 0.5 * v), 23, 0)

    def dot(u, v):
        return jnp.sum(u[0] * v[0] + u[1] * v[1], axis=0, keepdims=True)

    pair = (0, 1)
    unit, zero = jnp.where(first, 1.0, 0.0), jnp.zeros((24, LANES), F32)
    pp, rr, pr = moments(0, 2 * STEPS + 1), moments(2, 2 * STEPS - 1), moments(4, 2 * STEPS)
    xc, pc, rc = (zero, zero), (unit, zero), (zero, unit)
    with_r, with_q = (pr, rr), (raised(pp), raised(pr))
    norm = dot(rc, with_r)
    for _ in range(STEPS):
        t = norm / dot(pc, with_q)
        inverse = 1.0 / norm
        with_r = [with_r[i] - t * with_q[i] for i in pair]
        rc, xc = [rc[i] - t * mapped(pc[i]) for i in pair], [xc[i] + t * pc[i] for i in pair]
        norm = dot(rc, with_r)
        ratio = norm * inverse
        with_q = [raised(with_r[i]) + ratio * with_q[i] for i in pair]
        pc = [rc[i] + ratio * pc[i] for i in pair]
    spots = [(0, k) for k in range(STEPS + 1)] + [(1, k) for k in range(STEPS)]
    xs = [jnp.broadcast_to(xc[i][k : k + 1, :], (8, LANES)) for i, k in spots]
    rs = [jnp.broadcast_to(rc[i][k : k + 1, :], (8, LANES)) for i, k in spots]
    copies = []
    for part in range(4):
        for g in range(part * ROWS // 32, (part + 1) * ROWS // 32):
            above = below = None
            for k in range(VECTORS):
                tile = basis_ref[k, pl.ds(16 + 8 * g, 8), :]
                above = xs[k] * tile if above is None else above + xs[k] * tile
                below = rs[k] * tile if below is None else below + rs[k] * tile
            height_ref[pl.ds(8 * g, 8), :] = above
            residual_ref[pl.ds(8 * g, 8), :] = below
        rows = pl.ds(part * ROWS // 4, ROWS // 4)
        for i, (source, target) in enumerate(((height_ref, height_hbm), (residual_ref, residual_hbm))):
            copies.append(pltpu.make_async_copy(source.at[rows], target.at[rows], sems.at[2 * part + i]))
            copies[-1].start()
    for copy in copies:
        copy.wait()


def shape(*dims):
    return pltpu.VMEM(dims, F32)


def held(*values, space=pltpu.VMEM):
    return tuple(pltpu.with_memory_space_constraint(v, space) for v in values)


def limit(mib):
    return pltpu.CompilerParams(vmem_limit_bytes=mib << 20)


def per_device(forcing, search_direction, ocean_depth, land_mask, fold_map):
    lat_count, lon_count = lax.axis_size("lat"), lax.axis_size(LON)
    call = pl.pallas_call
    fields, first, second, reach, choice = call(
        functools.partial(pack_kernel, lon_count // 2), name="pack",
        in_specs=[pl.BlockSpec(memory_space=pl.ANY)] * 5,
        out_specs=[pl.BlockSpec(memory_space=pltpu.VMEM)] * 3 + [pl.BlockSpec(memory_space=pltpu.SMEM)] * 2,
        out_shape=(shape(3, ROWS, LANES), shape(BLK + 32, LANES), shape(BLK + 32, LANES),
                   pltpu.SMEM((1,), jnp.int32), pltpu.SMEM((1,), jnp.int32)),
        scratch_shapes=[pltpu.VMEM((ROWS, LANES), F32)] * 3 + [
            pltpu.VMEM((ROWS, LANES), jnp.int32), pltpu.SMEM((LANES,), jnp.int32), pltpu.SemaphoreType.DMA((5,)),
        ],
        compiler_params=limit(4),
    )(*held(forcing, search_direction, ocean_depth, land_mask, fold_map, space=pltpu.HBM))
    evens, odds = range(0, lon_count, 2), range(1, lon_count, 2)
    wrap = [(i, (i + 1) % lon_count) for i in odds]
    second = lax.ppermute(second, LON, wrap + [(b, a) for a, b in wrap])
    first = lax.ppermute(first, LON, [(i, i + 1) for i in evens] + [(i + 1, i) for i in evens])

    one, two, two_next = call(
        functools.partial(turn_kernel, lat_count - 1), name="turn",
        in_specs=[pl.BlockSpec(memory_space=pltpu.SMEM)] + [pl.BlockSpec(memory_space=pltpu.VMEM)] * 3,
        out_shape=(shape(64, LANES),) * 3,
        scratch_shapes=[pltpu.VMEM((BLK + 32, LANES), F32)] * 2 + [pltpu.VMEM((64, LANES), F32)] * 4,
        compiler_params=limit(4),
    )(reach, *held(fields, second, first))

    evens, odds = range(0, lat_count, 2), range(1, lat_count - 1, 2)
    pairs = [(i, i + 1) for i in evens] + [(i + 1, i) for i in evens]
    swaps = [
        (i * lon_count + c, (i + s) * lon_count + c)
        for k in odds for i, s in ((k, 1), (k + 1, -1)) for c in range(lon_count)
    ]
    top = (lat_count - 1) * lon_count

    def second_round(value, pairing, others):
        fold = [(top + i, top + (2 * pairing - i) % lon_count) for i in range(lon_count)]
        return lax.ppermute(value, ("lat",) + LON, others + fold)

    def branch(index):
        def exchange(one, near, far, fields, second, first):
            value = second_round(near, index // 2, swaps)
            if index % 2:
                pairing = (index // 2 + 1) % (lon_count // 2)
                value = value + second_round(far, pairing, swaps if pairing == 0 else [])
            one = lax.ppermute(one, "lat", pairs)
            ready = call(
                prepare_kernel, name="prepare",
                out_shape=(shape(2, PITCH, LANES), shape(2, PITCH, LANES), shape(2, PITCH, LANES),
                           shape(2, 9, PITCH, LANES)),
                scratch_shapes=[pltpu.VMEM((BLK + 32, LANES), F32)] * 2,
                compiler_params=limit(4),
                cost_estimate=pl.CostEstimate(flops=4_000_000, transcendentals=0, bytes_accessed=0),
            )(*held(fields, second, first))
            landed = call(
                land_kernel, name="land", out_shape=(shape(64, LANES),) * 2, compiler_params=limit(2),
            )(*held(value, one))
            return *ready, *landed

        return exchange

    depth, side, inv, coef, south, north = lax.switch(
        choice[0], [branch(i) for i in range(lon_count)], one, two, two_next, fields, second, first
    )

    basis, sums, *_ = call(
        basis_kernel, name="basis",
        out_shape=(shape(VECTORS, PITCH, LANES), shape(lon_count, LANES), shape(2, PITCH, LANES),
                   shape(2, PITCH, LANES), shape(2, 9, PITCH, LANES)),
        scratch_shapes=[
            pltpu.VMEM((VECTORS, PITCH, LANES), F32),
            pltpu.VMEM((6 * STEPS, 8, LANES), F32),
        ],
        input_output_aliases={2: 2, 3: 3, 4: 4},
        compiler_params=limit(12),
    )(*held(fields, side, depth, inv, coef, south, north))
    sums = lax.all_to_all(sums, LON, split_axis=0, concat_axis=0, tiled=True)
    sums = call(middle_kernel, name="middle", out_shape=shape(lat_count, LANES), compiler_params=limit(2))(*held(sums))
    sums = lax.all_to_all(sums, "lat", split_axis=0, concat_axis=0, tiled=True)
    return call(
        final_kernel, name="final", out_shape=(jax.ShapeDtypeStruct((ROWS, LANES), F32),) * 2,
        out_specs=[pl.BlockSpec(memory_space=pl.ANY)] * 2,
        scratch_shapes=[pltpu.VMEM((ROWS, LANES), F32)] * 2 + [pltpu.SemaphoreType.DMA((8,))],
        compiler_params=limit(4),
    )(*held(sums, basis))


def solution(mesh):
    lon = mesh.shape["lon"]
    split = Mesh(mesh.devices.reshape(mesh.shape["lat"], lon // 4, 4), ("lat", "lon_0", "lon_1"))
    return jax.shard_map(
        per_device,
        mesh=split,
        in_specs=(P("lat", LON), P("lat", LON), P("lat", LON), P("lat", LON), P()),
        out_specs=(P("lat", LON), P("lat", LON)),
        check_vma=False,
    )
```

```python
import functools

import jax
import jax.numpy as jnp
from jax import lax
from jax.experimental import pallas as pl
from jax.experimental.pallas import tpu as pltpu
from jax.sharding import Mesh
from jax.sharding import PartitionSpec as P

STEPS = 8
REACH = 256
ROWS = 160
LANES = 128
EXT = ROWS + 32
PITCH = 216
EDGE = 9
BLK = 32
LON = ("lon_0", "lon_1")
VECTORS = 2 * STEPS + 1
F32 = jnp.float32


def edge_of(q, blk):
    return 25 * blk + (0, 9, 17)[q], (9, 8, 8)[q]


def lanes_of(rows):
    return lax.broadcasted_iota(jnp.int32, (rows, LANES), 1)


def shift_east(a, b, lane):
    ra, rb = pltpu.roll(a, 1, 1), pltpu.roll(b, 1, 1)
    first = lane == 0
    return jnp.where(first, rb, ra), jnp.where(first, ra, rb)


def shift_west(a, b, lane):
    ra, rb = pltpu.roll(a, LANES - 1, 1), pltpu.roll(b, LANES - 1, 1)
    last = lane == LANES - 1
    return jnp.where(last, rb, ra), jnp.where(last, ra, rb)


def pack_kernel(pairs, f_hbm, p_hbm, d_hbm, m_hbm, map_hbm, x_ref, first_ref, second_ref, reach_ref, choice_ref,
                f_ref, p_ref, d_ref, m_ref, pivot, sems):
    even = turns(LON)
    copies = [
        pltpu.make_async_copy(source, target, sems.at[i])
        for i, (source, target) in enumerate((
            (m_hbm, m_ref), (d_hbm, d_ref), (f_hbm, f_ref), (p_hbm, p_ref), (map_hbm.at[pl.ds(0, LANES)], pivot),
        ))
    ]
    for copy in copies:
        copy.start()
    for copy in copies:
        copy.wait()
    for g in range(ROWS // 8):
        rows = pl.ds(8 * g, 8)
        flag = m_ref[rows, :].astype(F32)
        x_ref[0, rows, :] = d_ref[rows, :] * flag
        x_ref[1, rows, :] = f_ref[rows, :] * flag
        x_ref[2, rows, :] = p_ref[rows, :] * flag
    lane = lanes_of(8)
    for v in range(BLK // 8):
        east = jnp.zeros((8, LANES), F32)
        west = jnp.zeros((8, LANES), F32)
        for q in range(3):
            for blk in range(ROWS // BLK):
                at, width = edge_of(q, blk)
                tile = x_ref[q, pl.ds(BLK * blk + 8 * v, 8), :]
                inside = (lane >= at) & (lane < at + width)
                west = jnp.where(inside, pltpu.roll(tile, at, 1) if at else tile, west)
                east = jnp.where(inside, pltpu.roll(tile, (at + width) % LANES, 1), east)
        first_ref[pl.ds(8 * v, 8), :] = jnp.where(even, east, west)
        second_ref[pl.ds(8 * v, 8), :] = jnp.where(even, west, east)
    for slot, (q, row) in enumerate(((0, ROWS - 8), (1, ROWS - 8), (2, ROWS - 8), (0, ROWS - 16))):
        tile = x_ref[q, pl.ds(row, 8), :]
        first_ref[pl.ds(BLK + 8 * slot, 8), :] = tile
        second_ref[pl.ds(BLK + 8 * slot, 8), :] = tile
    past = pivot[0] + (2 * pairs * LANES - 8)
    reach = past % (2 * LANES) + 8
    reach_ref[0] = reach
    split = jnp.where(reach + EDGE >= 2 * LANES, 1, 0)
    choice_ref[0] = 2 * ((past // (2 * LANES)) % pairs) + split


def unpack_halo(from_west, from_east, q, blk, v, lane):
    at, width = edge_of(q, blk)
    right = from_east[pl.ds(8 * v, 8), :]
    left = from_west[pl.ds(8 * v, 8), :]
    right = pltpu.roll(right, LANES - at, 1) if at else right
    left = pltpu.roll(left, (2 * LANES - width - at) % LANES, 1)
    return jnp.where(lane < EDGE, right, jnp.where(lane >= LANES - EDGE, left, 0.0))


def turns(axis):
    place = lax.axis_index("lat")
    if axis == LON:
        place = place + lax.axis_index(LON)
    return place % 2 == 0


def sort_partners(axis, first, second, before, after):
    even = turns(axis)
    for g in range(first.shape[0] // 8):
        rows = pl.ds(8 * g, 8)
        a, b = first[rows, :], second[rows, :]
        before[rows, :] = jnp.where(even, b, a)
        after[rows, :] = jnp.where(even, a, b)


def turn_kernel(tops, r_ref, x_ref, second_ref, first_ref, one_ref, two_ref, next_ref,
                fw_ref, fe_ref, north_ref, south_ref, t1_ref, t2_ref):
    lane = lanes_of(8)
    lat = lax.axis_index("lat")
    even, top_row = lat % 2 == 0, lat == tops
    sort_partners(LON, first_ref, second_ref, fw_ref, fe_ref)
    top, low = ROWS // 8 - 1, 0
    for ref, rows in (
        (north_ref, ((0, top), (1, top), (2, top), (0, top - 1))),
        (south_ref, ((0, low), (1, low), (2, low), (0, low + 1))),
    ):
        for slot, (q, g) in enumerate(rows):
            ref[pl.ds(8 * slot, 8), :] = x_ref[q, pl.ds(8 * g, 8), :]
            blk, v = 8 * g // BLK, (8 * g % BLK) // 8
            ref[pl.ds(32 + 8 * slot, 8), :] = unpack_halo(fw_ref, fe_ref, q, blk, v, lane)
    for g in range(8):
        rows = pl.ds(8 * g, 8)
        north, south = north_ref[rows, :], south_ref[rows, :]
        one_ref[rows, :] = jnp.where(even, north, south)
        two_ref[rows, :] = jnp.where(even, south, north)
        next_ref[rows, :] = jnp.zeros((8, LANES), F32)

    @pl.when(top_row)
    def _():
        across_fold(r_ref[0], lane, north_ref, fw_ref, fe_ref, two_ref, next_ref, t1_ref, t2_ref)


def across_fold(reach, lane, north_ref, fw_ref, fe_ref, fold_ref, next_ref, t1_ref, t2_ref):
    along = reach - lane
    pick = along & (LANES - 1)
    place_a = along
    place_b = jnp.where(lane < EDGE, along - LANES, along + LANES)
    halo = (lane < EDGE) | (lane >= LANES - EDGE)
    for slot in range(4):
        rows = pl.ds(8 * slot, 8)
        own = jnp.take_along_axis(north_ref[rows, :], pick, axis=1, mode="promise_in_bounds")
        west = jnp.take_along_axis(fw_ref[pl.ds(BLK + 8 * slot, 8), :], pick, axis=1, mode="promise_in_bounds")
        east = jnp.take_along_axis(fe_ref[pl.ds(BLK + 8 * slot, 8), :], pick, axis=1, mode="promise_in_bounds")
        for part, place in ((0, place_a), (32, place_b)):
            near = jnp.where(place < 0, west, jnp.where(place < LANES, own, east))
            near = jnp.where(place < 2 * LANES, near, 0.0)
            far = jnp.where(place >= 2 * LANES, own, 0.0)
            if part:
                near = jnp.where(halo, near, 0.0)
                far = jnp.where(halo, far, 0.0)
            t1_ref[pl.ds(part + 8 * slot, 8), :] = near
            t2_ref[pl.ds(part + 8 * slot, 8), :] = far
    for g in range(8):
        for m in range(8):
            fold_ref[pl.ds(8 * g + m, 1), :] = t1_ref[pl.ds(8 * g + 7 - m, 1), :]
            next_ref[pl.ds(8 * g + m, 1), :] = t2_ref[pl.ds(8 * g + 7 - m, 1), :]


GROUPS = ROWS // 8 + 2


def root_of(depth, inv, at, lane):
    vert, mid, wet_mid, deep = [], [], [], []
    for t in range(2):
        down = depth[t, pl.ds(at - 1, 8), :]
        here = depth[t, pl.ds(at, 8), :]
        up = depth[t, pl.ds(at + 1, 8), :]
        wet = jnp.where(here > 0.0, 1.0, 0.0)
        wets = jnp.where(down > 0.0, 1.0, 0.0) + jnp.where(up > 0.0, 1.0, 0.0)
        vert.append((down + up, wets))
        mid.append((here + 0.5 * (down + up), wet + 0.5 * wets))
        deep.append(here)
        wet_mid.append(wet)
    sums = []
    for c in range(2):
        ea, eb = shift_east(mid[0][c], mid[1][c], lane)
        wa, wb = shift_west(mid[0][c], mid[1][c], lane)
        sums.append((vert[0][c] + (ea + wa), vert[1][c] + (eb + wb)))
    for t in range(2):
        links = 0.5 * (deep[t] * sums[1][t] + sums[0][t])
        diagonal = wet_mid[t] * (deep[t] / (REACH * REACH) + links) + (1.0 - wet_mid[t])
        inv[t, pl.ds(at, 8), :] = lax.rsqrt(diagonal) * wet_mid[t]


def coefs_of(depth, inv, coef, at, lane):
    d = [[depth[t, pl.ds(at + s, 8), :] for s in (-1, 0, 1)] for t in range(2)]
    r = [[inv[t, pl.ds(at + s, 8), :] for s in (-1, 0, 1)] for t in range(2)]
    de, re = shift_east(d[0][1], d[1][1], lane), shift_east(r[0][1], r[1][1], lane)
    dw, rw = shift_west(d[0][1], d[1][1], lane), shift_west(r[0][1], r[1][1], lane)
    for t in range(2):
        for base, (dc, rc) in enumerate(((d[t][1], r[t][1]), (de[t], re[t]), (dw[t], rw[t]))):
            for s in range(3):
                if base == 0 and s == 1:
                    continue
                whole = base == 0 or s == 1
                c = (dc + d[t][s]) * (rc * r[t][s])
                coef[t, 3 * base + s, pl.ds(at, 8), :] = c * (-1.0 if whole else -0.5)


def prepare_kernel(x_ref, second_ref, first_ref, depth, side, inv, coef, fw_ref, fe_ref):
    sort_partners(LON, first_ref, second_ref, fw_ref, fe_ref)
    lane = lanes_of(8)

    def unpack(v, carry):
        for q, ref in ((0, depth.at[1]), (1, side.at[1]), (2, side.at[0])):
            for blk in range(ROWS // BLK):
                rows = pl.ds(pl.multiple_of(16 + BLK * blk + 8 * v, 8), 8)
                ref[rows, :] = unpack_halo(fw_ref, fe_ref, q, blk, v, lane)
        return carry

    for g in range(ROWS // 8):
        depth[0, pl.ds(16 + 8 * g, 8), :] = x_ref[0, pl.ds(8 * g, 8), :]
    lax.fori_loop(0, BLK // 8, unpack, 0)

    def roots(i, carry):
        for g in range(6):
            root_of(depth, inv, pl.multiple_of(24 + 48 * i, 8) + 8 * g, lane)
        return carry

    def coefs(i, carry):
        for g in range(4):
            coefs_of(depth, inv, coef, pl.multiple_of(32 + 32 * i, 8) + 8 * g, lane)
        return carry

    lax.fori_loop(0, 3, roots, 0)
    lax.fori_loop(0, 4, coefs, 0)


def land_kernel(two_ref, one_ref, south_ref, north_ref):
    sort_partners("lat", one_ref, two_ref, south_ref, north_ref)


def basis_kernel(x_ref, side_ref, _depth, _inv, _coef, fs_ref, fn_ref, basis_ref, sums_ref, depth, inv, coef,
                 side, acc):
    lane = lanes_of(8)
    zero = jnp.zeros((8, LANES), F32)
    for q, k in ((1, STEPS + 1), (2, 0)):
        for g in range(ROWS // 8):
            rows = pl.ds(16 + 8 * g, 8)
            basis_ref[k, rows, :] = x_ref[q, pl.ds(8 * g, 8), :]
            side[k, rows, :] = side_ref[2 - q, rows, :]
    targets = (
        lambda t: depth.at[t],
        lambda t: (basis_ref if t == 0 else side).at[STEPS + 1],
        lambda t: (basis_ref if t == 0 else side).at[0],
    )
    for q in range(3):
        own, rim = targets[q](0), targets[q](1)
        for t, ref in ((0, own), (1, rim)):
            at = 32 * t + 8 * q
            ref[pl.ds(8, 8), :] = fs_ref[pl.ds(at, 8), :]
            ref[pl.ds(EXT - 16, 8), :] = fn_ref[pl.ds(at, 8), :]
            if q == 0:
                at = 32 * t + 24
                ref[pl.ds(0, 8), :] = fs_ref[pl.ds(at, 8), :]
                ref[pl.ds(EXT - 8, 8), :] = fn_ref[pl.ds(at, 8), :]
            else:
                ref[pl.ds(0, 8), :] = zero
                ref[pl.ds(EXT - 8, 8), :] = zero
    for k in list(range(1, STEPS + 1)) + list(range(STEPS + 2, VECTORS)):
        for ref in (basis_ref, side):
            ref[k, pl.ds(0, 8), :] = zero
            ref[k, pl.ds(EXT - 8, 8), :] = zero
    for t in range(2):
        inv[t, pl.ds(0, 8), :] = zero
        inv[t, pl.ds(EXT - 8, 8), :] = zero

    for g in (0, 1, GROUPS - 2, GROUPS - 1):
        root_of(depth, inv, 8 + 8 * g, lane)
    for g in (0, 1, 2, GROUPS - 3, GROUPS - 2, GROUPS - 1):
        coefs_of(depth, inv, coef, 8 + 8 * g, lane)

    def twice_applied(k, at, tiles, weights):
        parts = []
        for t in range(2):
            ref = basis_ref if t == 0 else side
            down, here, up = (ref[k, pl.ds(at + s, 8), :] for s in (-1, 0, 1))
            w = weights[t]
            straight = w[0] * down + w[2] * up
            toward_w = (w[3] * down + w[5] * up) + w[4] * here
            toward_e = (w[6] * down + w[8] * up) + w[7] * here
            parts.append((straight, toward_w, toward_e, here))
        wa, wb = shift_west(parts[0][1], parts[1][1], lane)
        ea, eb = shift_east(parts[0][2], parts[1][2], lane)
        return ((parts[0][0] + (wa + ea), parts[1][0] + (wb + eb))[:tiles], parts[0][3])

    def weights_at(at):
        return [[None if i == 1 else coef[t, i, pl.ds(at, 8), :] for i in range(9)] for t in range(2)]

    def step(k, first, last):
        total = [zero] * 6
        tiles = 1 if last else 2
        for g in range(1, GROUPS - 1) if last else range(GROUPS):
            at = 8 + 8 * g
            w = weights_at(at)
            now, new = [], []
            for base in ((0,) if last else (0, STEPS + 1)):
                out, here = twice_applied(base + k, at, tiles, w)
                now.append(here)
                for t in range(tiles):
                    ref = basis_ref if t == 0 else side
                    value = 0.5 * out[t] if first else out[t] - ref[base + k - 1, pl.ds(at, 8), :]
                    ref[base + k + 1, pl.ds(at, 8), :] = value
                    if t == 0:
                        new.append(value)
            if last:
                now.append(basis_ref[STEPS + 1 + k, pl.ds(at, 8), :])
            if 1 <= g <= ROWS // 8:
                p, r = now
                total[0] += p * p
                total[1] += p * new[0]
                total[2] += r * r
                total[3] += new[0] * new[0] if last else r * new[1]
                total[4] += p * r
                total[5] += new[0] * r
        for i in range(6):
            acc[6 * k + i, :, :] = total[i]

    step(0, True, False)

    def middle(k, carry):
        step(k, False, False)
        return carry

    lax.fori_loop(1, STEPS - 1, middle, 0)
    step(STEPS - 1, False, True)

    flat = jnp.sum(acc[...], axis=1)
    flat = jnp.concatenate([flat, jnp.zeros((LANES - 6 * STEPS, LANES), F32)], axis=0)
    row = jnp.broadcast_to(jnp.sum(flat.T, axis=0, keepdims=True), (8, LANES))
    for g in range(sums_ref.shape[0] // 8):
        sums_ref[pl.ds(8 * g, 8), :] = row


def middle_kernel(in_ref, out_ref):
    out_ref[...] = jnp.broadcast_to(jnp.sum(in_ref[...], axis=0, keepdims=True), out_ref.shape)


def final_kernel(sum_ref, basis_ref, height_hbm, residual_hbm, height_ref, residual_ref, sems):
    products = jnp.broadcast_to(jnp.sum(sum_ref[...], axis=0, keepdims=True), (8, LANES))
    row = lax.broadcasted_iota(jnp.int32, (24, LANES), 0)
    first = row == 0
    odd = row & 1

    def gathered(index):
        parts = [
            jnp.take_along_axis(products, index[8 * g : 8 * g + 8], axis=1, mode="promise_in_bounds")
            for g in range(3)
        ]
        return jnp.concatenate(parts, axis=0)

    def moments(slot, count):
        index = jnp.where(row < count, 6 * (row >> 1) + odd + slot, LANES - 1)
        if count > 2 * STEPS:
            index = jnp.where(row == 2 * STEPS, 6 * (STEPS - 1) + 3, index)
        return 2.0 * gathered(index) - gathered(jnp.where(row < count, odd + slot, LANES - 1))

    def raised(v):
        up = pltpu.roll(v, 23, 0)
        return v + 0.5 * (up + jnp.where(first, up, pltpu.roll(v, 1, 0)))

    def mapped(v):
        down = pltpu.roll(jnp.where(first, v, 0.5 * v), 1, 0)
        return v + down + pltpu.roll(jnp.where(first, 0.0, 0.5 * v), 23, 0)

    def dot(u, v):
        return jnp.sum(u[0] * v[0] + u[1] * v[1], axis=0, keepdims=True)

    pair = (0, 1)
    unit, zero = jnp.where(first, 1.0, 0.0), jnp.zeros((24, LANES), F32)
    pp, rr, pr = moments(0, 2 * STEPS + 1), moments(2, 2 * STEPS - 1), moments(4, 2 * STEPS)
    xc, pc, rc = (zero, zero), (unit, zero), (zero, unit)
    with_r, with_q = (pr, rr), (raised(pp), raised(pr))
    norm = dot(rc, with_r)
    for _ in range(STEPS):
        t = norm / dot(pc, with_q)
        inverse = 1.0 / norm
        with_r = [with_r[i] - t * with_q[i] for i in pair]
        rc, xc = [rc[i] - t * mapped(pc[i]) for i in pair], [xc[i] + t * pc[i] for i in pair]
        norm = dot(rc, with_r)
        ratio = norm * inverse
        with_q = [raised(with_r[i]) + ratio * with_q[i] for i in pair]
        pc = [rc[i] + ratio * pc[i] for i in pair]
    spots = [(0, k) for k in range(STEPS + 1)] + [(1, k) for k in range(STEPS)]
    xs = [jnp.broadcast_to(xc[i][k : k + 1, :], (8, LANES)) for i, k in spots]
    rs = [jnp.broadcast_to(rc[i][k : k + 1, :], (8, LANES)) for i, k in spots]
    copies = []
    for part in range(4):
        for g in range(part * ROWS // 32, (part + 1) * ROWS // 32):
            above = below = None
            for k in range(VECTORS):
                tile = basis_ref[k, pl.ds(16 + 8 * g, 8), :]
                above = xs[k] * tile if above is None else above + xs[k] * tile
                below = rs[k] * tile if below is None else below + rs[k] * tile
            height_ref[pl.ds(8 * g, 8), :] = above
            residual_ref[pl.ds(8 * g, 8), :] = below
        rows = pl.ds(part * ROWS // 4, ROWS // 4)
        for i, (source, target) in enumerate(((height_ref, height_hbm), (residual_ref, residual_hbm))):
            copies.append(pltpu.make_async_copy(source.at[rows], target.at[rows], sems.at[2 * part + i]))
            copies[-1].start()
    for copy in copies:
        copy.wait()


def shape(*dims):
    return pltpu.VMEM(dims, F32)


def held(*values, space=pltpu.VMEM):
    return tuple(pltpu.with_memory_space_constraint(v, space) for v in values)


def limit(mib):
    return pltpu.CompilerParams(vmem_limit_bytes=mib << 20)


def per_device(forcing, search_direction, ocean_depth, land_mask, fold_map):
    lat_count, lon_count = lax.axis_size("lat"), lax.axis_size(LON)
    call = pl.pallas_call
    fields, first, second, reach, choice = call(
        functools.partial(pack_kernel, lon_count // 2), name="pack",
        in_specs=[pl.BlockSpec(memory_space=pl.ANY)] * 5,
        out_specs=[pl.BlockSpec(memory_space=pltpu.VMEM)] * 3 + [pl.BlockSpec(memory_space=pltpu.SMEM)] * 2,
        out_shape=(shape(3, ROWS, LANES), shape(BLK + 32, LANES), shape(BLK + 32, LANES),
                   pltpu.SMEM((1,), jnp.int32), pltpu.SMEM((1,), jnp.int32)),
        scratch_shapes=[pltpu.VMEM((ROWS, LANES), F32)] * 3 + [
            pltpu.VMEM((ROWS, LANES), jnp.int32), pltpu.SMEM((LANES,), jnp.int32), pltpu.SemaphoreType.DMA((5,)),
        ],
        compiler_params=limit(4),
    )(*held(forcing, search_direction, ocean_depth, land_mask, fold_map, space=pltpu.HBM))
    def lon_round(start):
        pairs = []
        for row in range(lat_count):
            for i in range((start + row) % 2, lon_count, 2):
                a, b = row * lon_count + i, row * lon_count + (i + 1) % lon_count
                pairs += [(a, b), (b, a)]
        return pairs

    second = lax.ppermute(second, ("lat",) + LON, lon_round(1))
    first = lax.ppermute(first, ("lat",) + LON, lon_round(0))

    one, two, two_next = call(
        functools.partial(turn_kernel, lat_count - 1), name="turn",
        in_specs=[pl.BlockSpec(memory_space=pltpu.SMEM)] + [pl.BlockSpec(memory_space=pltpu.VMEM)] * 3,
        out_shape=(shape(64, LANES),) * 3,
        scratch_shapes=[pltpu.VMEM((BLK + 32, LANES), F32)] * 2 + [pltpu.VMEM((64, LANES), F32)] * 4,
        compiler_params=limit(4),
    )(reach, *held(fields, second, first))

    evens, odds = range(0, lat_count, 2), range(1, lat_count - 1, 2)
    pairs = [(i, i + 1) for i in evens] + [(i + 1, i) for i in evens]
    swaps = [
        (i * lon_count + c, (i + s) * lon_count + c)
        for k in odds for i, s in ((k, 1), (k + 1, -1)) for c in range(lon_count)
    ]
    top = (lat_count - 1) * lon_count

    def second_round(value, pairing, others):
        fold = [(top + i, top + (2 * pairing - i) % lon_count) for i in range(lon_count)]
        return lax.ppermute(value, ("lat",) + LON, others + fold)

    def branch(index):
        def exchange(one, near, far, fields, second, first):
            value = second_round(near, index // 2, swaps)
            if index % 2:
                pairing = (index // 2 + 1) % (lon_count // 2)
                value = value + second_round(far, pairing, swaps if pairing == 0 else [])
            one = lax.ppermute(one, "lat", pairs)
            ready = call(
                prepare_kernel, name="prepare",
                out_shape=(shape(2, PITCH, LANES), shape(2, PITCH, LANES), shape(2, PITCH, LANES),
                           shape(2, 9, PITCH, LANES)),
                scratch_shapes=[pltpu.VMEM((BLK + 32, LANES), F32)] * 2,
                compiler_params=limit(4),
                cost_estimate=pl.CostEstimate(flops=4_000_000, transcendentals=0, bytes_accessed=0),
            )(*held(fields, second, first))
            landed = call(
                land_kernel, name="land", out_shape=(shape(64, LANES),) * 2, compiler_params=limit(2),
            )(*held(value, one))
            return *ready, *landed

        return exchange

    depth, side, inv, coef, south, north = lax.switch(
        choice[0], [branch(i) for i in range(lon_count)], one, two, two_next, fields, second, first
    )

    basis, sums, *_ = call(
        basis_kernel, name="basis",
        out_shape=(shape(VECTORS, PITCH, LANES), shape(lon_count, LANES), shape(2, PITCH, LANES),
                   shape(2, PITCH, LANES), shape(2, 9, PITCH, LANES)),
        scratch_shapes=[
            pltpu.VMEM((VECTORS, PITCH, LANES), F32),
            pltpu.VMEM((6 * STEPS, 8, LANES), F32),
        ],
        input_output_aliases={2: 2, 3: 3, 4: 4},
        compiler_params=limit(12),
    )(*held(fields, side, depth, inv, coef, south, north))
    sums = lax.all_to_all(sums, LON, split_axis=0, concat_axis=0, tiled=True)
    sums = call(middle_kernel, name="middle", out_shape=shape(lat_count, LANES), compiler_params=limit(2))(*held(sums))
    sums = lax.all_to_all(sums, "lat", split_axis=0, concat_axis=0, tiled=True)
    return call(
        final_kernel, name="final", out_shape=(jax.ShapeDtypeStruct((ROWS, LANES), F32),) * 2,
        out_specs=[pl.BlockSpec(memory_space=pl.ANY)] * 2,
        scratch_shapes=[pltpu.VMEM((ROWS, LANES), F32)] * 2 + [pltpu.SemaphoreType.DMA((8,))],
        compiler_params=limit(4),
    )(*held(sums, basis))


def solution(mesh):
    lon = mesh.shape["lon"]
    split = Mesh(mesh.devices.reshape(mesh.shape["lat"], lon // 4, 4), ("lat", "lon_0", "lon_1"))
    return jax.shard_map(
        per_device,
        mesh=split,
        in_specs=(P("lat", LON), P("lat", LON), P("lat", LON), P("lat", LON), P()),
        out_specs=(P("lat", LON), P("lat", LON)),
        check_vma=False,
    )
```

```python
import functools

import jax
import jax.numpy as jnp
from jax import lax
from jax.experimental import pallas as pl
from jax.experimental.pallas import tpu as pltpu
from jax.sharding import Mesh
from jax.sharding import PartitionSpec as P

STEPS = 8
REACH = 256
ROWS = 160
LANES = 128
EXT = ROWS + 32
PITCH = 216
EDGE = 9
BLK = 32
LON = ("lon_0", "lon_1")
VECTORS = 2 * STEPS + 1
F32 = jnp.float32


def edge_of(q, blk):
    return (9 * blk, 45 + 8 * blk, 85 + 8 * blk)[q], (9, 8, 8)[q]


def lanes_of(rows):
    return lax.broadcasted_iota(jnp.int32, (rows, LANES), 1)


def shift_east(a, b, lane):
    ra, rb = pltpu.roll(a, 1, 1), pltpu.roll(b, 1, 1)
    first = lane == 0
    return jnp.where(first, rb, ra), jnp.where(first, ra, rb)


def shift_west(a, b, lane):
    ra, rb = pltpu.roll(a, LANES - 1, 1), pltpu.roll(b, LANES - 1, 1)
    last = lane == LANES - 1
    return jnp.where(last, rb, ra), jnp.where(last, ra, rb)


def pack_kernel(pairs, f_hbm, p_hbm, d_hbm, m_hbm, map_hbm, x_ref, first_ref, second_ref, reach_ref, choice_ref,
                f_ref, p_ref, d_ref, m_ref, pivot, sems):
    even = turns(LON)
    copies = [
        pltpu.make_async_copy(source, target, sems.at[i])
        for i, (source, target) in enumerate((
            (m_hbm, m_ref), (d_hbm, d_ref), (f_hbm, f_ref), (p_hbm, p_ref), (map_hbm.at[pl.ds(0, LANES)], pivot),
        ))
    ]
    for copy in copies:
        copy.start()
    for copy in copies:
        copy.wait()
    for g in range(ROWS // 8):
        rows = pl.ds(8 * g, 8)
        flag = m_ref[rows, :].astype(F32)
        x_ref[0, rows, :] = d_ref[rows, :] * flag
        x_ref[1, rows, :] = f_ref[rows, :] * flag
        x_ref[2, rows, :] = p_ref[rows, :] * flag
    lane = lanes_of(8)
    for v in range(BLK // 8):
        east = jnp.zeros((8, LANES), F32)
        west = jnp.zeros((8, LANES), F32)
        for q in range(3):
            for blk in range(ROWS // BLK):
                at, width = edge_of(q, blk)
                tile = x_ref[q, pl.ds(BLK * blk + 8 * v, 8), :]
                tile = pltpu.roll(tile, at, 1) if at else tile
                west = jnp.where((lane >= at) & (lane < at + width), tile, west)
                start = (at - width) % LANES
                east = jnp.where((lane >= start) & (lane < start + width), tile, east)
        first_ref[pl.ds(8 * v, 8), :] = jnp.where(even, east, west)
        second_ref[pl.ds(8 * v, 8), :] = jnp.where(even, west, east)
    for slot, (q, row) in enumerate(((0, ROWS - 8), (1, ROWS - 8), (2, ROWS - 8), (0, ROWS - 16))):
        tile = x_ref[q, pl.ds(row, 8), :]
        first_ref[pl.ds(BLK + 8 * slot, 8), :] = tile
        second_ref[pl.ds(BLK + 8 * slot, 8), :] = tile
    past = pivot[0] + (2 * pairs * LANES - 8)
    reach = past % (2 * LANES) + 8
    reach_ref[0] = reach
    split = jnp.where(reach + EDGE >= 2 * LANES, 1, 0)
    choice_ref[0] = 2 * ((past // (2 * LANES)) % pairs) + split


def unpack_halo(from_west, from_east, q, blk, v, lane):
    at, width = edge_of(q, blk)
    right = from_east[pl.ds(8 * v, 8), :]
    left = from_west[pl.ds(8 * v, 8), :]
    both = jnp.where((lane >= at) & (lane < at + EDGE), right, left)
    both = pltpu.roll(both, LANES - at, 1) if at else both
    return jnp.where((lane < EDGE) | (lane >= LANES - EDGE), both, 0.0)


def turns(axis):
    place = lax.axis_index("lat")
    if axis == LON:
        place = place + lax.axis_index(LON)
    return place % 2 == 0


def sort_partners(axis, first, second, before, after):
    even = turns(axis)
    for g in range(first.shape[0] // 8):
        rows = pl.ds(8 * g, 8)
        a, b = first[rows, :], second[rows, :]
        before[rows, :] = jnp.where(even, b, a)
        after[rows, :] = jnp.where(even, a, b)


def turn_kernel(tops, r_ref, x_ref, second_ref, first_ref, one_ref, two_ref, next_ref,
                fw_ref, fe_ref, north_ref, south_ref, t1_ref, t2_ref):
    lane = lanes_of(8)
    lat = lax.axis_index("lat")
    even, top_row = lat % 2 == 0, lat == tops
    sort_partners(LON, first_ref, second_ref, fw_ref, fe_ref)
    top, low = ROWS // 8 - 1, 0
    for ref, rows in (
        (north_ref, ((0, top), (1, top), (2, top), (0, top - 1))),
        (south_ref, ((0, low), (1, low), (2, low), (0, low + 1))),
    ):
        for slot, (q, g) in enumerate(rows):
            ref[pl.ds(8 * slot, 8), :] = x_ref[q, pl.ds(8 * g, 8), :]
            blk, v = 8 * g // BLK, (8 * g % BLK) // 8
            ref[pl.ds(32 + 8 * slot, 8), :] = unpack_halo(fw_ref, fe_ref, q, blk, v, lane)
    for g in range(8):
        rows = pl.ds(8 * g, 8)
        north, south = north_ref[rows, :], south_ref[rows, :]
        one_ref[rows, :] = jnp.where(even, north, south)
        two_ref[rows, :] = jnp.where(even, south, north)
        next_ref[rows, :] = jnp.zeros((8, LANES), F32)

    @pl.when(top_row)
    def _():
        across_fold(r_ref[0], lane, north_ref, fw_ref, fe_ref, two_ref, next_ref, t1_ref, t2_ref)


def across_fold(reach, lane, north_ref, fw_ref, fe_ref, fold_ref, next_ref, t1_ref, t2_ref):
    along = reach - lane
    pick = along & (LANES - 1)
    place_a = along
    place_b = jnp.where(lane < EDGE, along - LANES, along + LANES)
    halo = (lane < EDGE) | (lane >= LANES - EDGE)
    for slot in range(4):
        rows = pl.ds(8 * slot, 8)
        own = jnp.take_along_axis(north_ref[rows, :], pick, axis=1, mode="promise_in_bounds")
        west = jnp.take_along_axis(fw_ref[pl.ds(BLK + 8 * slot, 8), :], pick, axis=1, mode="promise_in_bounds")
        east = jnp.take_along_axis(fe_ref[pl.ds(BLK + 8 * slot, 8), :], pick, axis=1, mode="promise_in_bounds")
        for part, place in ((0, place_a), (32, place_b)):
            near = jnp.where(place < 0, west, jnp.where(place < LANES, own, east))
            near = jnp.where(place < 2 * LANES, near, 0.0)
            far = jnp.where(place >= 2 * LANES, own, 0.0)
            if part:
                near = jnp.where(halo, near, 0.0)
                far = jnp.where(halo, far, 0.0)
            t1_ref[pl.ds(part + 8 * slot, 8), :] = near
            t2_ref[pl.ds(part + 8 * slot, 8), :] = far
    for g in range(8):
        for m in range(8):
            fold_ref[pl.ds(8 * g + m, 1), :] = t1_ref[pl.ds(8 * g + 7 - m, 1), :]
            next_ref[pl.ds(8 * g + m, 1), :] = t2_ref[pl.ds(8 * g + 7 - m, 1), :]


GROUPS = ROWS // 8 + 2


def root_of(depth, inv, at, lane):
    vert, mid, wet_mid, deep = [], [], [], []
    for t in range(2):
        down = depth[t, pl.ds(at - 1, 8), :]
        here = depth[t, pl.ds(at, 8), :]
        up = depth[t, pl.ds(at + 1, 8), :]
        wet = jnp.where(here > 0.0, 1.0, 0.0)
        wets = jnp.where(down > 0.0, 1.0, 0.0) + jnp.where(up > 0.0, 1.0, 0.0)
        vert.append((down + up, wets))
        mid.append((here + 0.5 * (down + up), wet + 0.5 * wets))
        deep.append(here)
        wet_mid.append(wet)
    sums = []
    for c in range(2):
        ea, eb = shift_east(mid[0][c], mid[1][c], lane)
        wa, wb = shift_west(mid[0][c], mid[1][c], lane)
        sums.append((vert[0][c] + (ea + wa), vert[1][c] + (eb + wb)))
    for t in range(2):
        links = 0.5 * (deep[t] * sums[1][t] + sums[0][t])
        diagonal = wet_mid[t] * (deep[t] / (REACH * REACH) + links) + (1.0 - wet_mid[t])
        inv[t, pl.ds(at, 8), :] = lax.rsqrt(diagonal) * wet_mid[t]


def coefs_of(depth, inv, coef, at, lane):
    d = [[depth[t, pl.ds(at + s, 8), :] for s in (-1, 0, 1)] for t in range(2)]
    r = [[inv[t, pl.ds(at + s, 8), :] for s in (-1, 0, 1)] for t in range(2)]
    de, re = shift_east(d[0][1], d[1][1], lane), shift_east(r[0][1], r[1][1], lane)
    dw, rw = shift_west(d[0][1], d[1][1], lane), shift_west(r[0][1], r[1][1], lane)
    for t in range(2):
        for base, (dc, rc) in enumerate(((d[t][1], r[t][1]), (de[t], re[t]), (dw[t], rw[t]))):
            for s in range(3):
                if base == 0 and s == 1:
                    continue
                whole = base == 0 or s == 1
                c = (dc + d[t][s]) * (rc * r[t][s])
                coef[t, 3 * base + s, pl.ds(at, 8), :] = c * (-1.0 if whole else -0.5)


def prepare_kernel(x_ref, second_ref, first_ref, depth, side, inv, coef, fw_ref, fe_ref):
    sort_partners(LON, first_ref, second_ref, fw_ref, fe_ref)
    lane = lanes_of(8)

    def unpack(v, carry):
        for q, ref in ((0, depth.at[1]), (1, side.at[1]), (2, side.at[0])):
            for blk in range(ROWS // BLK):
                rows = pl.ds(pl.multiple_of(16 + BLK * blk + 8 * v, 8), 8)
                ref[rows, :] = unpack_halo(fw_ref, fe_ref, q, blk, v, lane)
        return carry

    for g in range(ROWS // 8):
        depth[0, pl.ds(16 + 8 * g, 8), :] = x_ref[0, pl.ds(8 * g, 8), :]
    lax.fori_loop(0, BLK // 8, unpack, 0)

    def roots(i, carry):
        for g in range(6):
            root_of(depth, inv, pl.multiple_of(24 + 48 * i, 8) + 8 * g, lane)
        return carry

    def coefs(i, carry):
        for g in range(4):
            coefs_of(depth, inv, coef, pl.multiple_of(32 + 32 * i, 8) + 8 * g, lane)
        return carry

    lax.fori_loop(0, 3, roots, 0)
    lax.fori_loop(0, 4, coefs, 0)


def land_kernel(two_ref, one_ref, south_ref, north_ref):
    sort_partners("lat", one_ref, two_ref, south_ref, north_ref)


def basis_kernel(x_ref, side_ref, _depth, _inv, _coef, fs_ref, fn_ref, basis_ref, sums_ref, depth, inv, coef,
                 side, acc):
    lane = lanes_of(8)
    zero = jnp.zeros((8, LANES), F32)
    for q, k in ((1, STEPS + 1), (2, 0)):
        for g in range(ROWS // 8):
            rows = pl.ds(16 + 8 * g, 8)
            basis_ref[k, rows, :] = x_ref[q, pl.ds(8 * g, 8), :]
            side[k, rows, :] = side_ref[2 - q, rows, :]
    targets = (
        lambda t: depth.at[t],
        lambda t: (basis_ref if t == 0 else side).at[STEPS + 1],
        lambda t: (basis_ref if t == 0 else side).at[0],
    )
    for q in range(3):
        own, rim = targets[q](0), targets[q](1)
        for t, ref in ((0, own), (1, rim)):
            at = 32 * t + 8 * q
            ref[pl.ds(8, 8), :] = fs_ref[pl.ds(at, 8), :]
            ref[pl.ds(EXT - 16, 8), :] = fn_ref[pl.ds(at, 8), :]
            if q == 0:
                at = 32 * t + 24
                ref[pl.ds(0, 8), :] = fs_ref[pl.ds(at, 8), :]
                ref[pl.ds(EXT - 8, 8), :] = fn_ref[pl.ds(at, 8), :]
            else:
                ref[pl.ds(0, 8), :] = zero
                ref[pl.ds(EXT - 8, 8), :] = zero
    for k in list(range(1, STEPS + 1)) + list(range(STEPS + 2, VECTORS)):
        for ref in (basis_ref, side):
            ref[k, pl.ds(0, 8), :] = zero
            ref[k, pl.ds(EXT - 8, 8), :] = zero
    for t in range(2):
        inv[t, pl.ds(0, 8), :] = zero
        inv[t, pl.ds(EXT - 8, 8), :] = zero

    for g in (0, 1, GROUPS - 2, GROUPS - 1):
        root_of(depth, inv, 8 + 8 * g, lane)
    for g in (0, 1, 2, GROUPS - 3, GROUPS - 2, GROUPS - 1):
        coefs_of(depth, inv, coef, 8 + 8 * g, lane)

    def twice_applied(k, at, tiles, weights):
        parts = []
        for t in range(2):
            ref = basis_ref if t == 0 else side
            down, here, up = (ref[k, pl.ds(at + s, 8), :] for s in (-1, 0, 1))
            w = weights[t]
            straight = w[0] * down + w[2] * up
            toward_w = (w[3] * down + w[5] * up) + w[4] * here
            toward_e = (w[6] * down + w[8] * up) + w[7] * here
            parts.append((straight, toward_w, toward_e, here))
        wa, wb = shift_west(parts[0][1], parts[1][1], lane)
        ea, eb = shift_east(parts[0][2], parts[1][2], lane)
        return ((parts[0][0] + (wa + ea), parts[1][0] + (wb + eb))[:tiles], parts[0][3])

    def weights_at(at):
        return [[None if i == 1 else coef[t, i, pl.ds(at, 8), :] for i in range(9)] for t in range(2)]

    def step(k, first, last):
        total = [zero] * 6
        tiles = 1 if last else 2
        for g in range(1, GROUPS - 1) if last else range(GROUPS):
            at = 8 + 8 * g
            w = weights_at(at)
            now, new = [], []
            for base in ((0,) if last else (0, STEPS + 1)):
                out, here = twice_applied(base + k, at, tiles, w)
                now.append(here)
                for t in range(tiles):
                    ref = basis_ref if t == 0 else side
                    value = 0.5 * out[t] if first else out[t] - ref[base + k - 1, pl.ds(at, 8), :]
                    ref[base + k + 1, pl.ds(at, 8), :] = value
                    if t == 0:
                        new.append(value)
            if last:
                now.append(basis_ref[STEPS + 1 + k, pl.ds(at, 8), :])
            if 1 <= g <= ROWS // 8:
                p, r = now
                total[0] += p * p
                total[1] += p * new[0]
                total[2] += r * r
                total[3] += new[0] * new[0] if last else r * new[1]
                total[4] += p * r
                total[5] += new[0] * r
        for i in range(6):
            acc[6 * k + i, :, :] = total[i]

    step(0, True, False)

    def middle(k, carry):
        step(k, False, False)
        return carry

    lax.fori_loop(1, STEPS - 1, middle, 0, unroll=2)
    step(STEPS - 1, False, True)

    flat = jnp.sum(acc[...], axis=1)
    flat = jnp.concatenate([flat, jnp.zeros((LANES - 6 * STEPS, LANES), F32)], axis=0)
    row = jnp.broadcast_to(jnp.sum(flat.T, axis=0, keepdims=True), (8, LANES))
    for g in range(sums_ref.shape[0] // 8):
        sums_ref[pl.ds(8 * g, 8), :] = row


def middle_kernel(in_ref, out_ref):
    out_ref[...] = jnp.broadcast_to(jnp.sum(in_ref[...], axis=0, keepdims=True), out_ref.shape)


def final_kernel(sum_ref, basis_ref, height_hbm, residual_hbm, height_ref, residual_ref, sems):
    products = jnp.broadcast_to(jnp.sum(sum_ref[...], axis=0, keepdims=True), (8, LANES))
    row = lax.broadcasted_iota(jnp.int32, (24, LANES), 0)
    first = row == 0
    odd = row & 1

    def gathered(index):
        parts = [
            jnp.take_along_axis(products, index[8 * g : 8 * g + 8], axis=1, mode="promise_in_bounds")
            for g in range(3)
        ]
        return jnp.concatenate(parts, axis=0)

    def moments(slot, count):
        index = jnp.where(row < count, 6 * (row >> 1) + odd + slot, LANES - 1)
        if count > 2 * STEPS:
            index = jnp.where(row == 2 * STEPS, 6 * (STEPS - 1) + 3, index)
        return 2.0 * gathered(index) - gathered(jnp.where(row < count, odd + slot, LANES - 1))

    def raised(v):
        up = pltpu.roll(v, 23, 0)
        return v + 0.5 * (up + jnp.where(first, up, pltpu.roll(v, 1, 0)))

    def mapped(v):
        down = pltpu.roll(jnp.where(first, v, 0.5 * v), 1, 0)
        return v + down + pltpu.roll(jnp.where(first, 0.0, 0.5 * v), 23, 0)

    def dot(u, v):
        return jnp.sum(u[0] * v[0] + u[1] * v[1], axis=0, keepdims=True)

    pair = (0, 1)
    unit, zero = jnp.where(first, 1.0, 0.0), jnp.zeros((24, LANES), F32)
    pp, rr, pr = moments(0, 2 * STEPS + 1), moments(2, 2 * STEPS - 1), moments(4, 2 * STEPS)
    xc, pc, rc = (zero, zero), (unit, zero), (zero, unit)
    with_r, with_q = (pr, rr), (raised(pp), raised(pr))
    norm = dot(rc, with_r)
    for _ in range(STEPS):
        t = norm / dot(pc, with_q)
        inverse = 1.0 / norm
        with_r = [with_r[i] - t * with_q[i] for i in pair]
        rc, xc = [rc[i] - t * mapped(pc[i]) for i in pair], [xc[i] + t * pc[i] for i in pair]
        norm = dot(rc, with_r)
        ratio = norm * inverse
        with_q = [raised(with_r[i]) + ratio * with_q[i] for i in pair]
        pc = [rc[i] + ratio * pc[i] for i in pair]
    spots = [(0, k) for k in range(STEPS + 1)] + [(1, k) for k in range(STEPS)]
    xs = [jnp.broadcast_to(xc[i][k : k + 1, :], (8, LANES)) for i, k in spots]
    rs = [jnp.broadcast_to(rc[i][k : k + 1, :], (8, LANES)) for i, k in spots]
    copies = []
    for part in range(4):
        for g in range(part * ROWS // 32, (part + 1) * ROWS // 32):
            above = below = None
            for k in range(VECTORS):
                tile = basis_ref[k, pl.ds(16 + 8 * g, 8), :]
                above = xs[k] * tile if above is None else above + xs[k] * tile
                below = rs[k] * tile if below is None else below + rs[k] * tile
            height_ref[pl.ds(8 * g, 8), :] = above
            residual_ref[pl.ds(8 * g, 8), :] = below
        rows = pl.ds(part * ROWS // 4, ROWS // 4)
        for i, (source, target) in enumerate(((height_ref, height_hbm), (residual_ref, residual_hbm))):
            copies.append(pltpu.make_async_copy(source.at[rows], target.at[rows], sems.at[2 * part + i]))
            copies[-1].start()
    for copy in copies:
        copy.wait()


def shape(*dims):
    return pltpu.VMEM(dims, F32)


def held(*values, space=pltpu.VMEM):
    return tuple(pltpu.with_memory_space_constraint(v, space) for v in values)


def limit(mib):
    return pltpu.CompilerParams(vmem_limit_bytes=mib << 20)


def per_device(forcing, search_direction, ocean_depth, land_mask, fold_map):
    lat_count, lon_count = lax.axis_size("lat"), lax.axis_size(LON)
    call = pl.pallas_call
    fields, first, second, reach, choice = call(
        functools.partial(pack_kernel, lon_count // 2), name="pack",
        in_specs=[pl.BlockSpec(memory_space=pl.ANY)] * 5,
        out_specs=[pl.BlockSpec(memory_space=pltpu.VMEM)] * 3 + [pl.BlockSpec(memory_space=pltpu.SMEM)] * 2,
        out_shape=(shape(3, ROWS, LANES), shape(BLK + 32, LANES), shape(BLK + 32, LANES),
                   pltpu.SMEM((1,), jnp.int32), pltpu.SMEM((1,), jnp.int32)),
        scratch_shapes=[pltpu.VMEM((ROWS, LANES), F32)] * 3 + [
            pltpu.VMEM((ROWS, LANES), jnp.int32), pltpu.SMEM((LANES,), jnp.int32), pltpu.SemaphoreType.DMA((5,)),
        ],
        compiler_params=limit(4),
    )(*held(forcing, search_direction, ocean_depth, land_mask, fold_map, space=pltpu.HBM))
    def lon_round(start):
        pairs = []
        for row in range(lat_count):
            for i in range((start + row) % 2, lon_count, 2):
                a, b = row * lon_count + i, row * lon_count + (i + 1) % lon_count
                pairs += [(a, b), (b, a)]
        return pairs

    second = lax.ppermute(second, ("lat",) + LON, lon_round(1))
    first = lax.ppermute(first, ("lat",) + LON, lon_round(0))

    one, two, two_next = call(
        functools.partial(turn_kernel, lat_count - 1), name="turn",
        in_specs=[pl.BlockSpec(memory_space=pltpu.SMEM)] + [pl.BlockSpec(memory_space=pltpu.VMEM)] * 3,
        out_shape=(shape(64, LANES),) * 3,
        scratch_shapes=[pltpu.VMEM((BLK + 32, LANES), F32)] * 2 + [pltpu.VMEM((64, LANES), F32)] * 4,
        compiler_params=limit(4),
    )(reach, *held(fields, second, first))

    evens, odds = range(0, lat_count, 2), range(1, lat_count - 1, 2)
    pairs = [(i, i + 1) for i in evens] + [(i + 1, i) for i in evens]
    swaps = [
        (i * lon_count + c, (i + s) * lon_count + c)
        for k in odds for i, s in ((k, 1), (k + 1, -1)) for c in range(lon_count)
    ]
    top = (lat_count - 1) * lon_count

    def second_round(value, pairing, others):
        fold = [(top + i, top + (2 * pairing - i) % lon_count) for i in range(lon_count)]
        return lax.ppermute(value, ("lat",) + LON, others + fold)

    def branch(index):
        def exchange(one, near, far, fields, second, first):
            value = second_round(near, index // 2, swaps)
            if index % 2:
                pairing = (index // 2 + 1) % (lon_count // 2)
                value = value + second_round(far, pairing, swaps if pairing == 0 else [])
            one = lax.ppermute(one, "lat", pairs)
            ready = call(
                prepare_kernel, name="prepare",
                out_shape=(shape(2, PITCH, LANES), shape(2, PITCH, LANES), shape(2, PITCH, LANES),
                           shape(2, 9, PITCH, LANES)),
                scratch_shapes=[pltpu.VMEM((BLK + 32, LANES), F32)] * 2,
                compiler_params=limit(4),
                cost_estimate=pl.CostEstimate(flops=4_000_000, transcendentals=0, bytes_accessed=0),
            )(*held(fields, second, first))
            landed = call(
                land_kernel, name="land", out_shape=(shape(64, LANES),) * 2, compiler_params=limit(2),
            )(*held(value, one))
            return *ready, *landed

        return exchange

    depth, side, inv, coef, south, north = lax.switch(
        choice[0], [branch(i) for i in range(lon_count)], one, two, two_next, fields, second, first
    )

    basis, sums, *_ = call(
        basis_kernel, name="basis",
        out_shape=(shape(VECTORS, PITCH, LANES), shape(lon_count, LANES), shape(2, PITCH, LANES),
                   shape(2, PITCH, LANES), shape(2, 9, PITCH, LANES)),
        scratch_shapes=[
            pltpu.VMEM((VECTORS, PITCH, LANES), F32),
            pltpu.VMEM((6 * STEPS, 8, LANES), F32),
        ],
        input_output_aliases={2: 2, 3: 3, 4: 4},
        compiler_params=limit(12),
    )(*held(fields, side, depth, inv, coef, south, north))
    sums = lax.all_to_all(sums, LON, split_axis=0, concat_axis=0, tiled=True)
    sums = call(middle_kernel, name="middle", out_shape=shape(lat_count, LANES), compiler_params=limit(2))(*held(sums))
    sums = lax.all_to_all(sums, "lat", split_axis=0, concat_axis=0, tiled=True)
    return call(
        final_kernel, name="final", out_shape=(jax.ShapeDtypeStruct((ROWS, LANES), F32),) * 2,
        out_specs=[pl.BlockSpec(memory_space=pl.ANY)] * 2,
        scratch_shapes=[pltpu.VMEM((ROWS, LANES), F32)] * 2 + [pltpu.SemaphoreType.DMA((8,))],
        compiler_params=limit(4),
    )(*held(sums, basis))


def solution(mesh):
    lon = mesh.shape["lon"]
    split = Mesh(mesh.devices.reshape(mesh.shape["lat"], lon // 4, 4), ("lat", "lon_0", "lon_1"))
    return jax.shard_map(
        per_device,
        mesh=split,
        in_specs=(P("lat", LON), P("lat", LON), P("lat", LON), P("lat", LON), P()),
        out_specs=(P("lat", LON), P("lat", LON)),
        check_vma=False,
    )
```

```python
import functools

import jax
import jax.numpy as jnp
from jax import lax
from jax.experimental import pallas as pl
from jax.experimental.pallas import tpu as pltpu
from jax.sharding import Mesh
from jax.sharding import PartitionSpec as P

STEPS = 8
REACH = 256
ROWS = 160
LANES = 128
EXT = ROWS + 32
PITCH = 216
EDGE = 9
BLK = 32
LON = ("lon_0", "lon_1")
VECTORS = 2 * STEPS + 1
F32 = jnp.float32


def edge_of(q, blk):
    return (9 * blk, 45 + 8 * blk, 85 + 8 * blk)[q], (9, 8, 8)[q]


def lanes_of(rows):
    return lax.broadcasted_iota(jnp.int32, (rows, LANES), 1)


def shift_east(a, b, lane):
    ra, rb = pltpu.roll(a, 1, 1), pltpu.roll(b, 1, 1)
    first = lane == 0
    return jnp.where(first, rb, ra), jnp.where(first, ra, rb)


def shift_west(a, b, lane):
    ra, rb = pltpu.roll(a, LANES - 1, 1), pltpu.roll(b, LANES - 1, 1)
    last = lane == LANES - 1
    return jnp.where(last, rb, ra), jnp.where(last, ra, rb)


def pack_kernel(pairs, f_hbm, p_hbm, d_hbm, m_hbm, map_hbm, x_ref, first_ref, second_ref, reach_ref, choice_ref,
                f_ref, p_ref, d_ref, m_ref, pivot, sems):
    even = turns(LON)
    copies = [
        pltpu.make_async_copy(source, target, sems.at[i])
        for i, (source, target) in enumerate((
            (m_hbm, m_ref), (d_hbm, d_ref), (f_hbm, f_ref), (p_hbm, p_ref), (map_hbm.at[pl.ds(0, LANES)], pivot),
        ))
    ]
    for copy in copies:
        copy.start()
    for copy in copies:
        copy.wait()
    for g in range(ROWS // 8):
        rows = pl.ds(8 * g, 8)
        flag = m_ref[rows, :].astype(F32)
        x_ref[0, rows, :] = d_ref[rows, :] * flag
        x_ref[1, rows, :] = f_ref[rows, :] * flag
        x_ref[2, rows, :] = p_ref[rows, :] * flag
    lane = lanes_of(8)
    for v in range(BLK // 8):
        east = jnp.zeros((8, LANES), F32)
        west = jnp.zeros((8, LANES), F32)
        for q in range(3):
            for blk in range(ROWS // BLK):
                at, width = edge_of(q, blk)
                tile = x_ref[q, pl.ds(BLK * blk + 8 * v, 8), :]
                tile = pltpu.roll(tile, at, 1) if at else tile
                west = jnp.where((lane >= at) & (lane < at + width), tile, west)
                start = (at - width) % LANES
                east = jnp.where((lane >= start) & (lane < start + width), tile, east)
        first_ref[pl.ds(8 * v, 8), :] = jnp.where(even, east, west)
        second_ref[pl.ds(8 * v, 8), :] = jnp.where(even, west, east)
    for slot, (q, row) in enumerate(((0, ROWS - 8), (1, ROWS - 8), (2, ROWS - 8), (0, ROWS - 16))):
        tile = x_ref[q, pl.ds(row, 8), :]
        first_ref[pl.ds(BLK + 8 * slot, 8), :] = tile
        second_ref[pl.ds(BLK + 8 * slot, 8), :] = tile
    past = pivot[0] + (2 * pairs * LANES - 8)
    reach = past % (2 * LANES) + 8
    reach_ref[0] = reach
    split = jnp.where(reach + EDGE >= 2 * LANES, 1, 0)
    choice_ref[0] = 2 * ((past // (2 * LANES)) % pairs) + split


def unpack_halo(from_west, from_east, q, blk, v, lane):
    at, width = edge_of(q, blk)
    right = from_east[pl.ds(8 * v, 8), :]
    left = from_west[pl.ds(8 * v, 8), :]
    both = jnp.where((lane >= at) & (lane < at + EDGE), right, left)
    both = pltpu.roll(both, LANES - at, 1) if at else both
    return jnp.where((lane < EDGE) | (lane >= LANES - EDGE), both, 0.0)


def turns(axis):
    place = lax.axis_index("lat")
    if axis == LON:
        place = place + lax.axis_index(LON)
    return place % 2 == 0


def sort_partners(axis, first, second, before, after):
    even = turns(axis)
    for g in range(first.shape[0] // 8):
        rows = pl.ds(8 * g, 8)
        a, b = first[rows, :], second[rows, :]
        before[rows, :] = jnp.where(even, b, a)
        after[rows, :] = jnp.where(even, a, b)


def turn_kernel(tops, r_ref, x_ref, second_ref, first_ref, one_ref, two_ref, next_ref,
                fw_ref, fe_ref, north_ref, south_ref, t1_ref, t2_ref):
    lane = lanes_of(8)
    lat = lax.axis_index("lat")
    even, top_row = lat % 2 == 0, lat == tops
    sort_partners(LON, first_ref, second_ref, fw_ref, fe_ref)
    top, low = ROWS // 8 - 1, 0
    for ref, rows in (
        (north_ref, ((0, top), (1, top), (2, top), (0, top - 1))),
        (south_ref, ((0, low), (1, low), (2, low), (0, low + 1))),
    ):
        for slot, (q, g) in enumerate(rows):
            ref[pl.ds(8 * slot, 8), :] = x_ref[q, pl.ds(8 * g, 8), :]
            blk, v = 8 * g // BLK, (8 * g % BLK) // 8
            ref[pl.ds(32 + 8 * slot, 8), :] = unpack_halo(fw_ref, fe_ref, q, blk, v, lane)
    for g in range(8):
        rows = pl.ds(8 * g, 8)
        north, south = north_ref[rows, :], south_ref[rows, :]
        one_ref[rows, :] = jnp.where(even, north, south)
        two_ref[rows, :] = jnp.where(even, south, north)
        next_ref[rows, :] = jnp.zeros((8, LANES), F32)

    @pl.when(top_row)
    def _():
        across_fold(r_ref[0], lane, north_ref, fw_ref, fe_ref, two_ref, next_ref, t1_ref, t2_ref)


def across_fold(reach, lane, north_ref, fw_ref, fe_ref, fold_ref, next_ref, t1_ref, t2_ref):
    along = reach - lane
    pick = along & (LANES - 1)
    place_a = along
    place_b = jnp.where(lane < EDGE, along - LANES, along + LANES)
    halo = (lane < EDGE) | (lane >= LANES - EDGE)
    for slot in range(4):
        rows = pl.ds(8 * slot, 8)
        own = jnp.take_along_axis(north_ref[rows, :], pick, axis=1, mode="promise_in_bounds")
        west = jnp.take_along_axis(fw_ref[pl.ds(BLK + 8 * slot, 8), :], pick, axis=1, mode="promise_in_bounds")
        east = jnp.take_along_axis(fe_ref[pl.ds(BLK + 8 * slot, 8), :], pick, axis=1, mode="promise_in_bounds")
        for part, place in ((0, place_a), (32, place_b)):
            near = jnp.where(place < 0, west, jnp.where(place < LANES, own, east))
            near = jnp.where(place < 2 * LANES, near, 0.0)
            far = jnp.where(place >= 2 * LANES, own, 0.0)
            if part:
                near = jnp.where(halo, near, 0.0)
                far = jnp.where(halo, far, 0.0)
            t1_ref[pl.ds(part + 8 * slot, 8), :] = near
            t2_ref[pl.ds(part + 8 * slot, 8), :] = far
    for g in range(8):
        for m in range(8):
            fold_ref[pl.ds(8 * g + m, 1), :] = t1_ref[pl.ds(8 * g + 7 - m, 1), :]
            next_ref[pl.ds(8 * g + m, 1), :] = t2_ref[pl.ds(8 * g + 7 - m, 1), :]


GROUPS = ROWS // 8 + 2


def root_of(depth, inv, at, lane):
    vert, mid, wet_mid, deep = [], [], [], []
    for t in range(2):
        down = depth[t, pl.ds(at - 1, 8), :]
        here = depth[t, pl.ds(at, 8), :]
        up = depth[t, pl.ds(at + 1, 8), :]
        wet = jnp.where(here > 0.0, 1.0, 0.0)
        wets = jnp.where(down > 0.0, 1.0, 0.0) + jnp.where(up > 0.0, 1.0, 0.0)
        vert.append((down + up, wets))
        mid.append((here + 0.5 * (down + up), wet + 0.5 * wets))
        deep.append(here)
        wet_mid.append(wet)
    sums = []
    for c in range(2):
        ea, eb = shift_east(mid[0][c], mid[1][c], lane)
        wa, wb = shift_west(mid[0][c], mid[1][c], lane)
        sums.append((vert[0][c] + (ea + wa), vert[1][c] + (eb + wb)))
    for t in range(2):
        links = 0.5 * (deep[t] * sums[1][t] + sums[0][t])
        diagonal = wet_mid[t] * (deep[t] / (REACH * REACH) + links) + (1.0 - wet_mid[t])
        inv[t, pl.ds(at, 8), :] = lax.rsqrt(diagonal) * wet_mid[t]


def coefs_of(depth, inv, coef, at, lane):
    d = [[depth[t, pl.ds(at + s, 8), :] for s in (-1, 0, 1)] for t in range(2)]
    r = [[inv[t, pl.ds(at + s, 8), :] for s in (-1, 0, 1)] for t in range(2)]
    de, re = shift_east(d[0][1], d[1][1], lane), shift_east(r[0][1], r[1][1], lane)
    dw, rw = shift_west(d[0][1], d[1][1], lane), shift_west(r[0][1], r[1][1], lane)
    for t in range(2):
        for base, (dc, rc) in enumerate(((d[t][1], r[t][1]), (de[t], re[t]), (dw[t], rw[t]))):
            for s in range(3):
                if base == 0 and s == 1:
                    continue
                whole = base == 0 or s == 1
                c = (dc + d[t][s]) * (rc * r[t][s])
                coef[t, 3 * base + s, pl.ds(at, 8), :] = c * (-1.0 if whole else -0.5)


def prepare_kernel(x_ref, second_ref, first_ref, depth, side, inv, coef, fw_ref, fe_ref):
    sort_partners(LON, first_ref, second_ref, fw_ref, fe_ref)
    lane = lanes_of(8)

    def unpack(v, carry):
        for q, ref in ((0, depth.at[1]), (1, side.at[1]), (2, side.at[0])):
            for blk in range(ROWS // BLK):
                rows = pl.ds(pl.multiple_of(16 + BLK * blk + 8 * v, 8), 8)
                ref[rows, :] = unpack_halo(fw_ref, fe_ref, q, blk, v, lane)
        return carry

    for g in range(ROWS // 8):
        depth[0, pl.ds(16 + 8 * g, 8), :] = x_ref[0, pl.ds(8 * g, 8), :]
    lax.fori_loop(0, BLK // 8, unpack, 0)

    def roots(i, carry):
        for g in range(6):
            root_of(depth, inv, pl.multiple_of(24 + 48 * i, 8) + 8 * g, lane)
        return carry

    def coefs(i, carry):
        for g in range(4):
            coefs_of(depth, inv, coef, pl.multiple_of(32 + 32 * i, 8) + 8 * g, lane)
        return carry

    lax.fori_loop(0, 3, roots, 0)
    lax.fori_loop(0, 4, coefs, 0)


def land_kernel(two_ref, one_ref, south_ref, north_ref):
    sort_partners("lat", one_ref, two_ref, south_ref, north_ref)


def basis_kernel(x_ref, side_ref, _depth, _inv, _coef, fs_ref, fn_ref, basis_ref, sums_ref, depth, inv, coef,
                 side, acc):
    lane = lanes_of(8)
    zero = jnp.zeros((8, LANES), F32)
    for q, k in ((1, STEPS + 1), (2, 0)):
        for g in range(ROWS // 8):
            rows = pl.ds(16 + 8 * g, 8)
            basis_ref[k, rows, :] = x_ref[q, pl.ds(8 * g, 8), :]
            side[k, rows, :] = side_ref[2 - q, rows, :]
    targets = (
        lambda t: depth.at[t],
        lambda t: (basis_ref if t == 0 else side).at[STEPS + 1],
        lambda t: (basis_ref if t == 0 else side).at[0],
    )
    for q in range(3):
        own, rim = targets[q](0), targets[q](1)
        for t, ref in ((0, own), (1, rim)):
            at = 32 * t + 8 * q
            ref[pl.ds(8, 8), :] = fs_ref[pl.ds(at, 8), :]
            ref[pl.ds(EXT - 16, 8), :] = fn_ref[pl.ds(at, 8), :]
            if q == 0:
                at = 32 * t + 24
                ref[pl.ds(0, 8), :] = fs_ref[pl.ds(at, 8), :]
                ref[pl.ds(EXT - 8, 8), :] = fn_ref[pl.ds(at, 8), :]
            else:
                ref[pl.ds(0, 8), :] = zero
                ref[pl.ds(EXT - 8, 8), :] = zero
    for k in list(range(1, STEPS + 1)) + list(range(STEPS + 2, VECTORS)):
        for ref in (basis_ref, side):
            ref[k, pl.ds(0, 8), :] = zero
            ref[k, pl.ds(EXT - 8, 8), :] = zero
    for t in range(2):
        inv[t, pl.ds(0, 8), :] = zero
        inv[t, pl.ds(EXT - 8, 8), :] = zero

    for g in (0, 1, GROUPS - 2, GROUPS - 1):
        root_of(depth, inv, 8 + 8 * g, lane)
    for g in (0, 1, 2, GROUPS - 3, GROUPS - 2, GROUPS - 1):
        coefs_of(depth, inv, coef, 8 + 8 * g, lane)

    def twice_applied(k, at, tiles, weights):
        parts = []
        for t in range(2):
            ref = basis_ref if t == 0 else side
            down, here, up = (ref[k, pl.ds(at + s, 8), :] for s in (-1, 0, 1))
            w = weights[t]
            straight = w[0] * down + w[2] * up
            toward_w = (w[3] * down + w[5] * up) + w[4] * here
            toward_e = (w[6] * down + w[8] * up) + w[7] * here
            parts.append((straight, toward_w, toward_e, here))
        wa, wb = shift_west(parts[0][1], parts[1][1], lane)
        ea, eb = shift_east(parts[0][2], parts[1][2], lane)
        return ((parts[0][0] + (wa + ea), parts[1][0] + (wb + eb))[:tiles], parts[0][3])

    def weights_at(at):
        return [[None if i == 1 else coef[t, i, pl.ds(at, 8), :] for i in range(9)] for t in range(2)]

    def step(k, first, last):
        total = [zero] * 6
        tiles = 1 if last else 2
        for g in range(1, GROUPS - 1) if last else range(GROUPS):
            at = 8 + 8 * g
            w = weights_at(at)
            now, new = [], []
            for base in ((0,) if last else (0, STEPS + 1)):
                out, here = twice_applied(base + k, at, tiles, w)
                now.append(here)
                for t in range(tiles):
                    ref = basis_ref if t == 0 else side
                    value = 0.5 * out[t] if first else out[t] - ref[base + k - 1, pl.ds(at, 8), :]
                    ref[base + k + 1, pl.ds(at, 8), :] = value
                    if t == 0:
                        new.append(value)
            if last:
                now.append(basis_ref[STEPS + 1 + k, pl.ds(at, 8), :])
            if 1 <= g <= ROWS // 8:
                p, r = now
                total[0] += p * p
                total[1] += p * new[0]
                total[2] += r * r
                total[3] += new[0] * new[0] if last else r * new[1]
                total[4] += p * r
                total[5] += new[0] * r
        for i in range(6):
            acc[6 * k + i, :, :] = total[i]

    step(0, True, False)

    def middle(k, carry):
        step(k, False, False)
        return carry

    lax.fori_loop(1, STEPS - 1, middle, 0, unroll=2)
    step(STEPS - 1, False, True)

    flat = jnp.sum(acc[...], axis=1)
    flat = jnp.concatenate([flat, jnp.zeros((LANES - 6 * STEPS, LANES), F32)], axis=0)
    row = jnp.broadcast_to(jnp.sum(flat.T, axis=0, keepdims=True), (8, LANES))
    for g in range(sums_ref.shape[0] // 8):
        sums_ref[pl.ds(8 * g, 8), :] = row


def middle_kernel(in_ref, out_ref):
    out_ref[...] = jnp.broadcast_to(jnp.sum(in_ref[...], axis=0, keepdims=True), out_ref.shape)


def final_kernel(sum_ref, basis_ref, height_hbm, residual_hbm, height_ref, residual_ref, sems):
    products = jnp.broadcast_to(jnp.sum(sum_ref[...], axis=0, keepdims=True), (8, LANES))
    row = lax.broadcasted_iota(jnp.int32, (24, LANES), 0)
    first = row == 0
    odd = row & 1

    def gathered(index):
        parts = [
            jnp.take_along_axis(products, index[8 * g : 8 * g + 8], axis=1, mode="promise_in_bounds")
            for g in range(3)
        ]
        return jnp.concatenate(parts, axis=0)

    def moments(slot, count):
        index = jnp.where(row < count, 6 * (row >> 1) + odd + slot, LANES - 1)
        if count > 2 * STEPS:
            index = jnp.where(row == 2 * STEPS, 6 * (STEPS - 1) + 3, index)
        return 2.0 * gathered(index) - gathered(jnp.where(row < count, odd + slot, LANES - 1))

    def raised(v):
        up = pltpu.roll(v, 23, 0)
        return v + 0.5 * (up + jnp.where(first, up, pltpu.roll(v, 1, 0)))

    def mapped(v):
        down = pltpu.roll(jnp.where(first, v, 0.5 * v), 1, 0)
        return v + down + pltpu.roll(jnp.where(first, 0.0, 0.5 * v), 23, 0)

    def dot(u, v):
        return jnp.sum(u[0] * v[0] + u[1] * v[1], axis=0, keepdims=True)

    pair = (0, 1)
    unit, zero = jnp.where(first, 1.0, 0.0), jnp.zeros((24, LANES), F32)
    pp, rr, pr = moments(0, 2 * STEPS + 1), moments(2, 2 * STEPS - 1), moments(4, 2 * STEPS)
    xc, pc, rc = (zero, zero), (unit, zero), (zero, unit)
    with_r, with_q = (pr, rr), (raised(pp), raised(pr))
    norm = dot(rc, with_r)
    for _ in range(STEPS):
        t = norm / dot(pc, with_q)
        inverse = 1.0 / norm
        with_r = [with_r[i] - t * with_q[i] for i in pair]
        rc, xc = [rc[i] - t * mapped(pc[i]) for i in pair], [xc[i] + t * pc[i] for i in pair]
        norm = dot(rc, with_r)
        ratio = norm * inverse
        with_q = [raised(with_r[i]) + ratio * with_q[i] for i in pair]
        pc = [rc[i] + ratio * pc[i] for i in pair]
    spots = [(0, k) for k in range(STEPS + 1)] + [(1, k) for k in range(STEPS)]
    xs = [jnp.broadcast_to(xc[i][k : k + 1, :], (8, LANES)) for i, k in spots]
    rs = [jnp.broadcast_to(rc[i][k : k + 1, :], (8, LANES)) for i, k in spots]
    copies = []
    for part in range(4):
        for g in range(part * ROWS // 32, (part + 1) * ROWS // 32):
            above = below = None
            for k in range(VECTORS):
                tile = basis_ref[k, pl.ds(16 + 8 * g, 8), :]
                above = xs[k] * tile if above is None else above + xs[k] * tile
                below = rs[k] * tile if below is None else below + rs[k] * tile
            height_ref[pl.ds(8 * g, 8), :] = above
            residual_ref[pl.ds(8 * g, 8), :] = below
        rows = pl.ds(part * ROWS // 4, ROWS // 4)
        for i, (source, target) in enumerate(((height_ref, height_hbm), (residual_ref, residual_hbm))):
            copies.append(pltpu.make_async_copy(source.at[rows], target.at[rows], sems.at[2 * part + i]))
            copies[-1].start()
    for copy in copies:
        copy.wait()


def shape(*dims):
    return pltpu.VMEM(dims, F32)


def held(*values, space=pltpu.VMEM):
    return tuple(pltpu.with_memory_space_constraint(v, space) for v in values)


def limit(mib):
    return pltpu.CompilerParams(vmem_limit_bytes=mib << 20)


def per_device(forcing, search_direction, ocean_depth, land_mask, fold_map):
    lat_count, lon_count = lax.axis_size("lat"), lax.axis_size(LON)
    call = pl.pallas_call
    fields, first, second, reach, choice = call(
        functools.partial(pack_kernel, lon_count // 2), name="pack",
        in_specs=[pl.BlockSpec(memory_space=pl.ANY)] * 5,
        out_specs=[pl.BlockSpec(memory_space=pltpu.VMEM)] * 3 + [pl.BlockSpec(memory_space=pltpu.SMEM)] * 2,
        out_shape=(shape(3, ROWS, LANES), shape(BLK + 32, LANES), shape(BLK + 32, LANES),
                   pltpu.SMEM((1,), jnp.int32), pltpu.SMEM((1,), jnp.int32)),
        scratch_shapes=[pltpu.VMEM((ROWS, LANES), F32)] * 3 + [
            pltpu.VMEM((ROWS, LANES), jnp.int32), pltpu.SMEM((LANES,), jnp.int32), pltpu.SemaphoreType.DMA((5,)),
        ],
        compiler_params=limit(4),
    )(*held(forcing, search_direction, ocean_depth, land_mask, fold_map, space=pltpu.HBM))
    def lon_round(start):
        pairs = []
        for row in range(lat_count):
            for i in range((start + row) % 2, lon_count, 2):
                a, b = row * lon_count + i, row * lon_count + (i + 1) % lon_count
                pairs += [(a, b), (b, a)]
        return pairs

    second = lax.ppermute(second, ("lat",) + LON, lon_round(1))
    first = lax.ppermute(first, ("lat",) + LON, lon_round(0))

    one, two, two_next = call(
        functools.partial(turn_kernel, lat_count - 1), name="turn",
        in_specs=[pl.BlockSpec(memory_space=pltpu.SMEM)] + [pl.BlockSpec(memory_space=pltpu.VMEM)] * 3,
        out_shape=(shape(64, LANES),) * 3,
        scratch_shapes=[pltpu.VMEM((BLK + 32, LANES), F32)] * 2 + [pltpu.VMEM((64, LANES), F32)] * 4,
        compiler_params=limit(4),
    )(reach, *held(fields, second, first))

    evens, odds = range(0, lat_count, 2), range(1, lat_count - 1, 2)
    pairs = [(i, i + 1) for i in evens] + [(i + 1, i) for i in evens]
    swaps = [
        (i * lon_count + c, (i + s) * lon_count + c)
        for k in odds for i, s in ((k, 1), (k + 1, -1)) for c in range(lon_count)
    ]
    top = (lat_count - 1) * lon_count

    def second_round(value, pairing, others):
        fold = [(top + i, top + (2 * pairing - i) % lon_count) for i in range(lon_count)]
        return lax.ppermute(value, ("lat",) + LON, others + fold)

    def branch(index):
        def exchange(one, near, far, fields, second, first):
            value = second_round(near, index // 2, swaps)
            if index % 2:
                pairing = (index // 2 + 1) % (lon_count // 2)
                value = value + second_round(far, pairing, swaps if pairing == 0 else [])
            one = lax.ppermute(one, "lat", pairs)
            ready = call(
                prepare_kernel, name="prepare",
                out_shape=(shape(2, PITCH, LANES), shape(2, PITCH, LANES), shape(2, PITCH, LANES),
                           shape(2, 9, PITCH, LANES)),
                scratch_shapes=[pltpu.VMEM((BLK + 32, LANES), F32)] * 2,
                compiler_params=limit(4),
                cost_estimate=pl.CostEstimate(flops=4_000_000, transcendentals=0, bytes_accessed=0),
            )(*held(fields, second, first))
            landed = call(
                land_kernel, name="land", out_shape=(shape(64, LANES),) * 2, compiler_params=limit(2),
            )(*held(value, one))
            return *ready, *landed

        return exchange

    depth, side, inv, coef, south, north = lax.switch(
        choice[0], [branch(i) for i in range(lon_count)], one, two, two_next, fields, second, first
    )

    basis, sums, *_ = call(
        basis_kernel, name="basis",
        out_shape=(shape(VECTORS, PITCH, LANES), shape(lat_count, LANES), shape(2, PITCH, LANES),
                   shape(2, PITCH, LANES), shape(2, 9, PITCH, LANES)),
        scratch_shapes=[
            pltpu.VMEM((VECTORS, PITCH, LANES), F32),
            pltpu.VMEM((6 * STEPS, 8, LANES), F32),
        ],
        input_output_aliases={2: 2, 3: 3, 4: 4},
        compiler_params=limit(12),
    )(*held(fields, side, depth, inv, coef, south, north))
    sums = lax.all_to_all(sums, "lat", split_axis=0, concat_axis=0, tiled=True)
    sums = call(middle_kernel, name="middle", out_shape=shape(lon_count, LANES), compiler_params=limit(2))(*held(sums))
    sums = lax.all_to_all(sums, LON, split_axis=0, concat_axis=0, tiled=True)
    return call(
        final_kernel, name="final", out_shape=(jax.ShapeDtypeStruct((ROWS, LANES), F32),) * 2,
        out_specs=[pl.BlockSpec(memory_space=pl.ANY)] * 2,
        scratch_shapes=[pltpu.VMEM((ROWS, LANES), F32)] * 2 + [pltpu.SemaphoreType.DMA((8,))],
        compiler_params=limit(4),
    )(*held(sums, basis))


def solution(mesh):
    lon = mesh.shape["lon"]
    split = Mesh(mesh.devices.reshape(mesh.shape["lat"], lon // 4, 4), ("lat", "lon_0", "lon_1"))
    return jax.shard_map(
        per_device,
        mesh=split,
        in_specs=(P("lat", LON), P("lat", LON), P("lat", LON), P("lat", LON), P()),
        out_specs=(P("lat", LON), P("lat", LON)),
        check_vma=False,
    )
```

```python
import functools

import jax
import jax.numpy as jnp
from jax import lax
from jax.experimental import pallas as pl
from jax.experimental.pallas import tpu as pltpu
from jax.sharding import Mesh
from jax.sharding import PartitionSpec as P

STEPS = 8
REACH = 256
ROWS = 160
LANES = 128
EXT = ROWS + 32
PITCH = 216
EDGE = 9
BLK = 32
LON = ("lon_0", "lon_1")
VECTORS = 2 * STEPS + 1
F32 = jnp.float32


def edge_of(q, blk):
    return (9 * blk, 45 + 8 * blk, 85 + 8 * blk)[q], (9, 8, 8)[q]


def lanes_of(rows):
    return lax.broadcasted_iota(jnp.int32, (rows, LANES), 1)


def shift_east(a, b, lane):
    ra, rb = pltpu.roll(a, 1, 1), pltpu.roll(b, 1, 1)
    first = lane == 0
    return jnp.where(first, rb, ra), jnp.where(first, ra, rb)


def shift_west(a, b, lane):
    ra, rb = pltpu.roll(a, LANES - 1, 1), pltpu.roll(b, LANES - 1, 1)
    last = lane == LANES - 1
    return jnp.where(last, rb, ra), jnp.where(last, ra, rb)


def pack_kernel(pairs, f_hbm, p_hbm, d_hbm, m_hbm, map_hbm, x_ref, first_ref, second_ref, reach_ref, choice_ref,
                f_ref, p_ref, d_ref, m_ref, pivot, sems):
    even = turns(LON)
    copies = [
        pltpu.make_async_copy(source, target, sems.at[i])
        for i, (source, target) in enumerate((
            (m_hbm, m_ref), (d_hbm, d_ref), (f_hbm, f_ref), (p_hbm, p_ref), (map_hbm.at[pl.ds(0, LANES)], pivot),
        ))
    ]
    for copy in copies:
        copy.start()
    for copy in copies:
        copy.wait()
    for g in range(ROWS // 8):
        rows = pl.ds(8 * g, 8)
        flag = m_ref[rows, :].astype(F32)
        x_ref[0, rows, :] = d_ref[rows, :] * flag
        x_ref[1, rows, :] = f_ref[rows, :] * flag
        x_ref[2, rows, :] = p_ref[rows, :] * flag
    lane = lanes_of(8)
    for v in range(BLK // 8):
        east = jnp.zeros((8, LANES), F32)
        west = jnp.zeros((8, LANES), F32)
        for q in range(3):
            for blk in range(ROWS // BLK):
                at, width = edge_of(q, blk)
                tile = x_ref[q, pl.ds(BLK * blk + 8 * v, 8), :]
                tile = pltpu.roll(tile, at, 1) if at else tile
                west = jnp.where((lane >= at) & (lane < at + width), tile, west)
                start = (at - width) % LANES
                east = jnp.where((lane >= start) & (lane < start + width), tile, east)
        first_ref[pl.ds(8 * v, 8), :] = jnp.where(even, east, west)
        second_ref[pl.ds(8 * v, 8), :] = jnp.where(even, west, east)
    for slot, (q, row) in enumerate(((0, ROWS - 8), (1, ROWS - 8), (2, ROWS - 8), (0, ROWS - 16))):
        tile = x_ref[q, pl.ds(row, 8), :]
        first_ref[pl.ds(BLK + 8 * slot, 8), :] = tile
        second_ref[pl.ds(BLK + 8 * slot, 8), :] = tile
    past = pivot[0] + (2 * pairs * LANES - 8)
    reach = past % (2 * LANES) + 8
    reach_ref[0] = reach
    split = jnp.where(reach + EDGE >= 2 * LANES, 1, 0)
    choice_ref[0] = 2 * ((past // (2 * LANES)) % pairs) + split


def unpack_halo(from_west, from_east, q, blk, v, lane):
    at, width = edge_of(q, blk)
    right = from_east[pl.ds(8 * v, 8), :]
    left = from_west[pl.ds(8 * v, 8), :]
    both = jnp.where((lane >= at) & (lane < at + EDGE), right, left)
    both = pltpu.roll(both, LANES - at, 1) if at else both
    return jnp.where((lane < EDGE) | (lane >= LANES - EDGE), both, 0.0)


def turns(axis):
    place = lax.axis_index("lat")
    if axis == LON:
        place = place + lax.axis_index(LON)
    return place % 2 == 0


def sort_partners(axis, first, second, before, after):
    even = turns(axis)
    for g in range(first.shape[0] // 8):
        rows = pl.ds(8 * g, 8)
        a, b = first[rows, :], second[rows, :]
        before[rows, :] = jnp.where(even, b, a)
        after[rows, :] = jnp.where(even, a, b)


def turn_kernel(tops, r_ref, x_ref, second_ref, first_ref, one_ref, two_ref, next_ref,
                fw_ref, fe_ref, north_ref, south_ref, t1_ref, t2_ref):
    lane = lanes_of(8)
    lat = lax.axis_index("lat")
    even, top_row = lat % 2 == 0, lat == tops
    sort_partners(LON, first_ref, second_ref, fw_ref, fe_ref)
    top, low = ROWS // 8 - 1, 0
    for ref, rows in (
        (north_ref, ((0, top), (1, top), (2, top), (0, top - 1))),
        (south_ref, ((0, low), (1, low), (2, low), (0, low + 1))),
    ):
        for slot, (q, g) in enumerate(rows):
            ref[pl.ds(8 * slot, 8), :] = x_ref[q, pl.ds(8 * g, 8), :]
            blk, v = 8 * g // BLK, (8 * g % BLK) // 8
            ref[pl.ds(32 + 8 * slot, 8), :] = unpack_halo(fw_ref, fe_ref, q, blk, v, lane)
    for g in range(8):
        rows = pl.ds(8 * g, 8)
        north, south = north_ref[rows, :], south_ref[rows, :]
        one_ref[rows, :] = jnp.where(even, north, south)
        two_ref[rows, :] = jnp.where(even, south, north)
        next_ref[rows, :] = jnp.zeros((8, LANES), F32)

    @pl.when(top_row)
    def _():
        across_fold(r_ref[0], lane, north_ref, fw_ref, fe_ref, two_ref, next_ref, t1_ref, t2_ref)


def across_fold(reach, lane, north_ref, fw_ref, fe_ref, fold_ref, next_ref, t1_ref, t2_ref):
    along = reach - lane
    pick = along & (LANES - 1)
    place_a = along
    place_b = jnp.where(lane < EDGE, along - LANES, along + LANES)
    halo = (lane < EDGE) | (lane >= LANES - EDGE)
    for slot in range(4):
        rows = pl.ds(8 * slot, 8)
        own = jnp.take_along_axis(north_ref[rows, :], pick, axis=1, mode="promise_in_bounds")
        west = jnp.take_along_axis(fw_ref[pl.ds(BLK + 8 * slot, 8), :], pick, axis=1, mode="promise_in_bounds")
        east = jnp.take_along_axis(fe_ref[pl.ds(BLK + 8 * slot, 8), :], pick, axis=1, mode="promise_in_bounds")
        for part, place in ((0, place_a), (32, place_b)):
            near = jnp.where(place < 0, west, jnp.where(place < LANES, own, east))
            near = jnp.where(place < 2 * LANES, near, 0.0)
            far = jnp.where(place >= 2 * LANES, own, 0.0)
            if part:
                near = jnp.where(halo, near, 0.0)
                far = jnp.where(halo, far, 0.0)
            t1_ref[pl.ds(part + 8 * slot, 8), :] = near
            t2_ref[pl.ds(part + 8 * slot, 8), :] = far
    for g in range(8):
        for m in range(8):
            fold_ref[pl.ds(8 * g + m, 1), :] = t1_ref[pl.ds(8 * g + 7 - m, 1), :]
            next_ref[pl.ds(8 * g + m, 1), :] = t2_ref[pl.ds(8 * g + 7 - m, 1), :]


GROUPS = ROWS // 8 + 2


def root_of(depth, inv, at, lane):
    vert, mid, wet_mid, deep = [], [], [], []
    for t in range(2):
        down = depth[t, pl.ds(at - 1, 8), :]
        here = depth[t, pl.ds(at, 8), :]
        up = depth[t, pl.ds(at + 1, 8), :]
        wet = jnp.where(here > 0.0, 1.0, 0.0)
        wets = jnp.where(down > 0.0, 1.0, 0.0) + jnp.where(up > 0.0, 1.0, 0.0)
        vert.append((down + up, wets))
        mid.append((here + 0.5 * (down + up), wet + 0.5 * wets))
        deep.append(here)
        wet_mid.append(wet)
    sums = []
    for c in range(2):
        ea, eb = shift_east(mid[0][c], mid[1][c], lane)
        wa, wb = shift_west(mid[0][c], mid[1][c], lane)
        sums.append((vert[0][c] + (ea + wa), vert[1][c] + (eb + wb)))
    for t in range(2):
        links = 0.5 * (deep[t] * sums[1][t] + sums[0][t])
        diagonal = wet_mid[t] * (deep[t] / (REACH * REACH) + links) + (1.0 - wet_mid[t])
        inv[t, pl.ds(at, 8), :] = lax.rsqrt(diagonal) * wet_mid[t]


def coefs_of(depth, inv, coef, at, lane):
    d = [[depth[t, pl.ds(at + s, 8), :] for s in (-1, 0, 1)] for t in range(2)]
    r = [[inv[t, pl.ds(at + s, 8), :] for s in (-1, 0, 1)] for t in range(2)]
    de, re = shift_east(d[0][1], d[1][1], lane), shift_east(r[0][1], r[1][1], lane)
    dw, rw = shift_west(d[0][1], d[1][1], lane), shift_west(r[0][1], r[1][1], lane)
    for t in range(2):
        for base, (dc, rc) in enumerate(((d[t][1], r[t][1]), (de[t], re[t]), (dw[t], rw[t]))):
            for s in range(3):
                if base == 0 and s == 1:
                    continue
                whole = base == 0 or s == 1
                c = (dc + d[t][s]) * (rc * r[t][s])
                coef[t, 3 * base + s, pl.ds(at, 8), :] = c * (-1.0 if whole else -0.5)


def prepare_kernel(x_ref, second_ref, first_ref, depth, side, inv, coef, fw_ref, fe_ref):
    sort_partners(LON, first_ref, second_ref, fw_ref, fe_ref)
    lane = lanes_of(8)

    def unpack(v, carry):
        for q, ref in ((0, depth.at[1]), (1, side.at[1]), (2, side.at[0])):
            for blk in range(ROWS // BLK):
                rows = pl.ds(pl.multiple_of(16 + BLK * blk + 8 * v, 8), 8)
                ref[rows, :] = unpack_halo(fw_ref, fe_ref, q, blk, v, lane)
        return carry

    for g in range(ROWS // 8):
        depth[0, pl.ds(16 + 8 * g, 8), :] = x_ref[0, pl.ds(8 * g, 8), :]
    lax.fori_loop(0, BLK // 8, unpack, 0)

    def roots(i, carry):
        for g in range(6):
            root_of(depth, inv, pl.multiple_of(24 + 48 * i, 8) + 8 * g, lane)
        return carry

    def coefs(i, carry):
        for g in range(4):
            coefs_of(depth, inv, coef, pl.multiple_of(32 + 32 * i, 8) + 8 * g, lane)
        return carry

    lax.fori_loop(0, 3, roots, 0)
    lax.fori_loop(0, 4, coefs, 0)


def land_kernel(two_ref, one_ref, south_ref, north_ref):
    sort_partners("lat", one_ref, two_ref, south_ref, north_ref)


def basis_kernel(x_ref, side_ref, _depth, _inv, _coef, fs_ref, fn_ref, basis_ref, sums_ref, depth, inv, coef,
                 side, acc):
    lane = lanes_of(8)
    zero = jnp.zeros((8, LANES), F32)
    for q, k in ((1, STEPS + 1), (2, 0)):
        for g in range(ROWS // 8):
            rows = pl.ds(16 + 8 * g, 8)
            basis_ref[k, rows, :] = x_ref[q, pl.ds(8 * g, 8), :]
            side[k, rows, :] = side_ref[2 - q, rows, :]
    targets = (
        lambda t: depth.at[t],
        lambda t: (basis_ref if t == 0 else side).at[STEPS + 1],
        lambda t: (basis_ref if t == 0 else side).at[0],
    )
    for q in range(3):
        own, rim = targets[q](0), targets[q](1)
        for t, ref in ((0, own), (1, rim)):
            at = 32 * t + 8 * q
            ref[pl.ds(8, 8), :] = fs_ref[pl.ds(at, 8), :]
            ref[pl.ds(EXT - 16, 8), :] = fn_ref[pl.ds(at, 8), :]
            if q == 0:
                at = 32 * t + 24
                ref[pl.ds(0, 8), :] = fs_ref[pl.ds(at, 8), :]
                ref[pl.ds(EXT - 8, 8), :] = fn_ref[pl.ds(at, 8), :]
            else:
                ref[pl.ds(0, 8), :] = zero
                ref[pl.ds(EXT - 8, 8), :] = zero
    for k in list(range(1, STEPS + 1)) + list(range(STEPS + 2, VECTORS)):
        for ref in (basis_ref, side):
            ref[k, pl.ds(0, 8), :] = zero
            ref[k, pl.ds(EXT - 8, 8), :] = zero
    for t in range(2):
        inv[t, pl.ds(0, 8), :] = zero
        inv[t, pl.ds(EXT - 8, 8), :] = zero

    for g in (0, 1, GROUPS - 2, GROUPS - 1):
        root_of(depth, inv, 8 + 8 * g, lane)
    for g in (0, 1, 2, GROUPS - 3, GROUPS - 2, GROUPS - 1):
        coefs_of(depth, inv, coef, 8 + 8 * g, lane)

    def twice_applied(k, at, tiles, weights):
        parts = []
        for t in range(2):
            ref = basis_ref if t == 0 else side
            down, here, up = (ref[k, pl.ds(at + s, 8), :] for s in (-1, 0, 1))
            w = weights[t]
            straight = w[0] * down + w[2] * up
            toward_w = (w[3] * down + w[5] * up) + w[4] * here
            toward_e = (w[6] * down + w[8] * up) + w[7] * here
            parts.append((straight, toward_w, toward_e, here))
        wa, wb = shift_west(parts[0][1], parts[1][1], lane)
        ea, eb = shift_east(parts[0][2], parts[1][2], lane)
        return ((parts[0][0] + (wa + ea), parts[1][0] + (wb + eb))[:tiles], parts[0][3])

    def weights_at(at):
        return [[None if i == 1 else coef[t, i, pl.ds(at, 8), :] for i in range(9)] for t in range(2)]

    def step(k, first, last, trim=False):
        total = [zero] * 6
        tiles = 1 if last else 2
        for g in range(1, GROUPS - 1) if last else range(GROUPS):
            at = 8 + 8 * g
            w = weights_at(at)
            now, new = [], []
            inner = 1 <= g <= ROWS // 8
            for base in ((0,) if last or (trim and not inner) else (0, STEPS + 1)):
                count = 1 if trim and base else tiles
                out, here = twice_applied(base + k, at, count, w)
                now.append(here)
                for t in range(count):
                    ref = basis_ref if t == 0 else side
                    value = 0.5 * out[t] if first else out[t] - ref[base + k - 1, pl.ds(at, 8), :]
                    ref[base + k + 1, pl.ds(at, 8), :] = value
                    if t == 0:
                        new.append(value)
            if last:
                now.append(basis_ref[STEPS + 1 + k, pl.ds(at, 8), :])
            if inner:
                p, r = now
                total[0] += p * p
                total[1] += p * new[0]
                total[2] += r * r
                total[3] += new[0] * new[0] if last else r * new[1]
                total[4] += p * r
                total[5] += new[0] * r
        for i in range(6):
            acc[6 * k + i, :, :] = total[i]

    step(0, True, False)

    def middle(k, carry):
        step(k, False, False)
        return carry

    lax.fori_loop(1, STEPS - 2, middle, 0, unroll=5)
    step(STEPS - 2, False, False, True)
    step(STEPS - 1, False, True)

    flat = jnp.sum(acc[...], axis=1)
    flat = jnp.concatenate([flat, jnp.zeros((LANES - 6 * STEPS, LANES), F32)], axis=0)
    row = jnp.broadcast_to(jnp.sum(flat.T, axis=0, keepdims=True), (8, LANES))
    for g in range(sums_ref.shape[0] // 8):
        sums_ref[pl.ds(8 * g, 8), :] = row


def middle_kernel(in_ref, out_ref):
    out_ref[...] = jnp.broadcast_to(jnp.sum(in_ref[...], axis=0, keepdims=True), out_ref.shape)


def final_kernel(sum_ref, basis_ref, height_hbm, residual_hbm, height_ref, residual_ref, sems):
    products = jnp.broadcast_to(jnp.sum(sum_ref[...], axis=0, keepdims=True), (8, LANES))
    row = lax.broadcasted_iota(jnp.int32, (24, LANES), 0)
    first = row == 0
    odd = row & 1

    def gathered(index):
        parts = [
            jnp.take_along_axis(products, index[8 * g : 8 * g + 8], axis=1, mode="promise_in_bounds")
            for g in range(3)
        ]
        return jnp.concatenate(parts, axis=0)

    def moments(slot, count):
        index = jnp.where(row < count, 6 * (row >> 1) + odd + slot, LANES - 1)
        if count > 2 * STEPS:
            index = jnp.where(row == 2 * STEPS, 6 * (STEPS - 1) + 3, index)
        return 2.0 * gathered(index) - gathered(jnp.where(row < count, odd + slot, LANES - 1))

    def raised(v):
        up = pltpu.roll(v, 23, 0)
        return v + 0.5 * (up + jnp.where(first, up, pltpu.roll(v, 1, 0)))

    def mapped(v):
        down = pltpu.roll(jnp.where(first, v, 0.5 * v), 1, 0)
        return v + down + pltpu.roll(jnp.where(first, 0.0, 0.5 * v), 23, 0)

    def dot(u, v):
        return jnp.sum(u[0] * v[0] + u[1] * v[1], axis=0, keepdims=True)

    pair = (0, 1)
    unit, zero = jnp.where(first, 1.0, 0.0), jnp.zeros((24, LANES), F32)
    pp, rr, pr = moments(0, 2 * STEPS + 1), moments(2, 2 * STEPS - 1), moments(4, 2 * STEPS)
    xc, pc, rc = (zero, zero), (unit, zero), (zero, unit)
    with_r, with_q = (pr, rr), (raised(pp), raised(pr))
    norm = dot(rc, with_r)
    for _ in range(STEPS):
        t = norm / dot(pc, with_q)
        inverse = 1.0 / norm
        with_r = [with_r[i] - t * with_q[i] for i in pair]
        rc, xc = [rc[i] - t * mapped(pc[i]) for i in pair], [xc[i] + t * pc[i] for i in pair]
        norm = dot(rc, with_r)
        ratio = norm * inverse
        with_q = [raised(with_r[i]) + ratio * with_q[i] for i in pair]
        pc = [rc[i] + ratio * pc[i] for i in pair]
    spots = [(0, k) for k in range(STEPS + 1)] + [(1, k) for k in range(STEPS)]
    xs = [jnp.broadcast_to(xc[i][k : k + 1, :], (8, LANES)) for i, k in spots]
    rs = [jnp.broadcast_to(rc[i][k : k + 1, :], (8, LANES)) for i, k in spots]
    copies = []
    for part in range(4):
        for g in range(part * ROWS // 32, (part + 1) * ROWS // 32):
            above = below = None
            for k in range(VECTORS):
                tile = basis_ref[k, pl.ds(16 + 8 * g, 8), :]
                above = xs[k] * tile if above is None else above + xs[k] * tile
                below = rs[k] * tile if below is None else below + rs[k] * tile
            height_ref[pl.ds(8 * g, 8), :] = above
            residual_ref[pl.ds(8 * g, 8), :] = below
        rows = pl.ds(part * ROWS // 4, ROWS // 4)
        for i, (source, target) in enumerate(((height_ref, height_hbm), (residual_ref, residual_hbm))):
            copies.append(pltpu.make_async_copy(source.at[rows], target.at[rows], sems.at[2 * part + i]))
            copies[-1].start()
    for copy in copies:
        copy.wait()


def shape(*dims):
    return pltpu.VMEM(dims, F32)


def held(*values, space=pltpu.VMEM):
    return tuple(pltpu.with_memory_space_constraint(v, space) for v in values)


def limit(mib):
    return pltpu.CompilerParams(vmem_limit_bytes=mib << 20)


def per_device(forcing, search_direction, ocean_depth, land_mask, fold_map):
    lat_count, lon_count = lax.axis_size("lat"), lax.axis_size(LON)
    call = pl.pallas_call
    fields, first, second, reach, choice = call(
        functools.partial(pack_kernel, lon_count // 2), name="pack",
        in_specs=[pl.BlockSpec(memory_space=pl.ANY)] * 5,
        out_specs=[pl.BlockSpec(memory_space=pltpu.VMEM)] * 3 + [pl.BlockSpec(memory_space=pltpu.SMEM)] * 2,
        out_shape=(shape(3, ROWS, LANES), shape(BLK + 32, LANES), shape(BLK + 32, LANES),
                   pltpu.SMEM((1,), jnp.int32), pltpu.SMEM((1,), jnp.int32)),
        scratch_shapes=[pltpu.VMEM((ROWS, LANES), F32)] * 3 + [
            pltpu.VMEM((ROWS, LANES), jnp.int32), pltpu.SMEM((LANES,), jnp.int32), pltpu.SemaphoreType.DMA((5,)),
        ],
        compiler_params=limit(4),
    )(*held(forcing, search_direction, ocean_depth, land_mask, fold_map, space=pltpu.HBM))
    def lon_round(start):
        pairs = []
        for row in range(lat_count):
            for i in range((start + row) % 2, lon_count, 2):
                a, b = row * lon_count + i, row * lon_count + (i + 1) % lon_count
                pairs += [(a, b), (b, a)]
        return pairs

    second = lax.ppermute(second, ("lat",) + LON, lon_round(1))
    first = lax.ppermute(first, ("lat",) + LON, lon_round(0))

    one, two, two_next = call(
        functools.partial(turn_kernel, lat_count - 1), name="turn",
        in_specs=[pl.BlockSpec(memory_space=pltpu.SMEM)] + [pl.BlockSpec(memory_space=pltpu.VMEM)] * 3,
        out_shape=(shape(64, LANES),) * 3,
        scratch_shapes=[pltpu.VMEM((BLK + 32, LANES), F32)] * 2 + [pltpu.VMEM((64, LANES), F32)] * 4,
        compiler_params=limit(4),
    )(reach, *held(fields, second, first))

    evens, odds = range(0, lat_count, 2), range(1, lat_count - 1, 2)
    pairs = [(i, i + 1) for i in evens] + [(i + 1, i) for i in evens]
    swaps = [
        (i * lon_count + c, (i + s) * lon_count + c)
        for k in odds for i, s in ((k, 1), (k + 1, -1)) for c in range(lon_count)
    ]
    top = (lat_count - 1) * lon_count

    def second_round(value, pairing, others):
        fold = [(top + i, top + (2 * pairing - i) % lon_count) for i in range(lon_count)]
        return lax.ppermute(value, ("lat",) + LON, others + fold)

    def branch(index):
        def exchange(one, near, far, fields, second, first):
            value = second_round(near, index // 2, swaps)
            if index % 2:
                pairing = (index // 2 + 1) % (lon_count // 2)
                value = value + second_round(far, pairing, swaps if pairing == 0 else [])
            one = lax.ppermute(one, "lat", pairs)
            ready = call(
                prepare_kernel, name="prepare",
                out_shape=(shape(2, PITCH, LANES), shape(2, PITCH, LANES), shape(2, PITCH, LANES),
                           shape(2, 9, PITCH, LANES)),
                scratch_shapes=[pltpu.VMEM((BLK + 32, LANES), F32)] * 2,
                compiler_params=limit(4),
                cost_estimate=pl.CostEstimate(flops=4_000_000, transcendentals=0, bytes_accessed=0),
            )(*held(fields, second, first))
            landed = call(
                land_kernel, name="land", out_shape=(shape(64, LANES),) * 2, compiler_params=limit(2),
            )(*held(value, one))
            return *ready, *landed

        return exchange

    depth, side, inv, coef, south, north = lax.switch(
        choice[0], [branch(i) for i in range(lon_count)], one, two, two_next, fields, second, first
    )

    basis, sums, *_ = call(
        basis_kernel, name="basis",
        out_shape=(shape(VECTORS, PITCH, LANES), shape(lat_count, LANES), shape(2, PITCH, LANES),
                   shape(2, PITCH, LANES), shape(2, 9, PITCH, LANES)),
        scratch_shapes=[
            pltpu.VMEM((VECTORS, PITCH, LANES), F32),
            pltpu.VMEM((6 * STEPS, 8, LANES), F32),
        ],
        input_output_aliases={2: 2, 3: 3, 4: 4},
        compiler_params=limit(12),
    )(*held(fields, side, depth, inv, coef, south, north))
    sums = lax.all_to_all(sums, "lat", split_axis=0, concat_axis=0, tiled=True)
    sums = call(middle_kernel, name="middle", out_shape=shape(lon_count, LANES), compiler_params=limit(2))(*held(sums))
    sums = lax.all_to_all(sums, LON, split_axis=0, concat_axis=0, tiled=True)
    return call(
        final_kernel, name="final", out_shape=(jax.ShapeDtypeStruct((ROWS, LANES), F32),) * 2,
        out_specs=[pl.BlockSpec(memory_space=pl.ANY)] * 2,
        scratch_shapes=[pltpu.VMEM((ROWS, LANES), F32)] * 2 + [pltpu.SemaphoreType.DMA((8,))],
        compiler_params=limit(4),
    )(*held(sums, basis))


def solution(mesh):
    lon = mesh.shape["lon"]
    split = Mesh(mesh.devices.reshape(mesh.shape["lat"], lon // 4, 4), ("lat", "lon_0", "lon_1"))
    return jax.shard_map(
        per_device,
        mesh=split,
        in_specs=(P("lat", LON), P("lat", LON), P("lat", LON), P("lat", LON), P()),
        out_specs=(P("lat", LON), P("lat", LON)),
        check_vma=False,
    )
```

```python
import functools

import jax
import jax.numpy as jnp
from jax import lax
from jax.experimental import pallas as pl
from jax.experimental.pallas import tpu as pltpu
from jax.sharding import Mesh
from jax.sharding import PartitionSpec as P

STEPS = 8
REACH = 256
ROWS = 160
LANES = 128
EXT = ROWS + 32
PITCH = 216
EDGE = 9
BLK = 32
LON = ("lon_0", "lon_1")
VECTORS = 2 * STEPS + 1
F32 = jnp.float32


def edge_of(q, blk):
    return (9 * blk, 45 + 8 * blk, 85 + 8 * blk)[q], (9, 8, 8)[q]


def lanes_of(rows):
    return lax.broadcasted_iota(jnp.int32, (rows, LANES), 1)


def shift_east(a, b, lane):
    ra, rb = pltpu.roll(a, 1, 1), pltpu.roll(b, 1, 1)
    first = lane == 0
    return jnp.where(first, rb, ra), jnp.where(first, ra, rb)


def shift_west(a, b, lane):
    ra, rb = pltpu.roll(a, LANES - 1, 1), pltpu.roll(b, LANES - 1, 1)
    last = lane == LANES - 1
    return jnp.where(last, rb, ra), jnp.where(last, ra, rb)


def pack_kernel(pairs, f_hbm, p_hbm, d_hbm, m_hbm, map_hbm, x_ref, first_ref, second_ref, reach_ref, choice_ref,
                f_ref, p_ref, d_ref, m_ref, pivot, sems):
    even = turns(LON)
    copies = [
        pltpu.make_async_copy(source, target, sems.at[i])
        for i, (source, target) in enumerate((
            (m_hbm, m_ref), (d_hbm, d_ref), (f_hbm, f_ref), (p_hbm, p_ref), (map_hbm.at[pl.ds(0, LANES)], pivot),
        ))
    ]
    for copy in copies:
        copy.start()
    for copy in copies:
        copy.wait()
    for g in range(ROWS // 8):
        rows = pl.ds(8 * g, 8)
        flag = m_ref[rows, :].astype(F32)
        x_ref[0, rows, :] = d_ref[rows, :] * flag
        x_ref[1, rows, :] = f_ref[rows, :] * flag
        x_ref[2, rows, :] = p_ref[rows, :] * flag
    lane = lanes_of(8)
    for v in range(BLK // 8):
        east = jnp.zeros((8, LANES), F32)
        west = jnp.zeros((8, LANES), F32)
        for q in range(3):
            for blk in range(ROWS // BLK):
                at, width = edge_of(q, blk)
                tile = x_ref[q, pl.ds(BLK * blk + 8 * v, 8), :]
                tile = pltpu.roll(tile, at, 1) if at else tile
                west = jnp.where((lane >= at) & (lane < at + width), tile, west)
                start = (at - width) % LANES
                east = jnp.where((lane >= start) & (lane < start + width), tile, east)
        first_ref[pl.ds(8 * v, 8), :] = jnp.where(even, east, west)
        second_ref[pl.ds(8 * v, 8), :] = jnp.where(even, west, east)
    for slot, (q, row) in enumerate(((0, ROWS - 8), (1, ROWS - 8), (2, ROWS - 8), (0, ROWS - 16))):
        tile = x_ref[q, pl.ds(row, 8), :]
        first_ref[pl.ds(BLK + 8 * slot, 8), :] = tile
        second_ref[pl.ds(BLK + 8 * slot, 8), :] = tile
    past = pivot[0] + (2 * pairs * LANES - 8)
    reach = past % (2 * LANES) + 8
    reach_ref[0] = reach
    split = jnp.where(reach + EDGE >= 2 * LANES, 1, 0)
    choice_ref[0] = 2 * ((past // (2 * LANES)) % pairs) + split


def unpack_halo(from_west, from_east, q, blk, v, lane):
    at, width = edge_of(q, blk)
    right = from_east[pl.ds(8 * v, 8), :]
    left = from_west[pl.ds(8 * v, 8), :]
    both = jnp.where((lane >= at) & (lane < at + EDGE), right, left)
    both = pltpu.roll(both, LANES - at, 1) if at else both
    return jnp.where((lane < EDGE) | (lane >= LANES - EDGE), both, 0.0)


def turns(axis):
    place = lax.axis_index("lat")
    if axis == LON:
        place = place + lax.axis_index(LON)
    return place % 2 == 0


def sort_partners(axis, first, second, before, after):
    even = turns(axis)
    for g in range(first.shape[0] // 8):
        rows = pl.ds(8 * g, 8)
        a, b = first[rows, :], second[rows, :]
        before[rows, :] = jnp.where(even, b, a)
        after[rows, :] = jnp.where(even, a, b)


def turn_kernel(tops, r_ref, x_ref, second_ref, first_ref, one_ref, two_ref, next_ref,
                fw_ref, fe_ref, north_ref, south_ref, t1_ref, t2_ref):
    lane = lanes_of(8)
    lat = lax.axis_index("lat")
    even, top_row = lat % 2 == 0, lat == tops
    sort_partners(LON, first_ref, second_ref, fw_ref, fe_ref)
    top, low = ROWS // 8 - 1, 0
    for ref, rows in (
        (north_ref, ((0, top), (1, top), (2, top), (0, top - 1))),
        (south_ref, ((0, low), (1, low), (2, low), (0, low + 1))),
    ):
        for slot, (q, g) in enumerate(rows):
            ref[pl.ds(8 * slot, 8), :] = x_ref[q, pl.ds(8 * g, 8), :]
            blk, v = 8 * g // BLK, (8 * g % BLK) // 8
            ref[pl.ds(32 + 8 * slot, 8), :] = unpack_halo(fw_ref, fe_ref, q, blk, v, lane)
    for g in range(8):
        rows = pl.ds(8 * g, 8)
        north, south = north_ref[rows, :], south_ref[rows, :]
        one_ref[rows, :] = jnp.where(even, north, south)
        two_ref[rows, :] = jnp.where(even, south, north)
        next_ref[rows, :] = jnp.zeros((8, LANES), F32)

    @pl.when(top_row)
    def _():
        across_fold(r_ref[0], lane, north_ref, fw_ref, fe_ref, two_ref, next_ref, t1_ref, t2_ref)


def across_fold(reach, lane, north_ref, fw_ref, fe_ref, fold_ref, next_ref, t1_ref, t2_ref):
    along = reach - lane
    pick = along & (LANES - 1)
    place_a = along
    place_b = jnp.where(lane < EDGE, along - LANES, along + LANES)
    halo = (lane < EDGE) | (lane >= LANES - EDGE)
    for slot in range(4):
        rows = pl.ds(8 * slot, 8)
        own = jnp.take_along_axis(north_ref[rows, :], pick, axis=1, mode="promise_in_bounds")
        west = jnp.take_along_axis(fw_ref[pl.ds(BLK + 8 * slot, 8), :], pick, axis=1, mode="promise_in_bounds")
        east = jnp.take_along_axis(fe_ref[pl.ds(BLK + 8 * slot, 8), :], pick, axis=1, mode="promise_in_bounds")
        for part, place in ((0, place_a), (32, place_b)):
            near = jnp.where(place < 0, west, jnp.where(place < LANES, own, east))
            near = jnp.where(place < 2 * LANES, near, 0.0)
            far = jnp.where(place >= 2 * LANES, own, 0.0)
            if part:
                near = jnp.where(halo, near, 0.0)
                far = jnp.where(halo, far, 0.0)
            t1_ref[pl.ds(part + 8 * slot, 8), :] = near
            t2_ref[pl.ds(part + 8 * slot, 8), :] = far
    for g in range(8):
        for m in range(8):
            fold_ref[pl.ds(8 * g + m, 1), :] = t1_ref[pl.ds(8 * g + 7 - m, 1), :]
            next_ref[pl.ds(8 * g + m, 1), :] = t2_ref[pl.ds(8 * g + 7 - m, 1), :]


GROUPS = ROWS // 8 + 2


def root_of(depth, inv, at, lane):
    vert, mid, wet_mid, deep = [], [], [], []
    for t in range(2):
        down = depth[t, pl.ds(at - 1, 8), :]
        here = depth[t, pl.ds(at, 8), :]
        up = depth[t, pl.ds(at + 1, 8), :]
        wet = jnp.where(here > 0.0, 1.0, 0.0)
        wets = jnp.where(down > 0.0, 1.0, 0.0) + jnp.where(up > 0.0, 1.0, 0.0)
        vert.append((down + up, wets))
        mid.append((here + 0.5 * (down + up), wet + 0.5 * wets))
        deep.append(here)
        wet_mid.append(wet)
    sums = []
    for c in range(2):
        ea, eb = shift_east(mid[0][c], mid[1][c], lane)
        wa, wb = shift_west(mid[0][c], mid[1][c], lane)
        sums.append((vert[0][c] + (ea + wa), vert[1][c] + (eb + wb)))
    for t in range(2):
        links = 0.5 * (deep[t] * sums[1][t] + sums[0][t])
        diagonal = wet_mid[t] * (deep[t] / (REACH * REACH) + links) + (1.0 - wet_mid[t])
        inv[t, pl.ds(at, 8), :] = lax.rsqrt(diagonal) * wet_mid[t]


def coefs_of(depth, inv, coef, at, lane):
    d = [[depth[t, pl.ds(at + s, 8), :] for s in (-1, 0, 1)] for t in range(2)]
    r = [[inv[t, pl.ds(at + s, 8), :] for s in (-1, 0, 1)] for t in range(2)]
    de, re = shift_east(d[0][1], d[1][1], lane), shift_east(r[0][1], r[1][1], lane)
    dw, rw = shift_west(d[0][1], d[1][1], lane), shift_west(r[0][1], r[1][1], lane)
    for t in range(2):
        for base, (dc, rc) in enumerate(((d[t][1], r[t][1]), (de[t], re[t]), (dw[t], rw[t]))):
            for s in range(3):
                if base == 0 and s == 1:
                    continue
                whole = base == 0 or s == 1
                c = (dc + d[t][s]) * (rc * r[t][s])
                coef[t, 3 * base + s, pl.ds(at, 8), :] = c * (-1.0 if whole else -0.5)


def prepare_kernel(x_ref, second_ref, first_ref, depth, side, inv, coef, fw_ref, fe_ref):
    sort_partners(LON, first_ref, second_ref, fw_ref, fe_ref)
    lane = lanes_of(8)

    def unpack(v, carry):
        for q, ref in ((0, depth.at[1]), (1, side.at[1]), (2, side.at[0])):
            for blk in range(ROWS // BLK):
                rows = pl.ds(pl.multiple_of(16 + BLK * blk + 8 * v, 8), 8)
                ref[rows, :] = unpack_halo(fw_ref, fe_ref, q, blk, v, lane)
        return carry

    for g in range(ROWS // 8):
        depth[0, pl.ds(16 + 8 * g, 8), :] = x_ref[0, pl.ds(8 * g, 8), :]
    lax.fori_loop(0, BLK // 8, unpack, 0)

    def roots(i, carry):
        for g in range(6):
            root_of(depth, inv, pl.multiple_of(24 + 48 * i, 8) + 8 * g, lane)
        return carry

    def coefs(i, carry):
        for g in range(4):
            coefs_of(depth, inv, coef, pl.multiple_of(32 + 32 * i, 8) + 8 * g, lane)
        return carry

    lax.fori_loop(0, 3, roots, 0)
    lax.fori_loop(0, 4, coefs, 0)


def land_kernel(two_ref, one_ref, south_ref, north_ref):
    sort_partners("lat", one_ref, two_ref, south_ref, north_ref)


def basis_kernel(x_ref, side_ref, _depth, _inv, _coef, fs_ref, fn_ref, basis_ref, sums_ref, depth, inv, coef,
                 side, acc):
    lane = lanes_of(8)
    zero = jnp.zeros((8, LANES), F32)
    for q, k in ((1, STEPS + 1), (2, 0)):
        for g in range(ROWS // 8):
            rows = pl.ds(16 + 8 * g, 8)
            basis_ref[k, rows, :] = x_ref[q, pl.ds(8 * g, 8), :]
            side[k, rows, :] = side_ref[2 - q, rows, :]
    targets = (
        lambda t: depth.at[t],
        lambda t: (basis_ref if t == 0 else side).at[STEPS + 1],
        lambda t: (basis_ref if t == 0 else side).at[0],
    )
    for q in range(3):
        own, rim = targets[q](0), targets[q](1)
        for t, ref in ((0, own), (1, rim)):
            at = 32 * t + 8 * q
            ref[pl.ds(8, 8), :] = fs_ref[pl.ds(at, 8), :]
            ref[pl.ds(EXT - 16, 8), :] = fn_ref[pl.ds(at, 8), :]
            if q == 0:
                at = 32 * t + 24
                ref[pl.ds(0, 8), :] = fs_ref[pl.ds(at, 8), :]
                ref[pl.ds(EXT - 8, 8), :] = fn_ref[pl.ds(at, 8), :]
            else:
                ref[pl.ds(0, 8), :] = zero
                ref[pl.ds(EXT - 8, 8), :] = zero
    for k in list(range(1, STEPS + 1)) + list(range(STEPS + 2, VECTORS)):
        for ref in (basis_ref, side):
            ref[k, pl.ds(0, 8), :] = zero
            ref[k, pl.ds(EXT - 8, 8), :] = zero
    for t in range(2):
        inv[t, pl.ds(0, 8), :] = zero
        inv[t, pl.ds(EXT - 8, 8), :] = zero

    for g in (0, 1, GROUPS - 2, GROUPS - 1):
        root_of(depth, inv, 8 + 8 * g, lane)
    for g in (0, 1, 2, GROUPS - 3, GROUPS - 2, GROUPS - 1):
        coefs_of(depth, inv, coef, 8 + 8 * g, lane)

    def twice_applied(k, at, tiles, weights):
        parts = []
        for t in range(2):
            ref = basis_ref if t == 0 else side
            down, here, up = (ref[k, pl.ds(at + s, 8), :] for s in (-1, 0, 1))
            w = weights[t]
            straight = w[0] * down + w[2] * up
            toward_w = (w[3] * down + w[5] * up) + w[4] * here
            toward_e = (w[6] * down + w[8] * up) + w[7] * here
            parts.append((straight, toward_w, toward_e, here))
        wa, wb = shift_west(parts[0][1], parts[1][1], lane)
        ea, eb = shift_east(parts[0][2], parts[1][2], lane)
        return ((parts[0][0] + (wa + ea), parts[1][0] + (wb + eb))[:tiles], parts[0][3])

    def weights_at(at):
        return [[None if i == 1 else coef[t, i, pl.ds(at, 8), :] for i in range(9)] for t in range(2)]

    def step(k, first, last):
        total = [zero] * 6
        tiles = 1 if last else 2
        for g in range(1, GROUPS - 1) if last else range(GROUPS):
            at = 8 + 8 * g
            w = weights_at(at)
            now, new = [], []
            for base in ((0,) if last else (0, STEPS + 1)):
                out, here = twice_applied(base + k, at, tiles, w)
                now.append(here)
                for t in range(tiles):
                    ref = basis_ref if t == 0 else side
                    value = 0.5 * out[t] if first else out[t] - ref[base + k - 1, pl.ds(at, 8), :]
                    ref[base + k + 1, pl.ds(at, 8), :] = value
                    if t == 0:
                        new.append(value)
            if last:
                now.append(basis_ref[STEPS + 1 + k, pl.ds(at, 8), :])
            if 1 <= g <= ROWS // 8:
                p, r = now
                total[0] += p * p
                total[1] += p * new[0]
                total[2] += r * r
                total[3] += new[0] * new[0] if last else r * new[1]
                total[4] += p * r
                total[5] += new[0] * r
        for i in range(6):
            acc[6 * k + i, :, :] = total[i]

    step(0, True, False)

    def middle(k, carry):
        step(k, False, False)
        return carry

    lax.fori_loop(1, STEPS - 1, middle, 0, unroll=2)
    step(STEPS - 1, False, True)

    flat = jnp.sum(acc[...], axis=1)
    flat = jnp.concatenate([flat, jnp.zeros((LANES - 6 * STEPS, LANES), F32)], axis=0)
    row = jnp.broadcast_to(jnp.sum(flat.T, axis=0, keepdims=True), (8, LANES))
    for g in range(sums_ref.shape[0] // 8):
        sums_ref[pl.ds(8 * g, 8), :] = row


def middle_kernel(in_ref, out_ref):
    out_ref[...] = jnp.broadcast_to(jnp.sum(in_ref[...], axis=0, keepdims=True), out_ref.shape)


def final_kernel(sum_ref, basis_ref, height_hbm, residual_hbm, height_ref, residual_ref, sems):
    products = jnp.broadcast_to(jnp.sum(sum_ref[...], axis=0, keepdims=True), (8, LANES))
    row = lax.broadcasted_iota(jnp.int32, (24, LANES), 0)
    first = row == 0
    odd = row & 1

    def gathered(index):
        parts = [
            jnp.take_along_axis(products, index[8 * g : 8 * g + 8], axis=1, mode="promise_in_bounds")
            for g in range(3)
        ]
        return jnp.concatenate(parts, axis=0)

    def moments(slot, count):
        index = jnp.where(row < count, 6 * (row >> 1) + odd + slot, LANES - 1)
        if count > 2 * STEPS:
            index = jnp.where(row == 2 * STEPS, 6 * (STEPS - 1) + 3, index)
        return 2.0 * gathered(index) - gathered(jnp.where(row < count, odd + slot, LANES - 1))

    def raised(v):
        up = pltpu.roll(v, 23, 0)
        return v + 0.5 * (up + jnp.where(first, up, pltpu.roll(v, 1, 0)))

    def mapped(v):
        down = pltpu.roll(jnp.where(first, v, 0.5 * v), 1, 0)
        return v + down + pltpu.roll(jnp.where(first, 0.0, 0.5 * v), 23, 0)

    def dot(u, v):
        return jnp.sum(u[0] * v[0] + u[1] * v[1], axis=0, keepdims=True)

    pair = (0, 1)
    unit, zero = jnp.where(first, 1.0, 0.0), jnp.zeros((24, LANES), F32)
    pp, rr, pr = moments(0, 2 * STEPS + 1), moments(2, 2 * STEPS - 1), moments(4, 2 * STEPS)
    xc, pc, rc = (zero, zero), (unit, zero), (zero, unit)
    with_r, with_q = (pr, rr), (raised(pp), raised(pr))
    norm = dot(rc, with_r)
    for _ in range(STEPS):
        t = norm / dot(pc, with_q)
        inverse = 1.0 / norm
        with_r = [with_r[i] - t * with_q[i] for i in pair]
        rc, xc = [rc[i] - t * mapped(pc[i]) for i in pair], [xc[i] + t * pc[i] for i in pair]
        norm = dot(rc, with_r)
        ratio = norm * inverse
        with_q = [raised(with_r[i]) + ratio * with_q[i] for i in pair]
        pc = [rc[i] + ratio * pc[i] for i in pair]
    spots = [(0, k) for k in range(STEPS + 1)] + [(1, k) for k in range(STEPS)]
    xs = [jnp.broadcast_to(xc[i][k : k + 1, :], (8, LANES)) for i, k in spots]
    rs = [jnp.broadcast_to(rc[i][k : k + 1, :], (8, LANES)) for i, k in spots]
    copies = []
    for part in range(4):
        for g in range(part * ROWS // 32, (part + 1) * ROWS // 32):
            above = below = None
            for k in range(VECTORS):
                tile = basis_ref[k, pl.ds(16 + 8 * g, 8), :]
                above = xs[k] * tile if above is None else above + xs[k] * tile
                below = rs[k] * tile if below is None else below + rs[k] * tile
            height_ref[pl.ds(8 * g, 8), :] = above
            residual_ref[pl.ds(8 * g, 8), :] = below
        rows = pl.ds(part * ROWS // 4, ROWS // 4)
        for i, (source, target) in enumerate(((height_ref, height_hbm), (residual_ref, residual_hbm))):
            copies.append(pltpu.make_async_copy(source.at[rows], target.at[rows], sems.at[2 * part + i]))
            copies[-1].start()
    for copy in copies:
        copy.wait()


def shape(*dims):
    return pltpu.VMEM(dims, F32)


def held(*values, space=pltpu.VMEM):
    return tuple(pltpu.with_memory_space_constraint(v, space) for v in values)


def limit(mib):
    return pltpu.CompilerParams(vmem_limit_bytes=mib << 20)


def per_device(forcing, search_direction, ocean_depth, land_mask, fold_map):
    lat_count, lon_count = lax.axis_size("lat"), lax.axis_size(LON)
    call = pl.pallas_call
    fields, first, second, reach, choice = call(
        functools.partial(pack_kernel, lon_count // 2), name="pack",
        in_specs=[pl.BlockSpec(memory_space=pl.ANY)] * 5,
        out_specs=[pl.BlockSpec(memory_space=pltpu.VMEM)] * 3 + [pl.BlockSpec(memory_space=pltpu.SMEM)] * 2,
        out_shape=(shape(3, ROWS, LANES), shape(BLK + 32, LANES), shape(BLK + 32, LANES),
                   pltpu.SMEM((1,), jnp.int32), pltpu.SMEM((1,), jnp.int32)),
        scratch_shapes=[pltpu.VMEM((ROWS, LANES), F32)] * 3 + [
            pltpu.VMEM((ROWS, LANES), jnp.int32), pltpu.SMEM((LANES,), jnp.int32), pltpu.SemaphoreType.DMA((5,)),
        ],
        compiler_params=limit(4),
    )(*held(forcing, search_direction, ocean_depth, land_mask, fold_map, space=pltpu.HBM))
    def lon_round(start):
        pairs = []
        for row in range(lat_count):
            for i in range((start + row) % 2, lon_count, 2):
                a, b = row * lon_count + i, row * lon_count + (i + 1) % lon_count
                pairs += [(a, b), (b, a)]
        return pairs

    second = lax.ppermute(second, ("lat",) + LON, lon_round(1))
    first = lax.ppermute(first, ("lat",) + LON, lon_round(0))

    one, two, two_next = call(
        functools.partial(turn_kernel, lat_count - 1), name="turn",
        in_specs=[pl.BlockSpec(memory_space=pltpu.SMEM)] + [pl.BlockSpec(memory_space=pltpu.VMEM)] * 3,
        out_shape=(shape(64, LANES),) * 3,
        scratch_shapes=[pltpu.VMEM((BLK + 32, LANES), F32)] * 2 + [pltpu.VMEM((64, LANES), F32)] * 4,
        compiler_params=limit(4),
    )(reach, *held(fields, second, first))

    evens, odds = range(0, lat_count, 2), range(1, lat_count - 1, 2)
    pairs = [(i, i + 1) for i in evens] + [(i + 1, i) for i in evens]
    swaps = [
        (i * lon_count + c, (i + s) * lon_count + c)
        for k in odds for i, s in ((k, 1), (k + 1, -1)) for c in range(lon_count)
    ]
    top = (lat_count - 1) * lon_count

    def second_round(value, pairing, others):
        fold = [(top + i, top + (2 * pairing - i) % lon_count) for i in range(lon_count)]
        return lax.ppermute(value, ("lat",) + LON, others + fold)

    def branch(index):
        def exchange(one, near, far, fields, second, first):
            value = second_round(near, index // 2, swaps)
            if index % 2:
                pairing = (index // 2 + 1) % (lon_count // 2)
                value = value + second_round(far, pairing, swaps if pairing == 0 else [])
            one = lax.ppermute(one, "lat", pairs)
            ready = call(
                prepare_kernel, name="prepare",
                out_shape=(shape(2, PITCH, LANES), shape(2, PITCH, LANES), shape(2, PITCH, LANES),
                           shape(2, 9, PITCH, LANES)),
                scratch_shapes=[pltpu.VMEM((BLK + 32, LANES), F32)] * 2,
                compiler_params=limit(4),
                cost_estimate=pl.CostEstimate(flops=4_000_000, transcendentals=0, bytes_accessed=0),
            )(*held(fields, second, first))
            landed = call(
                land_kernel, name="land", out_shape=(shape(64, LANES),) * 2, compiler_params=limit(2),
            )(*held(value, one))
            return *ready, *landed

        return exchange

    depth, side, inv, coef, south, north = lax.switch(
        choice[0], [branch(i) for i in range(lon_count)], one, two, two_next, fields, second, first
    )

    basis, sums, *_ = call(
        basis_kernel, name="basis",
        out_shape=(shape(VECTORS, PITCH, LANES), shape(lat_count, LANES), shape(2, PITCH, LANES),
                   shape(2, PITCH, LANES), shape(2, 9, PITCH, LANES)),
        scratch_shapes=[
            pltpu.VMEM((VECTORS, PITCH, LANES), F32),
            pltpu.VMEM((6 * STEPS, 8, LANES), F32),
        ],
        input_output_aliases={2: 2, 3: 3, 4: 4},
        compiler_params=pltpu.CompilerParams(vmem_limit_bytes=12 << 20),
    )(*held(fields, side, depth, inv, coef, south, north))
    sums = lax.all_to_all(sums, "lat", split_axis=0, concat_axis=0, tiled=True)
    sums = call(middle_kernel, name="middle", out_shape=shape(lon_count, LANES), compiler_params=limit(2))(*held(sums))
    sums = lax.all_to_all(sums, LON, split_axis=0, concat_axis=0, tiled=True)
    return call(
        final_kernel, name="final", out_shape=(jax.ShapeDtypeStruct((ROWS, LANES), F32),) * 2,
        out_specs=[pl.BlockSpec(memory_space=pl.ANY)] * 2,
        scratch_shapes=[pltpu.VMEM((ROWS, LANES), F32)] * 2 + [pltpu.SemaphoreType.DMA((8,))],
        compiler_params=limit(4),
    )(*held(sums, basis))


def solution(mesh):
    lon = mesh.shape["lon"]
    split = Mesh(mesh.devices.reshape(mesh.shape["lat"], lon // 4, 4), ("lat", "lon_0", "lon_1"))
    return jax.shard_map(
        per_device,
        mesh=split,
        in_specs=(P("lat", LON), P("lat", LON), P("lat", LON), P("lat", LON), P()),
        out_specs=(P("lat", LON), P("lat", LON)),
        check_vma=False,
    )
```
